16 devices in a mesh: dp: 2 (over y, z), pp: 8 (over x, core).
Axes of the slice: x: 4, y: 2, z: 1, core: 2. Of those that a mesh axis runs over, the one named last changes fastest.
The devices are a block of a 4x4x8 slice.
Arguments:
- x_in: bfloat16 [16, 4, 128, 768], P(('dp', 'pp')), parts along dimension 0
- dy_out: bfloat16 [16, 4, 128, 768], P(('dp', 'pp')), parts along dimension 0
- w_qkv: bfloat16 [8, 2, 1, 768, 3, 16, 48], P('pp')
- w_attn: bfloat16 [8, 2, 1, 16, 48, 768], P('pp')
- w_fc: bfloat16 [8, 2, 1, 768, 3072], P('pp')
- w_proj: bfloat16 [8, 2, 1, 3072, 768], P('pp')
- b_qkv: bfloat16 [8, 2, 1, 3, 16, 48], P('pp')
- b_fc: bfloat16 [8, 2, 1, 3072], P('pp')
- vec_d: bfloat16 [8, 2, 1, 6, 768], P('pp')
Outputs:
- output 1: bfloat16 [16, 4, 128, 768], P(('dp', 'pp')), parts along dimension 0
- output 2: bfloat16 [16, 4, 128, 768], P(('dp', 'pp')), parts along dimension 0
- output 3: float32 [16, 2, 1, 768, 3, 16, 48], P(('dp', 'pp')), parts along dimension 0
- output 4: float32 [16, 2, 1, 16, 48, 768], P(('dp', 'pp')), parts along dimension 0
- output 5: float32 [16, 2, 1, 768, 3072], P(('dp', 'pp')), parts along dimension 0
- output 6: float32 [16, 2, 1, 3072, 768], P(('dp', 'pp')), parts along dimension 0
- output 7: float32 [16, 2, 1, 3, 16, 48], P(('dp', 'pp')), parts along dimension 0
- output 8: float32 [16, 2, 1, 3072], P(('dp', 'pp')), parts along dimension 0
- output 9: float32 [16, 2, 1, 6, 768], P(('dp', 'pp')), parts along dimension 0
There are 2 independent parts. The reference program is written for one: setup_inputs(seed, part) draws one part's arguments, and reference() takes and returns one part's arrays. A program takes and returns all parts, laid end to end along the dimension named above; an argument that names none is the same for every part.
All inputs are finite; a program needn't handle non-finite values.
Results may differ from the reference program's by a relative error of at most 0.02.
Values are sent between devices in bfloat16 or wider.
A program may use at most 768 MiB of HBM per device.

```python
import jax
import jax.numpy as jnp
from jax import lax

STAGES = 8
MICRO = 8
LPS = 1
BATCH = 4
SEQ = 128
DM = 768
HEADS = 16
FF = 3072
HEAD = DM // HEADS
LAYERS = STAGES * LPS
EPSILON = 1e-5


def with_second_copy(stage_major):
    return jnp.stack([stage_major, stage_major[::-1]], axis=1).astype(jnp.bfloat16)


def setup_inputs(seed: int = 0, part: int = 0) -> dict:
    root_key = jax.random.key(seed)
    data_keys = jax.random.split(jax.random.fold_in(root_key, part), 2)
    w_keys = jax.random.split(jax.random.key(seed + 7919), 7)
    res_scale = (2.0 * LAYERS) ** -0.5
    act_shape = (MICRO, BATCH, SEQ, DM)
    x_in = jax.random.normal(data_keys[0], act_shape, jnp.float32).astype(jnp.bfloat16)
    dy_out = jax.random.normal(data_keys[1], act_shape, jnp.float32).astype(jnp.bfloat16)
    w_qkv = with_second_copy(jax.random.normal(w_keys[0], (STAGES, LPS, DM, 3, HEADS, HEAD), jnp.float32) * DM ** -0.5)
    w_attn = with_second_copy(jax.random.normal(w_keys[1], (STAGES, LPS, HEADS, HEAD, DM), jnp.float32) * (DM ** -0.5 * res_scale))
    w_fc = with_second_copy(jax.random.normal(w_keys[2], (STAGES, LPS, DM, FF), jnp.float32) * DM ** -0.5)
    w_proj = with_second_copy(jax.random.normal(w_keys[3], (STAGES, LPS, FF, DM), jnp.float32) * (FF ** -0.5 * res_scale))
    b_qkv = with_second_copy(0.3 * jax.random.normal(w_keys[4], (STAGES, LPS, 3, HEADS, HEAD), jnp.float32))
    b_fc = with_second_copy(0.3 * jax.random.normal(w_keys[5], (STAGES, LPS, FF), jnp.float32))
    row_scale = jnp.array([0.2, 0.2, 0.5 * res_scale, 0.2, 0.2, 0.5 * res_scale], jnp.float32)
    row_shift = jnp.array([1.0, 0.0, 0.0, 1.0, 0.0, 0.0], jnp.float32)
    vec_rows = jax.random.normal(w_keys[6], (STAGES, LPS, 6, DM), jnp.float32)
    vec_d = with_second_copy(vec_rows * row_scale[:, None] + row_shift[:, None])
    return {'x_in': x_in, 'dy_out': dy_out, 'w_qkv': w_qkv, 'w_attn': w_attn, 'w_fc': w_fc, 'w_proj': w_proj, 'b_qkv': b_qkv, 'b_fc': b_fc, 'vec_d': vec_d}


def layer_norm(rows_in, ln_gain, ln_shift):
    rows_f32 = rows_in.astype(jnp.float32)
    row_mean = jnp.mean(rows_f32, axis=-1, keepdims=True)
    centered = rows_f32 - row_mean
    row_var = jnp.mean(centered * centered, axis=-1, keepdims=True)
    scaled = centered * lax.rsqrt(row_var + EPSILON)
    return (scaled * ln_gain.astype(jnp.float32) + ln_shift.astype(jnp.float32)).astype(jnp.bfloat16)


def gpt_layer(hidden_in, layer_w):
    w_qkv, w_attn, w_fc, w_proj, b_qkv, b_fc, vec_d = layer_w
    n_batch, seq_len, d_model = hidden_in.shape
    n_heads, head_dim = w_qkv.shape[-2], w_qkv.shape[-1]
    tokens = n_batch * seq_len
    flat_rows = hidden_in.reshape(tokens, d_model)
    normed = layer_norm(flat_rows, vec_d[0], vec_d[1])
    qkv_proj = jnp.dot(normed, w_qkv.reshape(d_model, 3 * d_model), preferred_element_type=jnp.float32)
    qkv_proj = (qkv_proj + b_qkv.reshape(3 * d_model).astype(jnp.float32)).astype(jnp.bfloat16)
    qkv_proj = qkv_proj.reshape(n_batch, seq_len, 3, n_heads, head_dim)
    query_heads = qkv_proj[:, :, 0].astype(jnp.float32)
    key_heads = qkv_proj[:, :, 1].astype(jnp.float32)
    value_heads = qkv_proj[:, :, 2].astype(jnp.float32)
    scores = jnp.einsum('bqhe,bkhe->bhqk', query_heads, key_heads) * (head_dim ** -0.5)
    causal = jnp.arange(seq_len)[:, None] >= jnp.arange(seq_len)[None, :]
    scores = jnp.where(causal, scores, -1e30)
    attn_probs = jax.nn.softmax(scores, axis=-1).astype(jnp.bfloat16)
    mixed_heads = jnp.einsum('bhqk,bkhe->bqhe', attn_probs.astype(jnp.float32), value_heads).astype(jnp.bfloat16)
    attn_out = jnp.dot(mixed_heads.reshape(tokens, d_model), w_attn.reshape(d_model, d_model), preferred_element_type=jnp.float32)
    residual = (flat_rows.astype(jnp.float32) + attn_out + vec_d[2].astype(jnp.float32)).astype(jnp.bfloat16)
    normed_two = layer_norm(residual, vec_d[3], vec_d[4])
    hidden = jnp.dot(normed_two, w_fc, preferred_element_type=jnp.float32) + b_fc.astype(jnp.float32)
    hidden = jax.nn.gelu(hidden, approximate=True).astype(jnp.bfloat16)
    mlp_out = jnp.dot(hidden, w_proj, preferred_element_type=jnp.float32) + vec_d[5].astype(jnp.float32)
    return (residual.astype(jnp.float32) + mlp_out).astype(jnp.bfloat16).reshape(n_batch, seq_len, d_model)


def stack_forward(hidden_in, layer_ws):
    def scan_body(carry, layer_w):
        return gpt_layer(carry, layer_w), None
    out_h, _ = lax.scan(scan_body, hidden_in, layer_ws)
    return out_h


def copy_pass(x_part, dy_part, layer_ws):
    grad_zero = tuple(jnp.zeros(t.shape, jnp.float32) for t in layer_ws)
    def scan_body(grad_acc, mb_pair):
        x_mb, dy_mb = mb_pair
        y_mb, pull_back = jax.vjp(stack_forward, x_mb, layer_ws)
        dx_mb, dw_mb = pull_back(dy_mb)
        grad_acc = tuple(a + g.astype(jnp.float32) for a, g in zip(grad_acc, dw_mb))
        return grad_acc, (y_mb, dx_mb)
    grad_acc, (y_half, dx_half) = lax.scan(scan_body, grad_zero, (x_part, dy_part))
    return y_half, dx_half, grad_acc


def reference(x_in, dy_out, w_qkv, w_attn, w_fc, w_proj, b_qkv, b_fc, vec_d):
    params = (w_qkv, w_attn, w_fc, w_proj, b_qkv, b_fc, vec_d)
    half_micro = MICRO // 2
    down_ws = tuple(t[:, 0].reshape((LAYERS,) + t.shape[3:]) for t in params)
    up_ws = tuple(t[::-1, 1].reshape((LAYERS,) + t.shape[3:]) for t in params)
    y_down, dx_down, g_down = copy_pass(x_in[:half_micro], dy_out[:half_micro], down_ws)
    y_up, dx_up, g_up = copy_pass(x_in[half_micro:], dy_out[half_micro:], up_ws)
    y_out = jnp.concatenate([y_down, y_up], axis=0)
    dx_in = jnp.concatenate([dx_down, dx_up], axis=0)
    grads = []
    for orig, part_down, part_up in zip(params, g_down, g_up):
        total = (part_down + part_up).reshape((STAGES, LPS) + orig.shape[3:])
        grads.append(jnp.stack([total, total[::-1]], axis=1))
    return (y_out, dx_in, grads[0], grads[1], grads[2], grads[3], grads[4], grads[5], grads[6])
```

```python
import functools

import jax
import jax.numpy as jnp
from jax import lax
from jax.experimental import pallas as pl
from jax.experimental.pallas import tpu as pltpu
from jax.sharding import PartitionSpec as P

EPS = 1e-5
F32 = jnp.float32
BF16 = jnp.bfloat16
LANES = 128
ROWS = 96
CH = 256
SKEW = 3
K0 = 0.7978845608028654
K1 = K0 * 0.044715
VMEM_LIMIT = 67043328
HBM = pl.BlockSpec(memory_space=pl.ANY)


def dot(lhs, rhs, lc=1, rc=0):
    return lax.dot_general(lhs, rhs, (((lc,), (rc,)), ((), ())), preferred_element_type=F32)


def rows_sum(v):
    r, t = v.shape
    return jnp.sum(v.reshape(r // 8, 8, t), axis=0)


def wide(col, t):
    return jnp.concatenate([col] * (t // LANES), axis=1)


def lane_fold(v):
    return functools.reduce(jnp.add, [v[:, k:k + LANES] for k in range(0, v.shape[1], LANES)])


def block_diag(a, b):
    z = jnp.zeros_like(a)
    return jnp.concatenate([jnp.concatenate([a, z], 1), jnp.concatenate([z, b], 1)], 0)


def f_norm(src, gain, shift, dst, stats, row):
    d, t = src.shape
    acc = jnp.zeros((8, t), F32)
    for i in range(0, d, ROWS):
        acc += rows_sum(src[i:i + ROWS, :].astype(F32))
    mean = jnp.sum(acc, axis=0, keepdims=True) * (1.0 / d)
    acc = jnp.zeros((8, t), F32)
    for i in range(0, d, ROWS):
        c = src[i:i + ROWS, :].astype(F32) - mean
        acc += rows_sum(c * c)
    rstd = lax.rsqrt(jnp.sum(acc, axis=0, keepdims=True) * (1.0 / d) + EPS)
    for i in range(0, d, ROWS):
        c = (src[i:i + ROWS, :].astype(F32) - mean) * rstd
        g = wide(gain[i:i + ROWS, :].astype(F32), t)
        s = wide(shift[i:i + ROWS, :].astype(F32), t)
        dst[i:i + ROWS, :] = (c * g + s).astype(BF16)
    stats[row:row + 1, :] = mean
    stats[row + 1:row + 2, :] = rstd


def b_norm(dn, src, gain, skip, dst, stats, row, acc, lane):
    d, t = src.shape
    mean = stats[row:row + 1, :]
    rstd = stats[row + 1:row + 2, :]

    def terms(i):
        c = (src[i:i + ROWS, :].astype(F32) - mean) * rstd
        v = dn[i:i + ROWS, :].astype(F32)
        return c, v, v * wide(gain[i:i + ROWS, :].astype(F32), t)

    def token_sum(v):
        return jnp.sum(lane_fold(v), axis=1, keepdims=True).astype(BF16).astype(F32)

    at = lax.broadcasted_iota(jnp.int32, (ROWS, LANES), 1)
    s1 = jnp.zeros((8, t), F32)
    s2 = jnp.zeros((8, t), F32)
    for i in range(0, d, ROWS):
        c, v, g = terms(i)
        s1 += rows_sum(g)
        s2 += rows_sum(g * c)
        acc[i:i + ROWS, :] += jnp.where(at == lane, token_sum(v * c), jnp.where(at == lane + 1, token_sum(v), 0.0))
    m1 = jnp.sum(s1, axis=0, keepdims=True) * (1.0 / d)
    m2 = jnp.sum(s2, axis=0, keepdims=True) * (1.0 / d)
    for i in range(0, d, ROWS):
        c, _, g = terms(i)
        z = (g - m1 - c * m2) * rstd + skip[i:i + ROWS, :].astype(F32)
        dst[i:i + ROWS, :] = z.astype(BF16)


def skewed(jobs, first, second):
    pending = []
    for job in jobs:
        pending.append((job, first(*job)))
        if len(pending) > SKEW:
            job, v = pending.pop(0)
            second(*job, v)
    for job, v in pending:
        second(*job, v)


def f_heads(t, o, p, heads, seq):
    d, n = o.shape
    head = d // heads
    two = 2 * head
    pairs = heads // 2
    key = lax.broadcasted_iota(jnp.int32, (seq, 2 * seq), 0)
    qry = lax.rem(lax.broadcasted_iota(jnp.int32, (seq, 2 * seq), 1), seq)
    ok = key <= qry
    c = (head ** -0.5) * 1.4426950408889634

    def score(b, j):
        r0, lanes = two * j, slice(b * seq, (b + 1) * seq)
        q = t[r0:r0 + two, lanes]
        return dot(t[d + r0:d + r0 + two, lanes], block_diag(q[:head], q[head:]), 0, 0)

    def mix(b, j, s):
        r0, lanes = two * j, slice(b * seq, (b + 1) * seq)
        s = jnp.where(ok, s, -1e30)
        m = jnp.max(s, axis=0, keepdims=True)
        e = jnp.exp2((s - m) * c)
        e = e * (1.0 / jnp.sum(e, axis=0, keepdims=True))
        k0 = (b * pairs + j) * seq
        p[k0:k0 + seq, :] = e
        x = dot(t[2 * d + r0:2 * d + r0 + two, lanes], e.astype(BF16))
        o[r0:r0 + head, lanes] = x[:head, :seq].astype(BF16)
        o[r0 + head:r0 + two, lanes] = x[head:, seq:].astype(BF16)

    skewed([(b, j) for b in range(n // seq) for j in range(pairs)], score, mix)


def b_heads(t, do, dt, p, heads, seq):
    d, n = do.shape
    head = d // heads
    two = 2 * head
    pairs = heads // 2
    scale = head ** -0.5

    def first(b, j):
        r0, lanes = two * j, slice(b * seq, (b + 1) * seq)
        z = do[r0:r0 + two, lanes]
        return dot(t[2 * d + r0:2 * d + r0 + two, lanes], block_diag(z[:head], z[head:]), 0, 0)

    def diag(r0, lanes, x, k):
        dt[r0:r0 + head, lanes] = (x[:head, :seq] * k).astype(BF16)
        dt[r0 + head:r0 + two, lanes] = (x[head:, seq:] * k).astype(BF16)

    def second(b, j, dp):
        r0, lanes = two * j, slice(b * seq, (b + 1) * seq)
        k0 = (b * pairs + j) * seq
        e = p[k0:k0 + seq, :]
        w = e * dp
        ds = (w - e * jnp.sum(w, axis=0, keepdims=True)).astype(BF16)
        eb = e.astype(BF16)
        diag(r0, lanes, dot(t[d + r0:d + r0 + two, lanes], ds), scale)
        tall = jnp.concatenate([ds[:, :seq], ds[:, seq:]], 0)
        diag(d + r0, lanes, dot(t[r0:r0 + two, lanes], tall, 1, 1), scale)
        tall = jnp.concatenate([eb[:, :seq], eb[:, seq:]], 0)
        diag(2 * d + r0, lanes, dot(do[r0:r0 + two, lanes], tall, 1, 1), 1.0)

    skewed([(b, j) for b in range(n // seq) for j in range(pairs)], first, second)


def gelu_and_slope(x):
    x2 = x * x
    hp = 0.5 * jnp.tanh(x * (x2 * K1 + K0)) + 0.5
    u = x * hp
    return u, hp + (u - u * hp) * (x2 * (6.0 * K1) + 2.0 * K0)


class Group:
    def __init__(self, n):
        self.n, self.half, self.last = n, n // 2, n - 1
        self.me = lax.axis_index('pp')
        self.side = self.me // self.half
        self.depth = self.me + self.side * (self.last - 2 * self.me)
        self.inner = self.me + 1 - 2 * self.side
        self.outer = self.me - 1 + 2 * self.side
        self.lead = self.half + 1 - self.depth - self.depth // 2

    def place(self, i):
        far = lax.rem(i - self.half + self.half // 2, self.half) + self.half
        return jnp.where(i < self.half, i, far)

    def step(self, s):
        q = s - self.lead
        pair = q // 2
        even = (q - 2 * pair) == 0
        rest = self.n - self.lead
        head = s < self.lead
        alt = q < 2 * rest
        second = jnp.logical_and(jnp.logical_not(head), jnp.logical_or(jnp.logical_not(alt), even))
        m = jnp.where(head, s, jnp.where(alt, jnp.where(even, pair, self.lead + pair), q - rest))
        return second.astype(jnp.int32), m


def run_phase(g, c_first, src, final, slots, out, load_sems, recv_sems, send_sems, final_sem, feed_sems, weights, unit,
              begin=None):
    n, half = g.n, g.half
    inside = g.depth == half - 1
    outside = g.depth == 0

    def copies_of(c):
        return [pltpu.make_async_copy(h.at[c], v.at[c], load_sems.at[c, i]) for i, (h, v) in enumerate(weights)]

    for c in (c_first, 1 - c_first):
        for w in copies_of(c):
            w.start()
    barrier = pltpu.get_barrier_semaphore()
    for i in range(n):
        pl.semaphore_signal(barrier, inc=1, device_id={'pp': jnp.int32(i)})
    pl.semaphore_wait(barrier, n)
    if begin is not None:
        begin()

    def remote(a, b, send, recv, dev):
        return pltpu.make_async_remote_copy(src_ref=a, dst_ref=b, send_sem=send, recv_sem=recv, device_id={'pp': dev})

    for k, head in ((0, 0), (1, g.last)):
        spot = g.place(g.me + k * (g.last - 2 * g.me))

        @pl.when(g.me == head)
        def _():
            pltpu.make_async_copy(src, slots.at[0, spot], recv_sems.at[0, spot]).start()

        @pl.when(g.me != head)
        def _():
            remote(src, slots.at[0, spot], feed_sems.at[k], recv_sems.at[0, spot], jnp.int32(head)).start()

    def sent(s):
        sec, m = g.step(s)
        kept = jnp.logical_or(jnp.logical_and(sec == 0, inside),
                              jnp.logical_and(jnp.logical_and(sec == 1, outside), m >= half))
        return jnp.logical_not(kept)

    def settle(s):
        @pl.when(sent(s))
        def _():
            par = lax.rem(s, 2)
            remote(out.at[par], slots.at[0, 0], send_sems.at[par], recv_sems.at[0, 0], g.me).wait_send()

    def body(s, carry):
        sec, m = g.step(s)
        c = jnp.where(sec == 1, 1 - c_first, c_first)
        par = lax.rem(s, 2)

        @pl.when(jnp.logical_or(s == 0, s == g.lead))
        def _():
            for w in copies_of(c):
                w.wait()

        @pl.when(s >= 2)
        def _():
            settle(s - 2)

        @pl.when(jnp.logical_not(jnp.logical_and(sec == 1, inside)))
        def _():
            remote(out.at[par], slots.at[sec, m], send_sems.at[par], recv_sems.at[sec, m], g.me).wait_recv()

        unit(s, c, m, slots.at[sec, m], out.at[par])

        @pl.when(jnp.logical_and(sec == 0, inside))
        def _():
            slots[1, m] = out[par]

        @pl.when(jnp.logical_and(sec == 0, jnp.logical_not(inside)))
        def _():
            remote(out.at[par], slots.at[0, m], send_sems.at[par], recv_sems.at[0, m], g.inner).start()

        @pl.when(jnp.logical_and(sec == 1, jnp.logical_not(outside)))
        def _():
            remote(out.at[par], slots.at[1, m], send_sems.at[par], recv_sems.at[1, m], g.outer).start()

        owner = m + g.side * (g.last - 2 * m)
        done = jnp.logical_and(jnp.logical_and(sec == 1, outside), m < half)

        @pl.when(jnp.logical_and(done, owner == g.me))
        def _():
            pltpu.make_async_copy(out.at[par], final, send_sems.at[par]).start()

        @pl.when(jnp.logical_and(done, owner != g.me))
        def _():
            remote(out.at[par], final, send_sems.at[par], final_sem.at[0], owner).start()

        return carry

    lax.fori_loop(0, 2 * n, body, 0)
    settle(2 * n - 2)
    settle(2 * n - 1)
    for k, head in ((0, 0), (1, g.last)):
        @pl.when(g.me != head)
        def _():
            remote(src, slots.at[0, 0], feed_sems.at[k], recv_sems.at[0, 0], jnp.int32(head)).wait_send()

    @pl.when(jnp.logical_not(outside))
    def _():
        remote(out.at[0], final, send_sems.at[0], final_sem.at[0], g.me).wait_recv()


def forward_kernel(n, heads, seq, src, wq, wo, w1, w2, bq, b1, vec,
                   final, hs, ts, rs, ps, gs, ss, as_, os_, bs, us,
                   vwq, vwo, vw1, vw2, vbq, vb1, vvec, slots, out, a, t, o, r, u, pg, stats,
                   load_sems, recv_sems, send_sems, final_sem, feed_sems, sems):
    g = Group(n)
    d, tok = a.shape
    f = u.shape[0]
    prow = ps.shape[2]

    def unit(s, c, m, x, y):
        def save(i, v, dst):
            cp = pltpu.make_async_copy(v, dst.at[c, m], sems.at[i])
            cp.start()
            return cp

        waits = [save(0, x, hs)]
        f_norm(x, vvec.at[c, 0], vvec.at[c, 1], a, stats, 0)
        cp_a = save(1, a, as_)
        v = a[...]
        for i in range(0, 3 * d, CH):
            t[i:i + CH, :] = (dot(vwq[c, i:i + CH, :], v) + wide(vbq[c, i:i + CH, :].astype(F32), tok)).astype(BF16)
        waits.append(save(2, t, ts))
        f_heads(t, o, pg, heads, seq)
        waits.append(save(3, o, os_))
        cp_p = save(4, pg.at[pl.ds(0, prow), :], ps)
        v = o[...]
        for i in range(0, d, CH):
            z = dot(vwo[c, :, i:i + CH], v, 0, 0) + wide(vvec[c, 2, i:i + CH, :].astype(F32), tok)
            r[i:i + CH, :] = (z + x[i:i + CH, :].astype(F32)).astype(BF16)
        waits.append(save(5, r, rs))
        cp_a.wait()
        f_norm(r, vvec.at[c, 3], vvec.at[c, 4], a, stats, 2)
        waits.append(save(6, a, bs))
        waits.append(save(7, stats, ss))
        cp_p.wait()
        v = a[...]
        for i in range(0, f, CH):
            h = dot(vw1[c, :, i:i + CH], v, 0, 0) + wide(vb1[c, i:i + CH, :].astype(F32), tok)
            uu, slope = gelu_and_slope(h)
            u[i:i + CH, :] = uu.astype(BF16)
            pg[i:i + CH, :] = slope[:, :tok // 2]
            pg[f + i:f + i + CH, :] = slope[:, tok // 2:]
        waits.append(save(8, u, us))
        waits.append(save(9, pg, gs))
        v = u[...]
        for i in range(0, d, CH):
            z = dot(vw2[c, :, i:i + CH], v, 0, 0) + wide(vvec[c, 5, i:i + CH, :].astype(F32), tok)
            y[i:i + CH, :] = (z + r[i:i + CH, :].astype(F32)).astype(BF16)
        for w in waits:
            w.wait()

    weights = [(wq, vwq), (wo, vwo), (w1, vw1), (w2, vw2), (bq, vbq), (b1, vb1), (vec, vvec)]
    run_phase(g, g.side, src, final, slots, out, load_sems, recv_sems, send_sems, final_sem, feed_sems, weights, unit)


def backward_kernel(n, heads, seq, src, wq, wo, w1, w2, vec, hs, ts, rs, ps, gs, ss,
                    final, dys, dgs, drs, dts, sums,
                    vwq, vwo, vw1, vw2, vvec, slots, out, h, t, r, dg, dr, dt, pg, stats, acc,
                    load_sems, recv_sems, send_sems, final_sem, feed_sems, in_sems, sems):
    g = Group(n)
    d, tok = h.shape
    f = dg.shape[0]
    prow = ps.shape[2]
    c_first = 1 - g.side

    def fetch(i, s):
        sec, m = g.step(s)
        c = jnp.where(sec == 1, 1 - c_first, c_first)
        hbm, v = ((gs, pg), (ps, pg.at[pl.ds(0, prow), :]), (ts, t), (rs, r), (hs, h), (ss, stats))[i]
        return pltpu.make_async_copy(hbm.at[c, m], v, in_sems.at[i])

    def ahead(i, s):
        @pl.when(s + 1 < 2 * n)
        def _():
            fetch(i, s + 1).start()

    for i in (0, 2, 3, 4, 5):
        fetch(i, 0).start()
    acc[...] = jnp.zeros_like(acc)

    def unit(s, c, m, dy, y):
        def save(i, v, dst):
            cp = pltpu.make_async_copy(v, dst.at[c, m], sems.at[i])
            cp.start()
            return cp

        waits = [save(0, dy, dys)]
        fetch(0, s).wait()
        v = dy[...]
        for i in range(0, f, CH):
            du = dot(vw2[c, i:i + CH, :], v).astype(BF16).astype(F32)
            dg[i:i + CH, :tok // 2] = (du[:, :tok // 2] * pg[i:i + CH, :]).astype(BF16)
            dg[i:i + CH, tok // 2:] = (du[:, tok // 2:] * pg[f + i:f + i + CH, :]).astype(BF16)
        fetch(1, s).start()
        waits.append(save(1, dg, dgs))
        v = dg[...]
        for i in range(0, d, CH):
            y[i:i + CH, :] = dot(vw1[c, i:i + CH, :], v).astype(BF16)
        fetch(3, s).wait()
        fetch(5, s).wait()
        b_norm(y, r, vvec.at[c, 3], dy, dr, stats, 2, acc.at[c], 2)
        ahead(3, s)
        waits.append(save(2, dr, drs))
        v = dr[...]
        for i in range(0, d, CH):
            y[i:i + CH, :] = dot(vwo[c, i:i + CH, :], v).astype(BF16)
        fetch(1, s).wait()
        fetch(2, s).wait()
        b_heads(t, y, dt, pg, heads, seq)
        ahead(0, s)
        ahead(2, s)
        waits.append(save(3, dt, dts))
        v = dt[...]
        for i in range(0, d, CH):
            y[i:i + CH, :] = dot(vwq[c, :, i:i + CH], v, 0, 0).astype(BF16)
        fetch(4, s).wait()
        b_norm(y, h, vvec.at[c, 0], dr, y, stats, 0, acc.at[c], 0)
        ahead(4, s)
        ahead(5, s)
        for w in waits:
            w.wait()

    weights = [(wq, vwq), (wo, vwo), (w1, vw1), (w2, vw2), (vec, vvec)]
    run_phase(g, c_first, src, final, slots, out, load_sems, recv_sems, send_sems, final_sem, feed_sems, weights, unit)
    cp = pltpu.make_async_copy(acc, sums, sems.at[0])
    cp.start()
    cp.wait()


def run_forward(mesh, heads, seq, xt, weights):
    n = mesh.shape['pp']
    wq, wo, w1, w2, bq, b1, vec = weights
    d, tok = xt.shape
    f = w1.shape[2]
    prow = (tok // seq) * (heads // 2) * seq
    st = jax.ShapeDtypeStruct
    outs = [st((d, tok), BF16)] + [st((2, n) + v, k) for v, k in (
        ((d, tok), BF16), ((3 * d, tok), BF16), ((d, tok), BF16), ((prow, 2 * seq), F32), ((2 * f, tok // 2), F32),
        ((8, tok), F32), ((d, tok), BF16), ((d, tok), BF16), ((d, tok), BF16), ((f, tok), BF16))]
    vm = pltpu.VMEM
    scratch = [vm(w.shape, w.dtype) for w in weights] + [
        vm((2, n, d, tok), BF16), vm((2, d, tok), BF16), vm((d, tok), BF16), vm((3 * d, tok), BF16),
        vm((d, tok), BF16), vm((d, tok), BF16), vm((f, tok), BF16), vm((2 * f, tok // 2), F32), vm((8, tok), F32),
        pltpu.SemaphoreType.DMA((2, 7)), pltpu.SemaphoreType.DMA((2, n)), pltpu.SemaphoreType.DMA((2,)),
        pltpu.SemaphoreType.DMA((1,)), pltpu.SemaphoreType.DMA((2,)), pltpu.SemaphoreType.DMA((10,))]
    return pl.pallas_call(
        functools.partial(forward_kernel, n, heads, seq), out_shape=outs, in_specs=[HBM] * 8, out_specs=[HBM] * 11,
        scratch_shapes=scratch, name='forward_walk',
        compiler_params=pltpu.CompilerParams(vmem_limit_bytes=VMEM_LIMIT, collective_id=0, has_side_effects=True),
    )(xt, *weights)


def run_backward(mesh, heads, seq, dyt, weights, stash):
    n = mesh.shape['pp']
    wq, wo, w1, w2, _, _, vec = weights
    d, tok = dyt.shape
    f = w1.shape[2]
    st = jax.ShapeDtypeStruct
    outs = [st((d, tok), BF16)] + [st((2, n) + v, BF16) for v in ((d, tok), (f, tok), (d, tok), (3 * d, tok))]
    outs += [st((2, d, LANES), F32)]
    vm = pltpu.VMEM
    ws = (wq, wo, w1, w2, vec)
    scratch = [vm(w.shape, w.dtype) for w in ws] + [
        vm((2, n, d, tok), BF16), vm((2, d, tok), BF16), vm((d, tok), BF16), vm((3 * d, tok), BF16),
        vm((d, tok), BF16), vm((f, tok), BF16), vm((d, tok), BF16), vm((3 * d, tok), BF16),
        vm((2 * f, tok // 2), F32), vm((8, tok), F32), vm((2, d, LANES), F32),
        pltpu.SemaphoreType.DMA((2, 5)), pltpu.SemaphoreType.DMA((2, n)), pltpu.SemaphoreType.DMA((2,)),
        pltpu.SemaphoreType.DMA((1,)), pltpu.SemaphoreType.DMA((2,)), pltpu.SemaphoreType.DMA((6,)),
        pltpu.SemaphoreType.DMA((4,))]
    return pl.pallas_call(
        functools.partial(backward_kernel, n, heads, seq), out_shape=outs, in_specs=[HBM] * 12, out_specs=[HBM] * 6,
        scratch_shapes=scratch, name='backward_walk',
        compiler_params=pltpu.CompilerParams(vmem_limit_bytes=VMEM_LIMIT, collective_id=1, has_side_effects=True),
    )(dyt, *ws, *stash)


def weight_kernel(token_rows, lhs, rhs, out, side):
    m = pl.program_id(1)
    rows = out.shape[1]
    two = lhs.shape[1]

    def rounded(k, x):
        return dot(x, rhs[0, k], 1, 1).astype(BF16).astype(F32)

    def go(fresh):
        for i in range(0, rows, CH):
            z = 0.0 if fresh else out[0, i:i + CH, :]
            if i == 0 and token_rows:
                e = 0.0 if fresh else side[0]
                for k in range(two):
                    x = jnp.concatenate([lhs[0, k, i:i + CH, :], jnp.ones((16, lhs.shape[3]), BF16)], 0)
                    v = rounded(k, x)
                    z = z + v[:CH]
                    e = e + v[CH:CH + 8]
                side[0] = e
            else:
                for k in range(two):
                    z = z + rounded(k, lhs[0, k, i:i + CH, :])
            out[0, i:i + CH, :] = z
            if not token_rows:
                e = 0.0 if fresh else side[0, i:i + CH, :]
                for k in range(two):
                    v = lane_fold(lhs[0, k, i:i + CH, :].astype(F32))
                    e = e + jnp.sum(v, axis=1, keepdims=True).astype(BF16).astype(F32)
                side[0, i:i + CH, :] = jnp.broadcast_to(e, (CH, LANES))

    @pl.when(m == 0)
    def _():
        go(True)

    @pl.when(m > 0)
    def _():
        go(False)


def weight_grad(lhs, rhs, token_rows, name):
    c, n, rows, tok = lhs.shape
    cols = rhs.shape[2]
    two = 2
    side = (8, cols) if token_rows else (rows, LANES)
    return pl.pallas_call(
        functools.partial(weight_kernel, token_rows), grid=(c, n // two),
        out_shape=[jax.ShapeDtypeStruct((c, rows, cols), F32), jax.ShapeDtypeStruct((c,) + side, F32)],
        in_specs=[pl.BlockSpec((1, two, rows, tok), lambda i, j: (i, j, 0, 0)),
                  pl.BlockSpec((1, two, cols, tok), lambda i, j: (i, j, 0, 0))],
        out_specs=[pl.BlockSpec((1, rows, cols), lambda i, j: (i, 0, 0)),
                   pl.BlockSpec((1,) + side, lambda i, j: (i, 0, 0))],
        name=name,
        compiler_params=pltpu.CompilerParams(vmem_limit_bytes=VMEM_LIMIT, dimension_semantics=('arbitrary', 'arbitrary')),
    )(lhs, rhs)


def solution(mesh):
    data_spec = P(('dp', 'pp'))
    weight_spec = P('pp')

    def per_device(x, dy, w_qkv, w_attn, w_fc, w_proj, b_qkv, b_fc, vec_d):
        _, batch, seq, d = x.shape
        heads = w_qkv.shape[5]
        tok = batch * seq

        def column(v):
            return jnp.broadcast_to(v[..., None], v.shape + (LANES,))

        weights = (
            w_qkv.reshape(2, d, 3 * d).transpose(0, 2, 1), w_attn.reshape(2, d, d), w_fc[0, :, 0], w_proj[0, :, 0],
            column(b_qkv.reshape(2, 3 * d)), column(b_fc.reshape(2, -1)), column(vec_d[0, :, 0]))
        xt = x.reshape(tok, d).T
        dyt = dy.reshape(tok, d).T
        yt, hs, ts, rs, ps, gs, ss, as_, os_, bs, us = run_forward(mesh, heads, seq, xt, weights)
        dxt, dys, dgs, drs, dts, sums = run_backward(mesh, heads, seq, dyt, weights, (hs, ts, rs, ps, gs, ss))
        gq, gbq = weight_grad(dts, as_, False, 'grad_qkv')
        go, gbo = weight_grad(os_, drs, True, 'grad_attn')
        g1, gb1 = weight_grad(bs, dgs, True, 'grad_fc')
        g2, gb2 = weight_grad(us, dys, True, 'grad_proj')
        s = sums[:, :, :4].transpose(0, 2, 1)
        gv = jnp.stack([s[:, 0], s[:, 1], gbo[:, 0], s[:, 2], s[:, 3], gb2[:, 0]], axis=1)
        back = lambda v: v.T.reshape(x.shape)
        return (back(yt), back(dxt),
                gq.transpose(0, 2, 1).reshape(w_qkv.shape), go.reshape(w_attn.shape), g1.reshape(w_fc.shape),
                g2.reshape(w_proj.shape), gbq[:, :, 0].reshape(b_qkv.shape), gb1[:, 0].reshape(b_fc.shape),
                gv.reshape(vec_d.shape))

    return jax.shard_map(per_device, mesh=mesh, in_specs=(data_spec, data_spec) + (weight_spec,) * 7,
                         out_specs=(data_spec, data_spec) + (data_spec,) * 7, check_vma=False)
```

```python
import functools

import jax
import jax.numpy as jnp
from jax import lax
from jax.experimental import pallas as pl
from jax.experimental.pallas import tpu as pltpu
from jax.sharding import PartitionSpec as P

EPS = 1e-5
F32 = jnp.float32
BF16 = jnp.bfloat16
LANES = 128
ROWS = 96
CH = 256
SKEW = 8
K0 = 0.7978845608028654
K1 = K0 * 0.044715
VMEM_LIMIT = 67043328
HBM = pl.BlockSpec(memory_space=pl.ANY)


def dot(lhs, rhs, lc=1, rc=0):
    return lax.dot_general(lhs, rhs, (((lc,), (rc,)), ((), ())), preferred_element_type=F32)


def rows_sum(v):
    r, t = v.shape
    return jnp.sum(v.reshape(r // 8, 8, t), axis=0)


def column(cols, lane, row, count):
    return cols[row:row + count, lane:lane + 1].astype(F32)


def lane_fold(v):
    return functools.reduce(jnp.add, [v[:, k:k + LANES] for k in range(0, v.shape[1], LANES)])


def token_sum(v):
    return jnp.sum(lane_fold(v), axis=1, keepdims=True).astype(BF16).astype(F32)


def block_diag(a, b):
    z = jnp.zeros_like(a)
    return jnp.concatenate([jnp.concatenate([a, z], 1), jnp.concatenate([z, b], 1)], 0)


def f_norm(src, cols, lane, dst, stats, row):
    d, t = src.shape
    acc = jnp.zeros((8, t), F32)
    for i in range(0, d, ROWS):
        acc += rows_sum(src[i:i + ROWS, :].astype(F32))
    mean = jnp.sum(acc, axis=0, keepdims=True) * (1.0 / d)
    acc = jnp.zeros((8, t), F32)
    for i in range(0, d, ROWS):
        c = src[i:i + ROWS, :].astype(F32) - mean
        acc += rows_sum(c * c)
    rstd = lax.rsqrt(jnp.sum(acc, axis=0, keepdims=True) * (1.0 / d) + EPS)
    for i in range(0, d, ROWS):
        c = (src[i:i + ROWS, :].astype(F32) - mean) * rstd
        dst[i:i + ROWS, :] = (c * column(cols, lane, i, ROWS) + column(cols, lane + 1, i, ROWS)).astype(BF16)
    stats[row:row + 1, :] = mean
    stats[row + 1:row + 2, :] = rstd


def b_norm(dn, src, cols, gain, skip, dst, stats, row, acc, lane):
    d, t = src.shape
    mean = stats[row:row + 1, :]
    rstd = stats[row + 1:row + 2, :]

    def terms(i):
        c = (src[i:i + ROWS, :].astype(F32) - mean) * rstd
        v = dn[i:i + ROWS, :].astype(F32)
        return c, v, v * column(cols, gain, i, ROWS)

    at = lax.broadcasted_iota(jnp.int32, (ROWS, LANES), 1)
    s1 = jnp.zeros((8, t), F32)
    s2 = jnp.zeros((8, t), F32)
    for i in range(0, d, ROWS):
        c, v, g = terms(i)
        s1 += rows_sum(g)
        s2 += rows_sum(g * c)
        acc[i:i + ROWS, :] += jnp.where(at == lane, token_sum(v * c), jnp.where(at == lane + 1, token_sum(v), 0.0))
    m1 = jnp.sum(s1, axis=0, keepdims=True) * (1.0 / d)
    m2 = jnp.sum(s2, axis=0, keepdims=True) * (1.0 / d)
    for i in range(0, d, ROWS):
        c, _, g = terms(i)
        z = (g - m1 - c * m2) * rstd + skip[i:i + ROWS, :].astype(F32)
        dst[i:i + ROWS, :] = z.astype(BF16)


def skewed(jobs, first, second):
    pending = []
    for job in jobs:
        pending.append((job, first(*job)))
        if len(pending) > SKEW:
            job, v = pending.pop(0)
            second(*job, v)
    for job, v in pending:
        second(*job, v)


def f_heads(t, o, p, heads, seq, after):
    d, n = o.shape
    head = d // heads
    two = 2 * head
    pairs = heads // 2
    key = lax.broadcasted_iota(jnp.int32, (seq, 2 * seq), 0)
    qry = lax.rem(lax.broadcasted_iota(jnp.int32, (seq, 2 * seq), 1), seq)
    ok = key <= qry
    c = (head ** -0.5) * 1.4426950408889634

    def score(b, j):
        r0, lanes = two * j, slice(b * seq, (b + 1) * seq)
        q = t[r0:r0 + two, lanes]
        return dot(t[d + r0:d + r0 + two, lanes], block_diag(q[:head], q[head:]), 0, 0)

    def mix(b, j, s):
        r0, lanes = two * j, slice(b * seq, (b + 1) * seq)
        s = jnp.where(ok, s, -1e30)
        m = jnp.max(s, axis=0, keepdims=True)
        e = jnp.exp2((s - m) * c)
        e = e * (1.0 / jnp.sum(e, axis=0, keepdims=True))
        k0 = (b * pairs + j) * seq
        p[k0:k0 + seq, :] = e
        x = dot(t[2 * d + r0:2 * d + r0 + two, lanes], e.astype(BF16))
        o[r0:r0 + head, lanes] = x[:head, :seq].astype(BF16)
        o[r0 + head:r0 + two, lanes] = x[head:, seq:].astype(BF16)
        if j == pairs - 1:
            after(b)

    skewed([(b, j) for b in range(n // seq) for j in range(pairs)], score, mix)


def b_heads(t, do, dt, p, heads, seq, after):
    d, n = do.shape
    head = d // heads
    two = 2 * head
    pairs = heads // 2
    scale = head ** -0.5

    def first(b, j):
        r0, lanes = two * j, slice(b * seq, (b + 1) * seq)
        z = do[r0:r0 + two, lanes]
        return dot(t[2 * d + r0:2 * d + r0 + two, lanes], block_diag(z[:head], z[head:]), 0, 0)

    def diag(r0, lanes, x, k):
        dt[r0:r0 + head, lanes] = (x[:head, :seq] * k).astype(BF16)
        dt[r0 + head:r0 + two, lanes] = (x[head:, seq:] * k).astype(BF16)

    def second(b, j, dp):
        r0, lanes = two * j, slice(b * seq, (b + 1) * seq)
        k0 = (b * pairs + j) * seq
        e = p[k0:k0 + seq, :]
        w = e * dp
        ds = (w - e * jnp.sum(w, axis=0, keepdims=True)).astype(BF16)
        eb = e.astype(BF16)
        diag(r0, lanes, dot(t[d + r0:d + r0 + two, lanes], ds), scale)
        tall = jnp.concatenate([ds[:, :seq], ds[:, seq:]], 0)
        diag(d + r0, lanes, dot(t[r0:r0 + two, lanes], tall, 1, 1), scale)
        tall = jnp.concatenate([eb[:, :seq], eb[:, seq:]], 0)
        diag(2 * d + r0, lanes, dot(do[r0:r0 + two, lanes], tall, 1, 1), 1.0)
        if j == pairs - 1:
            after(b)

    skewed([(b, j) for b in range(n // seq) for j in range(pairs)], first, second)


def gelu_and_slope(x):
    x2 = x * x
    hp = 0.5 * jnp.tanh(x * (x2 * K1 + K0)) + 0.5
    u = x * hp
    return u, hp + (u - u * hp) * (x2 * (6.0 * K1) + 2.0 * K0)


class Group:
    def __init__(self, n):
        self.n, self.half, self.last = n, n // 2, n - 1
        self.me = lax.axis_index('pp')
        self.side = self.me // self.half
        self.depth = self.me + self.side * (self.last - 2 * self.me)
        self.inner = self.me + 1 - 2 * self.side
        self.outer = self.me - 1 + 2 * self.side
        self.lead = self.half + 1 - self.depth - self.depth // 2

    def place(self, i):
        far = lax.rem(i - self.half + self.half // 2, self.half) + self.half
        return jnp.where(i < self.half, i, far)

    def step(self, s):
        q = s - self.lead
        pair = q // 2
        even = (q - 2 * pair) == 0
        rest = self.n - self.lead
        head = s < self.lead
        alt = q < 2 * rest
        second = jnp.logical_and(jnp.logical_not(head), jnp.logical_or(jnp.logical_not(alt), even))
        m = jnp.where(head, s, jnp.where(alt, jnp.where(even, pair, self.lead + pair), q - rest))
        return second.astype(jnp.int32), m


def run_phase(g, c_first, src, final, slots, out, load_sems, recv_sems, send_sems, final_sem, feed_sems, weights, unit,
              begin=None):
    n, half = g.n, g.half
    inside = g.depth == half - 1
    outside = g.depth == 0

    def copies_of(c):
        return [pltpu.make_async_copy(h.at[c], v.at[c], load_sems.at[c, i]) for i, (h, v) in enumerate(weights)]

    for c in (c_first, 1 - c_first):
        for w in copies_of(c):
            w.start()
    barrier = pltpu.get_barrier_semaphore()
    for i in range(n):
        pl.semaphore_signal(barrier, inc=1, device_id={'pp': jnp.int32(i)})
    pl.semaphore_wait(barrier, n)
    if begin is not None:
        begin()

    def remote(a, b, send, recv, dev):
        return pltpu.make_async_remote_copy(src_ref=a, dst_ref=b, send_sem=send, recv_sem=recv, device_id={'pp': dev})

    for k, head in ((0, 0), (1, g.last)):
        spot = g.place(g.me + k * (g.last - 2 * g.me))

        @pl.when(g.me == head)
        def _():
            pltpu.make_async_copy(src, slots.at[0, spot], recv_sems.at[0, spot]).start()

        @pl.when(g.me != head)
        def _():
            remote(src, slots.at[0, spot], feed_sems.at[k], recv_sems.at[0, spot], jnp.int32(head)).start()

    def sent(s):
        sec, m = g.step(s)
        kept = jnp.logical_or(jnp.logical_and(sec == 0, inside),
                              jnp.logical_and(jnp.logical_and(sec == 1, outside), m >= half))
        return jnp.logical_not(kept)

    def settle(s):
        @pl.when(sent(s))
        def _():
            par = lax.rem(s, 2)
            remote(out.at[par], slots.at[0, 0], send_sems.at[par], recv_sems.at[0, 0], g.me).wait_send()

    def body(s, carry):
        sec, m = g.step(s)
        c = jnp.where(sec == 1, 1 - c_first, c_first)
        par = lax.rem(s, 2)

        @pl.when(jnp.logical_or(s == 0, s == g.lead))
        def _():
            for w in copies_of(c):
                w.wait()

        @pl.when(s >= 2)
        def _():
            settle(s - 2)

        @pl.when(jnp.logical_not(jnp.logical_and(sec == 1, inside)))
        def _():
            remote(out.at[par], slots.at[sec, m], send_sems.at[par], recv_sems.at[sec, m], g.me).wait_recv()

        unit(s, c, m, slots.at[sec, m], out.at[par])

        @pl.when(jnp.logical_and(sec == 0, inside))
        def _():
            slots[1, m] = out[par]

        @pl.when(jnp.logical_and(sec == 0, jnp.logical_not(inside)))
        def _():
            remote(out.at[par], slots.at[0, m], send_sems.at[par], recv_sems.at[0, m], g.inner).start()

        @pl.when(jnp.logical_and(sec == 1, jnp.logical_not(outside)))
        def _():
            remote(out.at[par], slots.at[1, m], send_sems.at[par], recv_sems.at[1, m], g.outer).start()

        owner = m + g.side * (g.last - 2 * m)
        done = jnp.logical_and(jnp.logical_and(sec == 1, outside), m < half)

        @pl.when(jnp.logical_and(done, owner == g.me))
        def _():
            pltpu.make_async_copy(out.at[par], final, send_sems.at[par]).start()

        @pl.when(jnp.logical_and(done, owner != g.me))
        def _():
            remote(out.at[par], final, send_sems.at[par], final_sem.at[0], owner).start()

        return carry

    lax.fori_loop(0, 2 * n, body, 0)
    settle(2 * n - 2)
    settle(2 * n - 1)
    for k, head in ((0, 0), (1, g.last)):
        @pl.when(g.me != head)
        def _():
            remote(src, slots.at[0, 0], feed_sems.at[k], recv_sems.at[0, 0], jnp.int32(head)).wait_send()

    @pl.when(jnp.logical_not(outside))
    def _():
        remote(out.at[0], final, send_sems.at[0], final_sem.at[0], g.me).wait_recv()


def forward_kernel(n, heads, seq, src, wq, wo, w1, w2, cols,
                   final, hs, ts, rs, ps, gs, ss, as_, os_, bs, us,
                   vwq, vwo, vw1, vw2, vcols, slots, out, a, t, o, r, u, pg, ya, stats,
                   load_sems, recv_sems, send_sems, final_sem, feed_sems, sems):
    g = Group(n)
    d, tok = a.shape
    f = u.shape[0]
    half = tok // 2
    part = ps.shape[2] // (tok // seq)

    def unit(s, c, m, x, y):
        def copy(i, v, dst, at=None):
            hbm = dst.at[c, m]
            if at is not None:
                v, hbm = v.at[pl.ds(*at), :], hbm.at[pl.ds(*at), :]
            return pltpu.make_async_copy(v, hbm, sems.at[i])

        cv = vcols.at[c]
        copy(0, x, hs).start()
        f_norm(x, cv, 0, a, stats, 0)
        copy(1, a, as_).start()
        v = a[...]
        for i in range(0, 3 * d, CH):
            z = dot(vwq[c, i:i + CH, :], v) + column(cv, 6 + i // d, i % d, CH)
            t[i:i + CH, :] = z.astype(BF16)
        copy(2, t, ts).start()
        f_heads(t, o, pg, heads, seq, lambda b: copy(4, pg, ps, (b * part, part)).start())
        copy(3, o, os_).start()
        v = o[...]
        for i in range(0, d, CH):
            z = dot(vwo[c, :, i:i + CH], v, 0, 0) + column(cv, 2, i, CH) + x[i:i + CH, :].astype(F32)
            r[i:i + CH, :] = z.astype(BF16)
        copy(5, r, rs).start()
        copy(1, a, as_).wait()
        f_norm(r, cv, 3, a, stats, 2)
        copy(6, a, bs).start()
        copy(7, stats, ss).start()
        copy(4, pg.at[pl.ds(0, ps.shape[2]), :], ps).wait()
        v = a[...]

        def up(k):
            for i in range(k * d, (k + 1) * d, CH):
                h = dot(vw1[c, :, i:i + CH], v, 0, 0) + column(cv, 9 + k, i % d, CH)
                uu, slope = gelu_and_slope(h)
                u[i:i + CH, :] = uu.astype(BF16)
                pg[2 * i:2 * i + CH, :] = slope[:, :half]
                pg[2 * i + CH:2 * i + 2 * CH, :] = slope[:, half:]
                copy(8, u, us, (i, CH)).start()
                copy(9, pg, gs, (2 * i, 2 * CH)).start()

        def down(k):
            w = u[k * d:(k + 1) * d, :]
            for i in range(0, d, CH):
                z = dot(vw2[c, k * d:(k + 1) * d, i:i + CH], w, 0, 0)
                z += (column(cv, 5, i, CH) + r[i:i + CH, :].astype(F32)) if k == 0 else ya[i:i + CH, :]
                if (k + 1) * d < f:
                    ya[i:i + CH, :] = z
                else:
                    y[i:i + CH, :] = z.astype(BF16)

        up(0)
        for k in range(1, f // d):
            up(k)
            down(k - 1)
        down(f // d - 1)
        for i, v, dst in ((0, x, hs), (2, t, ts), (3, o, os_), (5, r, rs), (6, a, bs), (7, stats, ss), (8, u, us),
                          (9, pg, gs)):
            copy(i, v, dst).wait()

    weights = [(wq, vwq), (wo, vwo), (w1, vw1), (w2, vw2), (cols, vcols)]
    run_phase(g, g.side, src, final, slots, out, load_sems, recv_sems, send_sems, final_sem, feed_sems, weights, unit)


def backward_kernel(n, heads, seq, src, wq, wo, w1, w2, cols, hs, ts, rs, ps, gs, ss,
                    final, dys, dgs, drs, dts, sums,
                    vwq, vwo, vw1, vw2, vcols, slots, out, h, t, r, dg, dr, dt, pg, stats, acc,
                    load_sems, recv_sems, send_sems, final_sem, feed_sems, in_sems, sems):
    g = Group(n)
    d, tok = h.shape
    f = dg.shape[0]
    half = tok // 2
    prow = ps.shape[2]
    part = prow // (tok // seq)
    c_first = 1 - g.side

    def fetch(i, s, at=None):
        sec, m = g.step(s)
        c = jnp.where(sec == 1, 1 - c_first, c_first)
        hbm, v = ((gs, pg), (ps, pg.at[pl.ds(0, prow), :]), (ts, t), (rs, r), (hs, h), (ss, stats))[i]
        hbm = hbm.at[c, m]
        if at is not None:
            hbm, v = hbm.at[pl.ds(*at), :], v.at[pl.ds(*at), :]
        return pltpu.make_async_copy(hbm, v, in_sems.at[i])

    def ahead(i, s, at=None):
        @pl.when(s + 1 < 2 * n)
        def _():
            fetch(i, s + 1, at).start()

    for i in (0, 2, 3, 4, 5):
        fetch(i, 0).start()
    acc[...] = jnp.zeros_like(acc)

    def unit(s, c, m, dy, y):
        def copy(i, v, dst, at=None):
            hbm = dst.at[c, m]
            if at is not None:
                v, hbm = v.at[pl.ds(*at), :], hbm.at[pl.ds(*at), :]
            return pltpu.make_async_copy(v, hbm, sems.at[i])

        cv = vcols.at[c]
        copy(0, dy, dys).start()
        fetch(0, s).wait()
        v = dy[...]
        for i in range(0, f, CH):
            du = dot(vw2[c, i:i + CH, :], v).astype(BF16).astype(F32)
            dg[i:i + CH, :half] = (du[:, :half] * pg[2 * i:2 * i + CH, :]).astype(BF16)
            dg[i:i + CH, half:] = (du[:, half:] * pg[2 * i + CH:2 * i + 2 * CH, :]).astype(BF16)
        fetch(1, s).start()
        ahead(0, s, (prow, 2 * f - prow))
        copy(1, dg, dgs).start()
        v = dg[...]
        for i in range(0, d, CH):
            y[i:i + CH, :] = dot(vw1[c, i:i + CH, :], v).astype(BF16)
        fetch(3, s).wait()
        fetch(5, s).wait()
        b_norm(y, r, cv, 3, dy, dr, stats, 2, acc.at[c], 2)
        ahead(3, s)
        copy(2, dr, drs).start()
        v = dr[...]
        for i in range(0, d, CH):
            y[i:i + CH, :] = dot(vwo[c, i:i + CH, :], v).astype(BF16)
        fetch(1, s).wait()
        fetch(2, s).wait()
        b_heads(t, y, dt, pg, heads, seq, lambda b: ahead(0, s, (b * part, part)))
        ahead(2, s)
        copy(3, dt, dts).start()
        v = dt[...]
        at = lax.broadcasted_iota(jnp.int32, (ROWS, LANES), 1)
        for i in range(0, d, CH):
            y[i:i + CH, :] = dot(vwq[c, :, i:i + CH], v, 0, 0).astype(BF16)
        for i in range(0, d, ROWS):
            e = 0.0
            for k in range(3):
                e = jnp.where(at == 4 + k, token_sum(dt[k * d + i:k * d + i + ROWS, :].astype(F32)), e)
            acc[c, i:i + ROWS, :] += e
        fetch(4, s).wait()
        b_norm(y, h, cv, 0, dr, y, stats, 0, acc.at[c], 0)
        ahead(4, s)
        ahead(5, s)
        for i, v, dst in ((0, dy, dys), (1, dg, dgs), (2, dr, drs), (3, dt, dts)):
            copy(i, v, dst).wait()

    weights = [(wq, vwq), (wo, vwo), (w1, vw1), (w2, vw2), (cols, vcols)]
    run_phase(g, c_first, src, final, slots, out, load_sems, recv_sems, send_sems, final_sem, feed_sems, weights, unit)
    cp = pltpu.make_async_copy(acc, sums, sems.at[0])
    cp.start()
    cp.wait()


def run_forward(mesh, heads, seq, xt, weights):
    n = mesh.shape['pp']
    d, tok = xt.shape
    f = weights[2].shape[2]
    prow = (tok // seq) * (heads // 2) * seq
    st = jax.ShapeDtypeStruct
    outs = [st((d, tok), BF16)] + [st((2, n) + v, k) for v, k in (
        ((d, tok), BF16), ((3 * d, tok), BF16), ((d, tok), BF16), ((prow, 2 * seq), F32), ((2 * f, tok // 2), F32),
        ((8, tok), F32), ((d, tok), BF16), ((d, tok), BF16), ((d, tok), BF16), ((f, tok), BF16))]
    vm = pltpu.VMEM
    scratch = [vm(w.shape, w.dtype) for w in weights] + [
        vm((2, n, d, tok), BF16), vm((2, d, tok), BF16), vm((d, tok), BF16), vm((3 * d, tok), BF16),
        vm((d, tok), BF16), vm((d, tok), BF16), vm((f, tok), BF16), vm((2 * f, tok // 2), F32), vm((d, tok), F32),
        vm((8, tok), F32),
        pltpu.SemaphoreType.DMA((2, 5)), pltpu.SemaphoreType.DMA((2, n)), pltpu.SemaphoreType.DMA((2,)),
        pltpu.SemaphoreType.DMA((1,)), pltpu.SemaphoreType.DMA((2,)), pltpu.SemaphoreType.DMA((10,))]
    return pl.pallas_call(
        functools.partial(forward_kernel, n, heads, seq), out_shape=outs, in_specs=[HBM] * 6, out_specs=[HBM] * 11,
        scratch_shapes=scratch, name='forward_walk',
        compiler_params=pltpu.CompilerParams(vmem_limit_bytes=VMEM_LIMIT, collective_id=0, has_side_effects=True),
    )(xt, *weights)


def run_backward(mesh, heads, seq, dyt, weights, stash):
    n = mesh.shape['pp']
    d, tok = dyt.shape
    f = weights[2].shape[2]
    st = jax.ShapeDtypeStruct
    outs = [st((d, tok), BF16)] + [st((2, n) + v, BF16) for v in ((d, tok), (f, tok), (d, tok), (3 * d, tok))]
    outs += [st((2, d, LANES), F32)]
    vm = pltpu.VMEM
    scratch = [vm(w.shape, w.dtype) for w in weights] + [
        vm((2, n, d, tok), BF16), vm((2, d, tok), BF16), vm((d, tok), BF16), vm((3 * d, tok), BF16),
        vm((d, tok), BF16), vm((f, tok), BF16), vm((d, tok), BF16), vm((3 * d, tok), BF16),
        vm((2 * f, tok // 2), F32), vm((8, tok), F32), vm((2, d, LANES), F32),
        pltpu.SemaphoreType.DMA((2, 5)), pltpu.SemaphoreType.DMA((2, n)), pltpu.SemaphoreType.DMA((2,)),
        pltpu.SemaphoreType.DMA((1,)), pltpu.SemaphoreType.DMA((2,)), pltpu.SemaphoreType.DMA((6,)),
        pltpu.SemaphoreType.DMA((4,))]
    return pl.pallas_call(
        functools.partial(backward_kernel, n, heads, seq), out_shape=outs, in_specs=[HBM] * 12, out_specs=[HBM] * 6,
        scratch_shapes=scratch, name='backward_walk',
        compiler_params=pltpu.CompilerParams(vmem_limit_bytes=VMEM_LIMIT, collective_id=1, has_side_effects=True),
    )(dyt, *weights, *stash)


PAIR = 2


def grads_kernel(n, *refs):
    ins, refs = refs[:8], refs[8:]
    outs, bias_outs, refs = refs[:4], refs[4:7], refs[7:]
    accs, biases, (buf, in_sems, out_sems) = refs[:4], refs[4:7], refs[7:]
    steps = n // PAIR
    tok = buf.shape[3]

    def fetches(c, k, j):
        slot = lax.rem(j, 2)
        rows, cols = ins[2 * k].shape[2], ins[2 * k + 1].shape[2]
        at = pl.ds(j * PAIR, PAIR)
        return (pltpu.make_async_copy(ins[2 * k].at[c, at], buf.at[slot, :, pl.ds(0, rows), :], in_sems.at[slot, 0]),
                pltpu.make_async_copy(ins[2 * k + 1].at[c, at], buf.at[slot, :, pl.ds(rows, cols), :], in_sems.at[slot, 1]))

    def begin(c, k, j):
        for cp in fetches(c, k, j):
            cp.start()

    def results(c, k):
        cps = [pltpu.make_async_copy(accs[k], outs[k].at[c], out_sems.at[k])]
        if k < 3:
            cps.append(pltpu.make_async_copy(biases[k], bias_outs[k].at[c], out_sems.at[4 + k]))
        return cps

    begin(jnp.int32(0), 0, jnp.int32(0))

    def stage(c, carry):
        for k in range(4):
            rows, cols = ins[2 * k].shape[2], ins[2 * k + 1].shape[2]

            def step(j, carry, k=k, rows=rows, cols=cols):
                @pl.when(j + 1 < steps)
                def _():
                    begin(c, k, j + 1)

                @pl.when(j + 1 == steps)
                def _():
                    if k < 3:
                        begin(c, k + 1, jnp.int32(0))
                    else:
                        @pl.when(c == 0)
                        def _():
                            begin(jnp.int32(1), 0, jnp.int32(0))

                @pl.when(jnp.logical_and(j == 0, c == 1))
                def _():
                    for cp in results(jnp.int32(0), k):
                        cp.wait()

                for cp in fetches(c, k, j):
                    cp.wait()
                slot = lax.rem(j, 2)
                later = j > 0
                for i in range(0, rows, CH):
                    z = jnp.where(later, accs[k][i:i + CH, :], 0.0)
                    if i == 0 and k < 3:
                        e = jnp.where(later, biases[k][...], 0.0)
                    for q in range(PAIR):
                        x = buf[slot, q, i:i + CH, :]
                        if i == 0 and k < 3:
                            x = jnp.concatenate([x, jnp.ones((16, tok), BF16)], 0)
                        v = dot(x, buf[slot, q, rows:rows + cols, :], 1, 1).astype(BF16).astype(F32)
                        z = z + v[:CH]
                        if i == 0 and k < 3:
                            e = e + v[CH:CH + 8]
                    accs[k][i:i + CH, :] = z
                    if i == 0 and k < 3:
                        biases[k][...] = e
                return carry

            lax.fori_loop(0, steps, step, 0)
            for cp in results(c, k):
                cp.start()
        return carry

    lax.fori_loop(0, 2, stage, 0)
    for k in range(4):
        for cp in results(jnp.int32(1), k):
            cp.wait()


def run_grads(pairs):
    n, tok = pairs[0][0].shape[1], pairs[0][0].shape[3]
    sizes = [(a.shape[2], b.shape[2]) for a, b in pairs]
    st = jax.ShapeDtypeStruct
    vm = pltpu.VMEM
    most = max(a + b for a, b in sizes)
    return pl.pallas_call(
        functools.partial(grads_kernel, n),
        out_shape=[st((2,) + v, F32) for v in sizes] + [st((2, 8, v[1]), F32) for v in sizes[:3]],
        in_specs=[HBM] * 8, out_specs=[HBM] * 7,
        scratch_shapes=[vm(v, F32) for v in sizes] + [vm((8, v[1]), F32) for v in sizes[:3]] + [
            vm((2, PAIR, most, tok), BF16), pltpu.SemaphoreType.DMA((2, 2)), pltpu.SemaphoreType.DMA((7,))],
        name='weight_grads', compiler_params=pltpu.CompilerParams(vmem_limit_bytes=VMEM_LIMIT),
    )(*[v for p in pairs for v in p])


def solution(mesh):
    data_spec = P(('dp', 'pp'))
    weight_spec = P('pp')

    def per_device(x, dy, w_qkv, w_attn, w_fc, w_proj, b_qkv, b_fc, vec_d):
        _, batch, seq, d = x.shape
        heads = w_qkv.shape[5]
        tok = batch * seq

        cols = jnp.concatenate([vec_d[0, :, 0], b_qkv.reshape(2, 3, d), b_fc.reshape(2, -1, d)], axis=1)
        cols = jnp.pad(cols.transpose(0, 2, 1), ((0, 0), (0, 0), (0, LANES - cols.shape[1])))
        weights = (w_qkv.reshape(2, d, 3 * d).transpose(0, 2, 1), w_attn.reshape(2, d, d), w_fc[0, :, 0], w_proj[0, :, 0],
                   cols)
        xt = x.reshape(tok, d).T
        dyt = dy.reshape(tok, d).T
        yt, hs, ts, rs, ps, gs, ss, as_, os_, bs, us = run_forward(mesh, heads, seq, xt, weights)
        dxt, dys, dgs, drs, dts, sums = run_backward(mesh, heads, seq, dyt, weights, (hs, ts, rs, ps, gs, ss))
        g1, g2, go, gq, gb1, gb2, gbo = run_grads(((bs, dgs), (us, dys), (os_, drs), (dts, as_)))
        s = sums[:, :, :7].transpose(0, 2, 1)
        gv = jnp.stack([s[:, 0], s[:, 1], gbo[:, 0], s[:, 2], s[:, 3], gb2[:, 0]], axis=1)
        back = lambda v: v.T.reshape(x.shape)
        return (back(yt), back(dxt),
                gq.transpose(0, 2, 1).reshape(w_qkv.shape), go.reshape(w_attn.shape), g1.reshape(w_fc.shape),
                g2.reshape(w_proj.shape), s[:, 4:7].reshape(b_qkv.shape), gb1[:, 0].reshape(b_fc.shape),
                gv.reshape(vec_d.shape))

    return jax.shard_map(per_device, mesh=mesh, in_specs=(data_spec, data_spec) + (weight_spec,) * 7,
                         out_specs=(data_spec, data_spec) + (data_spec,) * 7, check_vma=False)
```

```python
import functools

import jax
import jax.numpy as jnp
from jax import lax
from jax.experimental import pallas as pl
from jax.experimental.pallas import tpu as pltpu
from jax.sharding import PartitionSpec as P

EPS = 1e-5
F32 = jnp.float32
BF16 = jnp.bfloat16
LANES = 128
ROWS = 32
CH = 256
WIDE = 512
SKEW = 8
K0 = 0.7978845608028654
K1 = K0 * 0.044715
VMEM_LIMIT = 67043328
HBM = pl.BlockSpec(memory_space=pl.ANY)


def dot(lhs, rhs, lc=1, rc=0):
    return lax.dot_general(lhs, rhs, (((lc,), (rc,)), ((), ())), preferred_element_type=F32)


def rows_sum(v):
    r, t = v.shape
    return jnp.sum(v.reshape(r // 8, 8, t), axis=0)


def rounded(v):
    return v.astype(BF16).astype(F32)


def lane_fold(v):
    return functools.reduce(jnp.add, [v[:, k:k + LANES] for k in range(0, v.shape[1], LANES)])


def block_diag(a, b):
    z = jnp.zeros_like(a)
    return jnp.concatenate([jnp.concatenate([a, z], 1), jnp.concatenate([z, b], 1)], 0)


def f_norm(src, gain, shift, dst, stats, lo, hi):
    d = src.shape[1]
    at = lax.broadcasted_iota(jnp.int32, (ROWS, LANES), 1)
    for i in range(lo, hi, ROWS):
        x = src[i:i + ROWS, :].astype(F32)
        mean = jnp.sum(x, axis=1, keepdims=True) * (1.0 / d)
        x = x - mean
        rstd = lax.rsqrt(jnp.sum(x * x, axis=1, keepdims=True) * (1.0 / d) + EPS)
        dst[i:i + ROWS, :] = (x * rstd * gain + shift).astype(BF16)
        stats[i:i + ROWS, :] = jnp.where(at == 0, mean, rstd)


def b_norm(dn, src, gain, skip, dst, stats, lo, hi):
    d = src.shape[1]
    pg = pb = pr = jnp.zeros((8, d), F32)
    for i in range(lo, hi, ROWS):
        mean, rstd = stats[i:i + ROWS, 0:1], stats[i:i + ROWS, 1:2]
        c = (src[i:i + ROWS, :].astype(F32) - mean) * rstd
        v = dn(i, i + ROWS)
        pg += rows_sum(v * c)
        pb += rows_sum(v)
        g = v * gain
        m1 = jnp.sum(g, axis=1, keepdims=True) * (1.0 / d)
        m2 = jnp.sum(g * c, axis=1, keepdims=True) * (1.0 / d)
        z = ((g - m1 - c * m2) * rstd + skip[i:i + ROWS, :].astype(F32)).astype(BF16)
        dst[i:i + ROWS, :] = z
        pr += rows_sum(z.astype(F32))
    return pg, pb, pr


def skewed(jobs, first, second):
    pending = []

    def one(job):
        if job is not None:
            pending.append((job, first(*job)))
        if job is None or len(pending) > SKEW:
            j, v = pending.pop(0)
            second(*j, v)

    return [functools.partial(one, job) for job in jobs + [None] * min(SKEW, len(jobs))]


def f_heads(t, o, p, heads, seq, seqs, after):
    d = o.shape[0]
    head = d // heads
    two = 2 * head
    pairs = heads // 2
    c = (head ** -0.5) * 1.4426950408889634

    def score(b, j):
        r0, lanes = two * j, slice(b * seq, (b + 1) * seq)
        q = t[r0:r0 + two, lanes]
        return dot(t[d + r0:d + r0 + two, lanes], block_diag(q[:head], q[head:]), 0, 0)

    def mix(b, j, s):
        r0, lanes = two * j, slice(b * seq, (b + 1) * seq)
        key = lax.broadcasted_iota(jnp.int32, (seq, 2 * seq), 0)
        qry = lax.rem(lax.broadcasted_iota(jnp.int32, (seq, 2 * seq), 1), seq)
        s = jnp.where(key <= qry, s, -1e30)
        m = jnp.max(s, axis=0, keepdims=True)
        e = jnp.exp2((s - m) * c)
        e = e * (1.0 / jnp.sum(e, axis=0, keepdims=True))
        p[b * seq:(b + 1) * seq, 2 * seq * j:2 * seq * (j + 1)] = e
        x = dot(t[2 * d + r0:2 * d + r0 + two, lanes], e.astype(BF16))
        o[r0:r0 + head, lanes] = x[:head, :seq].astype(BF16)
        o[r0 + head:r0 + two, lanes] = x[head:, seq:].astype(BF16)
        if j == pairs - 1:
            after(b)

    return skewed([(b, j) for b in seqs for j in range(pairs)], score, mix)


def b_heads(t, do, p, heads, seq, seqs, after):
    d = do.shape[0]
    head = d // heads
    two = 2 * head
    pairs = heads // 2
    scale = head ** -0.5

    def first(b, j):
        r0, lanes = two * j, slice(b * seq, (b + 1) * seq)
        z = do[r0:r0 + two, lanes]
        return dot(t[2 * d + r0:2 * d + r0 + two, lanes], block_diag(z[:head], z[head:]), 0, 0)

    def diag(r0, lanes, x, k):
        t[r0:r0 + head, lanes] = (x[:head, :seq] * k).astype(BF16)
        t[r0 + head:r0 + two, lanes] = (x[head:, seq:] * k).astype(BF16)

    def second(b, j, dp):
        r0, lanes = two * j, slice(b * seq, (b + 1) * seq)
        e = p[b * seq:(b + 1) * seq, 2 * seq * j:2 * seq * (j + 1)]
        w = e * dp
        ds = (w - e * jnp.sum(w, axis=0, keepdims=True)).astype(BF16)
        eb = e.astype(BF16)
        q, k = t[r0:r0 + two, lanes], t[d + r0:d + r0 + two, lanes]
        tall = jnp.concatenate([ds[:, :seq], ds[:, seq:]], 0)
        dq, dk = dot(k, ds), dot(q, tall, 1, 1)
        tall = jnp.concatenate([eb[:, :seq], eb[:, seq:]], 0)
        dv = dot(do[r0:r0 + two, lanes], tall, 1, 1)
        diag(r0, lanes, dq, scale)
        diag(d + r0, lanes, dk, scale)
        diag(2 * d + r0, lanes, dv, 1.0)
        if j == pairs - 1:
            after(b)

    return skewed([(b, j) for b in seqs for j in range(pairs)], first, second)


def gelu_and_slope(x):
    x2 = x * x
    hp = 0.5 * jnp.tanh(x * (x2 * K1 + K0)) + 0.5
    u = x * hp
    return u, hp + (u - u * hp) * (x2 * (6.0 * K1) + 2.0 * K0)


def woven(*lists):
    total = max(len(v) for v in lists)
    done = [0] * len(lists)
    for k in range(total):
        for i, v in enumerate(lists):
            while done[i] * total < (k + 1) * len(v) and done[i] < len(v):
                v[done[i]]()
                done[i] += 1


class Group:
    def __init__(self, n):
        self.n, self.half, self.last = n, n // 2, n - 1
        self.me = lax.axis_index('pp')
        self.side = self.me // self.half
        self.depth = self.me + self.side * (self.last - 2 * self.me)
        self.inner = self.me + 1 - 2 * self.side
        self.outer = self.me - 1 + 2 * self.side
        self.lead = self.half + 1 - self.depth - self.depth // 2

    def place(self, i):
        far = lax.rem(i - self.half + self.half // 2, self.half) + self.half
        return jnp.where(i < self.half, i, far)

    def step(self, s):
        q = s - self.lead
        pair = q // 2
        even = (q - 2 * pair) == 0
        rest = self.n - self.lead
        head = s < self.lead
        alt = q < 2 * rest
        second = jnp.logical_and(jnp.logical_not(head), jnp.logical_or(jnp.logical_not(alt), even))
        m = jnp.where(head, s, jnp.where(alt, jnp.where(even, pair, self.lead + pair), q - rest))
        return second.astype(jnp.int32), m


def run_phase(g, c_first, src, final, slots, out, load_sems, recv_sems, send_sems, final_sem, feed_sems, weights, unit,
              begin=None):
    n, half = g.n, g.half
    inside = g.depth == half - 1
    outside = g.depth == 0

    def copies_of(c):
        return [pltpu.make_async_copy(h.at[c], v.at[c], load_sems.at[c, i]) for i, (h, v) in enumerate(weights)]

    for c in (c_first, 1 - c_first):
        for w in copies_of(c):
            w.start()
    barrier = pltpu.get_barrier_semaphore()
    for i in range(n):
        pl.semaphore_signal(barrier, inc=1, device_id={'pp': jnp.int32(i)})
    pl.semaphore_wait(barrier, n)
    if begin is not None:
        begin()

    def remote(a, b, send, recv, dev):
        return pltpu.make_async_remote_copy(src_ref=a, dst_ref=b, send_sem=send, recv_sem=recv, device_id={'pp': dev})

    for k, head in ((0, 0), (1, g.last)):
        spot = g.place(g.me + k * (g.last - 2 * g.me))

        @pl.when(g.me == head)
        def _():
            pltpu.make_async_copy(src, slots.at[0, spot], recv_sems.at[0, spot]).start()

        @pl.when(g.me != head)
        def _():
            remote(src, slots.at[0, spot], feed_sems.at[k], recv_sems.at[0, spot], jnp.int32(head)).start()

    def sent(s):
        sec, m = g.step(s)
        kept = jnp.logical_or(jnp.logical_and(sec == 0, inside),
                              jnp.logical_and(jnp.logical_and(sec == 1, outside), m >= half))
        return jnp.logical_not(kept)

    def settle(s):
        @pl.when(sent(s))
        def _():
            par = lax.rem(s, 2)
            remote(out.at[par], slots.at[0, 0], send_sems.at[par], recv_sems.at[0, 0], g.me).wait_send()

    def body(s, carry):
        sec, m = g.step(s)
        c = jnp.where(sec == 1, 1 - c_first, c_first)
        par = lax.rem(s, 2)

        @pl.when(jnp.logical_or(s == 0, s == g.lead))
        def _():
            for w in copies_of(c):
                w.wait()

        @pl.when(s >= 2)
        def _():
            settle(s - 2)

        @pl.when(jnp.logical_not(jnp.logical_and(sec == 1, inside)))
        def _():
            remote(out.at[par], slots.at[sec, m], send_sems.at[par], recv_sems.at[sec, m], g.me).wait_recv()

        unit(s, c, m, slots.at[sec, m], out.at[par])

        @pl.when(jnp.logical_and(sec == 0, inside))
        def _():
            slots[1, m] = out[par]

        @pl.when(jnp.logical_and(sec == 0, jnp.logical_not(inside)))
        def _():
            remote(out.at[par], slots.at[0, m], send_sems.at[par], recv_sems.at[0, m], g.inner).start()

        @pl.when(jnp.logical_and(sec == 1, jnp.logical_not(outside)))
        def _():
            remote(out.at[par], slots.at[1, m], send_sems.at[par], recv_sems.at[1, m], g.outer).start()

        owner = m + g.side * (g.last - 2 * m)
        done = jnp.logical_and(jnp.logical_and(sec == 1, outside), m < half)

        @pl.when(jnp.logical_and(done, owner == g.me))
        def _():
            pltpu.make_async_copy(out.at[par], final, send_sems.at[par]).start()

        @pl.when(jnp.logical_and(done, owner != g.me))
        def _():
            remote(out.at[par], final, send_sems.at[par], final_sem.at[0], owner).start()

        return carry

    lax.fori_loop(0, 2 * n, body, 0)
    settle(2 * n - 2)
    settle(2 * n - 1)
    for k, head in ((0, 0), (1, g.last)):
        @pl.when(g.me != head)
        def _():
            remote(src, slots.at[0, 0], feed_sems.at[k], recv_sems.at[0, 0], jnp.int32(head)).wait_send()

    @pl.when(jnp.logical_not(outside))
    def _():
        remote(out.at[0], final, send_sems.at[0], final_sem.at[0], g.me).wait_recv()


def forward_kernel(n, heads, seq, src, wq, wo, w1, w2, cols, rows, b1,
                   final, hs, ts, rs, ps, gs, ss, as_, os_, bs, us,
                   vwq, vwo, vw1, vw2, vcols, vrows, vb1, slots, out, a, bb, t, o, r, u, p, gp, ya, stats,
                   load_sems, recv_sems, send_sems, final_sem, feed_sems, sems):
    g = Group(n)
    tok, d = a.shape
    f = u.shape[1]
    half = tok // 2

    def unit(s, c, m, x, y):
        def copy(i, v, dst, at=None):
            hbm = dst.at[c, m]
            if at is not None:
                v, hbm = v.at[at], hbm.at[at]
            return pltpu.make_async_copy(v, hbm, sems.at[i])

        def vec(k):
            return vrows[c, k:k + 1, :]

        def norm1(q):
            f_norm(x, vec(0), vec(1), a, stats.at[0], q * half, (q + 1) * half)
            copy(1, a, as_, (pl.ds(q * half, half),)).start()

        def project(q, i):
            z = dot(vwq[c, i:i + CH, :], a[q * half:(q + 1) * half, :], 1, 1)
            z = z + vcols[c, i % d:i % d + CH, i // d:i // d + 1].astype(F32)
            t[i:i + CH, q * half:(q + 1) * half] = z.astype(BF16)

        def attend(q):
            seqs = range(q * half // seq, (q + 1) * half // seq)
            return f_heads(t, o, p, heads, seq, seqs, lambda b: copy(4, p, ps, (pl.ds(b * seq, seq),)).start())

        def merge(q):
            for i in range(q * half, (q + 1) * half, LANES):
                z = dot(o[:, i:i + LANES], vwo[c], 0, 0) + vec(2) + x[i:i + LANES, :].astype(F32)
                z = z.astype(BF16)
                r[i:i + LANES, :] = z
                ya[i:i + LANES, :] = z.astype(F32) + vec(5)

        def norm2(q):
            f_norm(r, vec(3), vec(4), bb, stats.at[1], q * half, (q + 1) * half)
            copy(5, r, rs, (pl.ds(q * half, half),)).start()
            copy(6, bb, bs, (pl.ds(q * half, half),)).start()

        def up(q, j):
            rs_, cs = slice(q * half, (q + 1) * half), slice(j, j + WIDE)
            h = dot(bb[rs_, :], vw1[c, :, cs]) + vb1[c, 0:1, cs]
            uu, slope = gelu_and_slope(h)
            u[rs_, cs] = uu.astype(BF16)
            gp[rs_, cs] = slope
            at = (pl.ds(q * half, half), pl.ds(j, WIDE))
            copy(8, u, us, at).start()
            copy(9, gp, gs, at).start()

        def down(q, j):
            rs_ = slice(q * half, (q + 1) * half)
            ks = slice(j, j + 2 * WIDE)

            def add(rs_, cs):
                z = ya[rs_, cs] + dot(u[rs_, ks], vw2[c, ks, cs])
                if j + 2 * WIDE < f:
                    ya[rs_, cs] = z
                else:
                    y[rs_, cs] = z.astype(BF16)

            add(rs_, slice(0, WIDE))
            add(slice(q * half, q * half + LANES), slice(WIDE, d))
            add(slice(q * half + LANES, (q + 1) * half), slice(WIDE, d))

        def each(fn, q, hi, step):
            return [functools.partial(fn, q, i) for i in range(0, hi, step)]

        copy(0, x, hs).start()
        norm1(0)
        first = each(project, 0, 3 * d, CH)
        woven(first[:2])
        norm1(1)
        woven(first[2:])
        woven(attend(0), each(project, 1, 3 * d, CH))
        copy(2, t, ts).start()
        merge(0)
        late = attend(1)
        woven(late[:4], [functools.partial(norm2, 0)])
        woven(late[4:], each(up, 0, f, WIDE))
        copy(3, o, os_).start()
        merge(1)
        ups, downs = each(up, 1, f, WIDE), each(down, 0, f, 2 * WIDE)
        woven([downs[0]], [functools.partial(norm2, 1)])
        woven(ups, downs[1:])
        woven(each(down, 1, f, 2 * WIDE))
        copy(7, stats, ss).start()
        for i, v, dst in ((0, x, hs), (1, a, as_), (2, t, ts), (3, o, os_), (4, p, ps), (5, r, rs), (6, bb, bs),
                          (7, stats, ss), (8, u, us), (9, gp, gs)):
            copy(i, v, dst).wait()

    weights = [(wq, vwq), (wo, vwo), (w1, vw1), (w2, vw2), (cols, vcols), (rows, vrows), (b1, vb1)]
    run_phase(g, g.side, src, final, slots, out, load_sems, recv_sems, send_sems, final_sem, feed_sems, weights, unit)


def backward_kernel(n, heads, seq, src, wq, wo, w1, w2, rows, hs, ts, rs, ps, gs, ss,
                    final, dys, dgs, drs, dts, sum_rows, sum_b1, sum_bq,
                    vwq, vwo, vw1, vw2, vrows, slots, out, h, t, r, dg, dr, do, pg, stats, acc_rows, acc_b1, acc_bq, part,
                    load_sems, recv_sems, send_sems, final_sem, feed_sems, in_sems, sems):
    g = Group(n)
    tok, d = h.shape
    f = dg.shape[1]
    half = tok // 2
    pcol = ps.shape[3]
    c_first = 1 - g.side

    def fetch(i, s, at=None):
        sec, m = g.step(s)
        c = jnp.where(sec == 1, 1 - c_first, c_first)
        hbm, v = ((gs, pg), (ps, pg.at[:, pl.ds(0, pcol)]), (ts, t), (rs, r), (hs, h), (ss, stats))[i]
        hbm = hbm.at[c, m]
        if at is not None:
            hbm, v = hbm.at[at], v.at[at]
        return pltpu.make_async_copy(hbm, v, in_sems.at[i])

    def ahead(i, s, at=None):
        @pl.when(s + 1 < 2 * n)
        def _():
            fetch(i, s + 1, at).start()

    for i in (0, 2, 3, 4, 5):
        fetch(i, 0).start()
    for v in (acc_rows, acc_b1, acc_bq):
        v[...] = jnp.zeros_like(v)

    def unit(s, c, m, dy, y):
        def copy(i, v, dst):
            return pltpu.make_async_copy(v, dst.at[c, m], sems.at[i])

        def vec(k):
            return vrows[c, k:k + 1, :]

        def down(j):
            cs = slice(j, j + WIDE)
            w = rounded(dot(dy[...], vw2[c, cs, :], 1, 1)) * pg[:, cs]
            dg[:, cs] = w.astype(BF16)
            acc_b1[c, 0:1, cs] += rounded(jnp.sum(rows_sum(w), axis=0, keepdims=True))

        def up(i):
            y[:, i:i + CH] = dot(vw1[c, i:i + CH, :], dg[...], 1, 1).astype(BF16).T

        def tally(k, v):
            acc_rows[c, k:k + 1, :] += rounded(jnp.sum(v, axis=0, keepdims=True))

        def norm(q, src, k, skip, dst, st):
            sums = b_norm(lambda i, e: y[i:e, :].astype(F32), src, vec(k), skip, dst, st, q * half, (q + 1) * half)
            for i, v in enumerate(sums if k else sums[:2]):
                if q == 0:
                    part[i] = v
                else:
                    tally((k, k + 1, 2)[i], part[i] + v)

        def unmerge(q):
            qs = slice(q * half, (q + 1) * half)
            for i in range(0, d, CH):
                do[i:i + CH, qs] = dot(vwo[c, i:i + CH, :], dr[qs, :], 1, 1).astype(BF16)

        def attend(q):
            seqs = range(q * half // seq, (q + 1) * half // seq)
            return b_heads(t, do, pg, heads, seq, seqs, lambda b: ahead(0, s, (pl.ds(b * seq, seq), pl.ds(0, pcol))))

        def unproject(q, i):
            y[i:i + LANES, :] = dot(t[:, i:i + LANES], vwq[c], 0, 0).astype(BF16)

        def bias_q(i):
            at = lax.broadcasted_iota(jnp.int32, (ROWS, LANES), 1)
            e = 0.0
            for k in range(3):
                w = lane_fold(t[k * d + i:k * d + i + ROWS, :].astype(F32))
                e = jnp.where(at == k, rounded(jnp.sum(w, axis=1, keepdims=True)), e)
            acc_bq[c, i:i + ROWS, :] += e

        copy(0, dy, dys).start()
        fetch(0, s).wait()
        woven([functools.partial(down, j) for j in range(0, f, WIDE)])
        fetch(1, s).start()
        ahead(0, s, (slice(None), pl.ds(pcol, f - pcol)))
        copy(1, dg, dgs).start()
        tally(5, rows_sum(dy[...].astype(F32)))
        woven([functools.partial(up, i) for i in range(0, d, CH)])
        fetch(3, s).wait()
        fetch(5, s).wait()
        norm(0, r, 3, dy, dr, stats.at[1])
        unmerge(0)
        norm(1, r, 3, dy, dr, stats.at[1])
        ahead(3, s)
        copy(2, dr, drs).start()
        fetch(1, s).wait()
        fetch(2, s).wait()
        woven(attend(0), [functools.partial(unmerge, 1)])
        fetch(4, s).wait()
        woven(attend(1), [functools.partial(unproject, 0, i) for i in range(0, half, LANES)])
        copy(3, t, dts).start()
        norm(0, h, 0, dr, y, stats.at[0])
        woven([functools.partial(unproject, 1, i) for i in range(half, tok, LANES)])
        woven([functools.partial(bias_q, i) for i in range(0, d, ROWS)])
        norm(1, h, 0, dr, y, stats.at[0])
        ahead(4, s)
        ahead(5, s)
        for i, v, dst in ((0, dy, dys), (1, dg, dgs), (2, dr, drs), (3, t, dts)):
            copy(i, v, dst).wait()
        ahead(2, s)

    weights = [(wq, vwq), (wo, vwo), (w1, vw1), (w2, vw2), (rows, vrows)]
    run_phase(g, c_first, src, final, slots, out, load_sems, recv_sems, send_sems, final_sem, feed_sems, weights, unit)
    cps = [pltpu.make_async_copy(v, o, sems.at[i])
           for i, (v, o) in enumerate(((acc_rows, sum_rows), (acc_b1, sum_b1), (acc_bq, sum_bq)))]
    for cp in cps:
        cp.start()
    for cp in cps:
        cp.wait()


def walk(kernel, name, number, outs, scratch, args):
    return pl.pallas_call(
        kernel, out_shape=outs, in_specs=[HBM] * len(args), out_specs=[HBM] * len(outs), scratch_shapes=scratch, name=name,
        compiler_params=pltpu.CompilerParams(vmem_limit_bytes=VMEM_LIMIT, collective_id=number, has_side_effects=True),
    )(*args)


def semaphores(n, weights, local):
    dma = pltpu.SemaphoreType.DMA
    return [dma((2, weights)), dma((2, n)), dma((2,)), dma((1,)), dma((2,))] + [dma((k,)) for k in local]


def run_forward(n, heads, seq, x, weights):
    tok, d = x.shape
    f = weights[2].shape[2]
    pcol = heads * seq
    vm, st = pltpu.VMEM, jax.ShapeDtypeStruct
    shapes = (((tok, d), BF16), ((3 * d, tok), BF16), ((tok, d), BF16), ((tok, pcol), F32), ((tok, f), F32),
              ((2, tok, LANES), F32), ((tok, d), BF16), ((d, tok), BF16), ((tok, d), BF16), ((tok, f), BF16))
    outs = [st((tok, d), BF16)] + [st((2, n) + v, k) for v, k in shapes]
    scratch = [vm(w.shape, w.dtype) for w in weights] + [
        vm((2, n, tok, d), BF16), vm((2, tok, d), BF16), vm((tok, d), BF16), vm((tok, d), BF16), vm((3 * d, tok), BF16),
        vm((d, tok), BF16), vm((tok, d), BF16), vm((tok, f), BF16), vm((tok, pcol), F32), vm((tok, f), F32),
        vm((tok, d), F32), vm((2, tok, LANES), F32)] + semaphores(n, len(weights), (10,))
    return walk(functools.partial(forward_kernel, n, heads, seq), 'forward_walk', 0, outs, scratch, (x, *weights))


def run_backward(n, heads, seq, dy, weights, stash):
    tok, d = dy.shape
    f = weights[2].shape[2]
    vm, st = pltpu.VMEM, jax.ShapeDtypeStruct
    outs = [st((tok, d), BF16)] + [st((2, n) + v, BF16) for v in ((tok, d), (tok, f), (tok, d), (3 * d, tok))]
    sums = [((2, 8, d), F32), ((2, 8, f), F32), ((2, d, LANES), F32)]
    outs += [st(*v) for v in sums]
    scratch = [vm(w.shape, w.dtype) for w in weights] + [
        vm((2, n, tok, d), BF16), vm((2, tok, d), BF16), vm((tok, d), BF16), vm((3 * d, tok), BF16), vm((tok, d), BF16),
        vm((tok, f), BF16), vm((tok, d), BF16), vm((d, tok), BF16), vm((tok, f), F32), vm((2, tok, LANES), F32)] + [
        vm(*v) for v in sums] + [vm((3, 8, d), F32)] + semaphores(n, len(weights), (6, 4))
    return walk(functools.partial(backward_kernel, n, heads, seq), 'backward_walk', 1, outs, scratch, (dy, *weights, *stash))


PAIR = 2


def grads_kernel(n, sides, *refs):
    ins, outs, accs, (broad, narrow, tall, in_sems, out_sems) = refs[:8], refs[8:12], refs[12:16], refs[16:]
    steps = n // PAIR
    short = tall.at[:, :, pl.ds(0, ins[4].shape[2]), :]
    bufs = ((narrow, broad), (broad, narrow), (short, narrow), (tall, narrow))

    def fetches(c, k, j):
        slot = lax.rem(j, 2)
        at = pl.ds(j * PAIR, PAIR)
        return [pltpu.make_async_copy(ins[2 * k + i].at[c, at], bufs[k][i].at[slot], in_sems.at[slot, i]) for i in range(2)]

    def begin(c, k, j):
        for cp in fetches(c, k, j):
            cp.start()

    def result(c, k):
        return pltpu.make_async_copy(accs[k], outs[k].at[c], out_sems.at[k])

    begin(jnp.int32(0), 0, jnp.int32(0))

    def stage(c, carry):
        for k in range(4):
            def step(j, carry, k=k):
                @pl.when(j + 1 < steps)
                def _():
                    begin(c, k, j + 1)

                @pl.when(j + 1 == steps)
                def _():
                    if k < 3:
                        begin(c, k + 1, jnp.int32(0))
                    else:
                        @pl.when(c == 0)
                        def _():
                            begin(jnp.int32(1), 0, jnp.int32(0))

                @pl.when(jnp.logical_and(j == 0, c == 1))
                def _():
                    result(jnp.int32(0), k).wait()

                for cp in fetches(c, k, j):
                    cp.wait()
                slot = lax.rem(j, 2)
                later = j > 0
                lhs, rhs = bufs[k]
                for i in range(0, accs[k].shape[0], CH):
                    z = jnp.where(later, accs[k][i:i + CH, :], 0.0)
                    for q in range(PAIR):
                        x = lhs[slot, q, :, i:i + CH] if sides[k] == 0 else lhs[slot, q, i:i + CH, :]
                        z = z + rounded(dot(x, rhs[slot, q], sides[k], 0))
                    accs[k][i:i + CH, :] = z
                return carry

            lax.fori_loop(0, steps, step, 0)
            result(c, k).start()
        return carry

    lax.fori_loop(0, 2, stage, 0)
    for k in range(4):
        result(jnp.int32(1), k).wait()


def run_grads(pairs, sides):
    n = pairs[0][0].shape[1]
    st, vm = jax.ShapeDtypeStruct, pltpu.VMEM
    sizes = [(a.shape[3 - s], b.shape[3]) for (a, b), s in zip(pairs, sides)]
    bufs = [vm((2, PAIR) + v.shape[2:], BF16) for v in (pairs[0][1], pairs[0][0], pairs[3][0])]
    return pl.pallas_call(
        functools.partial(grads_kernel, n, sides), out_shape=[st((2,) + v, F32) for v in sizes],
        in_specs=[HBM] * 8, out_specs=[HBM] * 4,
        scratch_shapes=[vm(v, F32) for v in sizes] + bufs + [pltpu.SemaphoreType.DMA((2, 2)), pltpu.SemaphoreType.DMA((4,))],
        name='weight_grads', compiler_params=pltpu.CompilerParams(vmem_limit_bytes=VMEM_LIMIT),
    )(*[v for p in pairs for v in p])


def solution(mesh):
    data_spec = P(('dp', 'pp'))
    weight_spec = P('pp')

    def per_device(x, dy, w_qkv, w_attn, w_fc, w_proj, b_qkv, b_fc, vec_d):
        _, batch, seq, d = x.shape
        heads = w_qkv.shape[5]
        tok = batch * seq

        n = mesh.shape['pp']
        cols = jnp.pad(b_qkv.reshape(2, 3, d).transpose(0, 2, 1), ((0, 0), (0, 0), (0, LANES - 3)))
        rows = jnp.pad(vec_d[0, :, 0].astype(F32), ((0, 0), (0, 2), (0, 0)))
        b1 = jnp.pad(b_fc.reshape(2, 1, -1).astype(F32), ((0, 0), (0, 7), (0, 0)))
        ws = (w_qkv.reshape(2, d, 3 * d).transpose(0, 2, 1), w_attn.reshape(2, d, d), w_fc[0, :, 0], w_proj[0, :, 0])
        y, hs, ts, rs, ps, gs, ss, as_, os_, bs, us = run_forward(n, heads, seq, x.reshape(tok, d), (*ws, cols, rows, b1))
        dx, dys, dgs, drs, dts, s_rows, s_b1, s_bq = run_backward(n, heads, seq, dy.reshape(tok, d), (*ws, rows),
                                                                  (hs, ts, rs, ps, gs, ss))
        g1, g2, go, gq = run_grads(((bs, dgs), (us, dys), (os_, drs), (dts, as_)), (0, 0, 1, 1))
        return (y.reshape(x.shape), dx.reshape(x.shape),
                gq.transpose(0, 2, 1).reshape(w_qkv.shape), go.reshape(w_attn.shape), g1.reshape(w_fc.shape),
                g2.reshape(w_proj.shape), s_bq[:, :, :3].transpose(0, 2, 1).reshape(b_qkv.shape),
                s_b1[:, 0].reshape(b_fc.shape), s_rows[:, :6].reshape(vec_d.shape))

    return jax.shard_map(per_device, mesh=mesh, in_specs=(data_spec, data_spec) + (weight_spec,) * 7,
                         out_specs=(data_spec, data_spec) + (data_spec,) * 7, check_vma=False)
```

```python
import functools

import jax
import jax.numpy as jnp
from jax import lax
from jax.experimental import pallas as pl
from jax.experimental.pallas import tpu as pltpu
from jax.sharding import PartitionSpec as P

EPS = 1e-5
F32 = jnp.float32
BF16 = jnp.bfloat16
LANES = 128
ROWS = 96
CH = 256
SKEW = 8
K0 = 0.7978845608028654
K1 = K0 * 0.044715
VMEM_LIMIT = 67043328
HBM = pl.BlockSpec(memory_space=pl.ANY)


def dot(lhs, rhs, lc=1, rc=0):
    return lax.dot_general(lhs, rhs, (((lc,), (rc,)), ((), ())), preferred_element_type=F32)


def rows_sum(v):
    r, t = v.shape
    return jnp.sum(v.reshape(r // 8, 8, t), axis=0)


def column(cols, lane, row, count):
    return cols[row:row + count, lane:lane + 1].astype(F32)


def lane_fold(v):
    return functools.reduce(jnp.add, [v[:, k:k + LANES] for k in range(0, v.shape[1], LANES)])


def token_sum(v):
    return jnp.sum(lane_fold(v), axis=1, keepdims=True).astype(BF16).astype(F32)


def block_diag(a, b):
    z = jnp.zeros_like(a)
    return jnp.concatenate([jnp.concatenate([a, z], 1), jnp.concatenate([z, b], 1)], 0)


def f_norm(src, cols, lane, dst, stats, row):
    d, t = src.shape
    acc = jnp.zeros((8, t), F32)
    for i in range(0, d, ROWS):
        acc += rows_sum(src[i:i + ROWS, :].astype(F32))
    mean = jnp.sum(acc, axis=0, keepdims=True) * (1.0 / d)
    acc = jnp.zeros((8, t), F32)
    for i in range(0, d, ROWS):
        c = src[i:i + ROWS, :].astype(F32) - mean
        acc += rows_sum(c * c)
    rstd = lax.rsqrt(jnp.sum(acc, axis=0, keepdims=True) * (1.0 / d) + EPS)
    for i in range(0, d, ROWS):
        c = (src[i:i + ROWS, :].astype(F32) - mean) * rstd
        dst[i:i + ROWS, :] = (c * column(cols, lane, i, ROWS) + column(cols, lane + 1, i, ROWS)).astype(BF16)
    stats[row:row + 1, :] = mean
    stats[row + 1:row + 2, :] = rstd


def b_norm(dn, src, cols, gain, skip, dst, stats, row, acc, lane):
    d, t = src.shape
    mean = stats[row:row + 1, :]
    rstd = stats[row + 1:row + 2, :]

    def terms(i):
        c = (src[i:i + ROWS, :].astype(F32) - mean) * rstd
        v = dn[i:i + ROWS, :].astype(F32)
        return c, v, v * column(cols, gain, i, ROWS)

    at = lax.broadcasted_iota(jnp.int32, (ROWS, LANES), 1)
    s1 = jnp.zeros((8, t), F32)
    s2 = jnp.zeros((8, t), F32)
    for i in range(0, d, ROWS):
        c, v, g = terms(i)
        s1 += rows_sum(g)
        s2 += rows_sum(g * c)
        acc[i:i + ROWS, :] += jnp.where(at == lane, token_sum(v * c), jnp.where(at == lane + 1, token_sum(v), 0.0))
    m1 = jnp.sum(s1, axis=0, keepdims=True) * (1.0 / d)
    m2 = jnp.sum(s2, axis=0, keepdims=True) * (1.0 / d)
    for i in range(0, d, ROWS):
        c, _, g = terms(i)
        z = (g - m1 - c * m2) * rstd + skip[i:i + ROWS, :].astype(F32)
        dst[i:i + ROWS, :] = z.astype(BF16)


def skewed(jobs, first, second):
    pending = []
    for job in jobs:
        pending.append((job, first(*job)))
        if len(pending) > SKEW:
            job, v = pending.pop(0)
            second(*job, v)
    for job, v in pending:
        second(*job, v)


def f_heads(t, o, p, heads, seq, after):
    d, n = o.shape
    head = d // heads
    two = 2 * head
    pairs = heads // 2
    key = lax.broadcasted_iota(jnp.int32, (seq, 2 * seq), 0)
    qry = lax.rem(lax.broadcasted_iota(jnp.int32, (seq, 2 * seq), 1), seq)
    ok = key <= qry
    c = (head ** -0.5) * 1.4426950408889634

    def score(b, j):
        r0, lanes = two * j, slice(b * seq, (b + 1) * seq)
        q = t[r0:r0 + two, lanes]
        return dot(t[d + r0:d + r0 + two, lanes], block_diag(q[:head], q[head:]), 0, 0)

    def mix(b, j, s):
        r0, lanes = two * j, slice(b * seq, (b + 1) * seq)
        s = jnp.where(ok, s, -1e30)
        m = jnp.max(s, axis=0, keepdims=True)
        e = jnp.exp2((s - m) * c)
        e = e * (1.0 / jnp.sum(e, axis=0, keepdims=True))
        k0 = (b * pairs + j) * seq
        p[k0:k0 + seq, :] = e
        x = dot(t[2 * d + r0:2 * d + r0 + two, lanes], e.astype(BF16))
        o[r0:r0 + head, lanes] = x[:head, :seq].astype(BF16)
        o[r0 + head:r0 + two, lanes] = x[head:, seq:].astype(BF16)
        if j == pairs - 1:
            after(b)

    skewed([(b, j) for b in range(n // seq) for j in range(pairs)], score, mix)


def b_heads(t, do, p, heads, seq, after):
    d, n = do.shape
    head = d // heads
    two = 2 * head
    pairs = heads // 2
    scale = head ** -0.5

    def first(b, j):
        r0, lanes = two * j, slice(b * seq, (b + 1) * seq)
        z = do[r0:r0 + two, lanes]
        return dot(t[2 * d + r0:2 * d + r0 + two, lanes], block_diag(z[:head], z[head:]), 0, 0)

    def diag(r0, lanes, x, k):
        t[r0:r0 + head, lanes] = (x[:head, :seq] * k).astype(BF16)
        t[r0 + head:r0 + two, lanes] = (x[head:, seq:] * k).astype(BF16)

    def second(b, j, dp):
        r0, lanes = two * j, slice(b * seq, (b + 1) * seq)
        k0 = (b * pairs + j) * seq
        e = p[k0:k0 + seq, :]
        w = e * dp
        ds = (w - e * jnp.sum(w, axis=0, keepdims=True)).astype(BF16)
        eb = e.astype(BF16)
        q, k = t[r0:r0 + two, lanes], t[d + r0:d + r0 + two, lanes]
        tall = jnp.concatenate([ds[:, :seq], ds[:, seq:]], 0)
        dq, dk = dot(k, ds), dot(q, tall, 1, 1)
        tall = jnp.concatenate([eb[:, :seq], eb[:, seq:]], 0)
        dv = dot(do[r0:r0 + two, lanes], tall, 1, 1)
        diag(r0, lanes, dq, scale)
        diag(d + r0, lanes, dk, scale)
        diag(2 * d + r0, lanes, dv, 1.0)
        if j == pairs - 1:
            after(b)

    skewed([(b, j) for b in range(n // seq) for j in range(pairs)], first, second)


def gelu_and_slope(x):
    x2 = x * x
    hp = 0.5 * jnp.tanh(x * (x2 * K1 + K0)) + 0.5
    u = x * hp
    return u, hp + (u - u * hp) * (x2 * (6.0 * K1) + 2.0 * K0)


ORDERS = (
    (0, 1, 2, 3, 4, 5, 6, 7, 8, 16, 9, 17, 10, 18, 11, 19, 12, 20, 13, 21, 14, 22, 15, 23, 24, 25, 26, 27, 28, 29, 30, 31),
    (0, 1, 2, 3, 4, 5, 6, 7, 8, 9, 16, 10, 17, 11, 12, 18, 13, 19, 14, 20, 15, 21, 24, 22, 25, 23, 26, 27, 28, 29, 30, 31),
    (0, 1, 2, 3, 8, 4, 9, 5, 10, 6, 11, 7, 12, 16, 13, 17, 14, 18, 15, 19, 24, 20, 25, 21, 26, 22, 27, 23, 28, 29, 30, 31),
    (0, 8, 1, 9, 2, 10, 3, 11, 4, 12, 5, 13, 6, 14, 7, 15, 16, 24, 17, 25, 18, 26, 19, 27, 20, 28, 21, 29, 22, 30, 23, 31),
)


class Group:
    def __init__(self, n):
        self.n, self.half, self.last, self.steps = n, n // 2, n - 1, 4 * n
        self.me = lax.axis_index('pp')
        self.side = self.me // self.half
        self.depth = self.me + self.side * (self.last - 2 * self.me)
        self.inner = self.me + 1 - 2 * self.side
        self.outer = self.me - 1 + 2 * self.side
        self.inside = self.depth == self.half - 1
        self.outside = self.depth == 0
        self.codes = []
        for k in range(self.steps):
            v = jnp.int32(ORDERS[0][k])
            for i in range(1, self.half):
                v = jnp.where(self.depth == i, ORDERS[i][k], v)
            self.codes.append(v)

    def place(self, i):
        far = lax.rem(i - self.half + self.half // 2, self.half) + self.half
        return jnp.where(i < self.half, i, far)

    def step(self, s):
        code = self.codes[0]
        for k in range(1, self.steps):
            code = jnp.where(s == k, self.codes[k], code)
        kind = code // self.n
        m = code - self.n * kind
        back = kind >= 2
        sec = jnp.where(jnp.logical_or(kind == 1, kind == 2), 1, 0)
        c = jnp.where(sec == 1, 1 - self.side, self.side)
        return kind, back, sec, m, c


def both(a, *rest):
    return functools.reduce(jnp.logical_and, rest, a)


def walk_kernel(n, heads, seq, x_in, dy_in, wq, wo, w1, w2, cols,
                y_out, dx_out, hs, ts, rs, ps, gs, ss, as_, os_, bs, us, dys, dgs, drs, dts, feed, sums,
                vwq, vwo, vw1, vw2, vcols, slots, out, a, t, o, r, u, pg, ya, stats, acc,
                load_sems, recv_sems, send_sems, final_sems, feed_send, feed_recv, f_sems, b_in, b_sems):
    g = Group(n)
    d, tok = a.shape
    f = u.shape[0]
    half = tok // 2
    prow = ps.shape[2]
    part = prow // (tok // seq)
    weights = ((wq, vwq), (wo, vwo), (w1, vw1), (w2, vw2), (cols, vcols))

    def weight_copies(c):
        return [pltpu.make_async_copy(h.at[c], v.at[c], load_sems.at[c, i]) for i, (h, v) in enumerate(weights)]

    def remote(src, dst, send, recv, dev):
        return pltpu.make_async_remote_copy(src_ref=src, dst_ref=dst, send_sem=send, recv_sem=recv, device_id={'pp': dev})

    def saver(c, m, sems):
        def copy(i, v, dst, at=None):
            hbm = dst.at[c, m]
            if at is not None:
                v, hbm = v.at[pl.ds(*at), :], hbm.at[pl.ds(*at), :]
            return pltpu.make_async_copy(v, hbm, sems.at[i])
        return copy

    def fetch(i, c, m, at=None):
        hbm, v = ((gs, pg), (ps, pg.at[pl.ds(0, prow), :]), (ts, t), (rs, r), (hs, a), (ss, stats))[i]
        hbm = hbm.at[c, m]
        if at is not None:
            hbm, v = hbm.at[pl.ds(*at), :], v.at[pl.ds(*at), :]
        return pltpu.make_async_copy(hbm, v, b_in.at[i])

    def forward(c, m, x, y):
        copy = saver(c, m, f_sems)
        cv = vcols.at[c]
        copy(0, x, hs).start()
        f_norm(x, cv, 0, a, stats, 0)
        copy(1, a, as_).start()
        v = a[...]
        for i in range(0, 3 * d, CH):
            z = dot(vwq[c, i:i + CH, :], v) + column(cv, 6 + i // d, i % d, CH)
            t[i:i + CH, :] = z.astype(BF16)
        copy(2, t, ts).start()
        f_heads(t, o, pg, heads, seq, lambda b: copy(4, pg, ps, (b * part, part)).start())
        copy(3, o, os_).start()
        v = o[...]
        for i in range(0, d, CH):
            z = dot(vwo[c, :, i:i + CH], v, 0, 0) + column(cv, 2, i, CH) + x[i:i + CH, :].astype(F32)
            r[i:i + CH, :] = z.astype(BF16)
        copy(5, r, rs).start()
        copy(1, a, as_).wait()
        f_norm(r, cv, 3, a, stats, 2)
        copy(6, a, bs).start()
        copy(7, stats, ss).start()
        copy(4, pg.at[pl.ds(0, prow), :], ps).wait()
        v = a[...]

        def up(k):
            for i in range(k * d, (k + 1) * d, CH):
                h = dot(vw1[c, :, i:i + CH], v, 0, 0) + column(cv, 9 + k, i % d, CH)
                uu, slope = gelu_and_slope(h)
                u[i:i + CH, :] = uu.astype(BF16)
                pg[2 * i:2 * i + CH, :] = slope[:, :half]
                pg[2 * i + CH:2 * i + 2 * CH, :] = slope[:, half:]
                copy(8, u, us, (i, CH)).start()
                copy(9, pg, gs, (2 * i, 2 * CH)).start()

        def down(k):
            w = u[k * d:(k + 1) * d, :]
            for i in range(0, d, CH):
                z = dot(vw2[c, k * d:(k + 1) * d, i:i + CH], w, 0, 0)
                z += (column(cv, 5, i, CH) + r[i:i + CH, :].astype(F32)) if k == 0 else ya[i:i + CH, :]
                if (k + 1) * d < f:
                    ya[i:i + CH, :] = z
                else:
                    y[i:i + CH, :] = z.astype(BF16)

        up(0)
        for k in range(1, f // d):
            up(k)
            down(k - 1)
        down(f // d - 1)
        for i, v, dst in ((0, x, hs), (2, t, ts), (3, o, os_), (5, r, rs), (6, a, bs), (7, stats, ss), (8, u, us),
                          (9, pg, gs)):
            copy(i, v, dst).wait()

    def backward(c, m, dy, y, then):
        copy = saver(c, m, b_sems)
        cv = vcols.at[c]
        copy(0, dy, dys).start()
        fetch(0, c, m).wait()
        v = dy[...]
        for i in range(0, f, CH):
            du = dot(vw2[c, i:i + CH, :], v).astype(BF16).astype(F32)
            u[i:i + CH, :half] = (du[:, :half] * pg[2 * i:2 * i + CH, :]).astype(BF16)
            u[i:i + CH, half:] = (du[:, half:] * pg[2 * i + CH:2 * i + 2 * CH, :]).astype(BF16)
        fetch(1, c, m).start()
        then(0, (prow, 2 * f - prow))
        copy(1, u, dgs).start()
        v = u[...]
        for i in range(0, d, CH):
            y[i:i + CH, :] = dot(vw1[c, i:i + CH, :], v).astype(BF16)
        fetch(3, c, m).wait()
        fetch(5, c, m).wait()
        b_norm(y, r, cv, 3, dy, o, stats, 2, acc.at[c], 2)
        then(3)
        copy(2, o, drs).start()
        v = o[...]
        for i in range(0, d, CH):
            y[i:i + CH, :] = dot(vwo[c, i:i + CH, :], v).astype(BF16)
        fetch(1, c, m).wait()
        fetch(2, c, m).wait()
        b_heads(t, y, pg, heads, seq, lambda b: then(0, (b * part, part)))
        copy(3, t, dts).start()
        v = t[...]
        at = lax.broadcasted_iota(jnp.int32, (ROWS, LANES), 1)
        for i in range(0, d, CH):
            y[i:i + CH, :] = dot(vwq[c, :, i:i + CH], v, 0, 0).astype(BF16)
        for i in range(0, d, ROWS):
            e = 0.0
            for k in range(3):
                e = jnp.where(at == 4 + k, token_sum(t[k * d + i:k * d + i + ROWS, :].astype(F32)), e)
            acc[c, i:i + ROWS, :] += e
        fetch(4, c, m).wait()
        b_norm(y, a, cv, 0, o, y, stats, 0, acc.at[c], 0)
        then(4)
        then(5)
        for i, v, dst in ((0, dy, dys), (1, u, dgs), (2, o, drs), (3, t, dts)):
            copy(i, v, dst).wait()
        then(2)

    for c in (g.side, 1 - g.side):
        for w in weight_copies(c):
            w.start()
    barrier = pltpu.get_barrier_semaphore()
    for i in range(n):
        pl.semaphore_signal(barrier, inc=1, device_id={'pp': jnp.int32(i)})
    pl.semaphore_wait(barrier, n)

    heads_at = ((0, 0), (1, g.last))
    for k, head in heads_at:
        spot = g.place(g.me + k * (g.last - 2 * g.me))

        @pl.when(g.me == head)
        def _():
            pltpu.make_async_copy(x_in, slots.at[0, spot], recv_sems.at[0, 0, spot]).start()

        @pl.when(g.me != head)
        def _():
            remote(x_in, slots.at[0, spot], feed_send.at[0, k], recv_sems.at[0, 0, spot], jnp.int32(head)).start()
            remote(dy_in, feed.at[spot], feed_send.at[1, k], feed_recv.at[spot], jnp.int32(head)).start()

    acc[...] = jnp.zeros_like(acc)

    def settle(par, flag):
        @pl.when(flag == 1)
        def _():
            remote(out.at[par], slots.at[0, 0], send_sems.at[par], recv_sems.at[0, 0, 0], g.me).wait_send()

    def body(s, carry):
        kind, back, sec, m, c = g.step(s)
        nxt = jnp.minimum(s + 1, g.steps - 1)
        _, back2, _, m2, c2 = g.step(nxt)
        more = both(back2, s + 1 < g.steps)
        par = lax.rem(s, 2)
        inward = jnp.logical_or(kind == 0, kind == 2)
        outward = jnp.logical_not(inward)
        way = jnp.where(back, 1, 0)

        @pl.when(jnp.logical_or(s == 0, both(kind == 1, m == 0)))
        def _():
            for w in weight_copies(c):
                w.wait()

        settle(par, carry[1])

        @pl.when(jnp.logical_not(both(outward, g.inside)))
        def _():
            remote(out.at[par], slots.at[sec, m], send_sems.at[par], recv_sems.at[way, sec, m], g.me).wait_recv()

        @pl.when(jnp.logical_not(back))
        def _():
            forward(c, m, slots.at[sec, m], out.at[par])

            @pl.when(more)
            def _():
                for i in (0, 2, 3, 4, 5):
                    fetch(i, c2, m2).start()

        @pl.when(back)
        def _():
            def then(i, at=None):
                @pl.when(more)
                def _():
                    fetch(i, c2, m2, at).start()

            backward(c, m, slots.at[sec, m], out.at[par], then)

        @pl.when(both(inward, g.inside))
        def _():
            slots[1 - sec, m] = out[par]

        @pl.when(both(inward, jnp.logical_not(g.inside)))
        def _():
            remote(out.at[par], slots.at[sec, m], send_sems.at[par], recv_sems.at[way, sec, m], g.inner).start()

        @pl.when(both(outward, jnp.logical_not(g.outside)))
        def _():
            remote(out.at[par], slots.at[sec, m], send_sems.at[par], recv_sems.at[way, sec, m], g.outer).start()

        owner = m + g.side * (g.last - 2 * m)
        done = both(outward, g.outside, m < g.half)
        for w, ref in ((0, y_out), (1, dx_out)):
            mine = both(done, way == w)

            @pl.when(both(mine, owner == g.me))
            def _():
                pltpu.make_async_copy(out.at[par], ref, send_sems.at[par]).start()

            @pl.when(both(mine, owner != g.me))
            def _():
                remote(out.at[par], ref, send_sems.at[par], final_sems.at[w], owner).start()

        @pl.when(both(kind == 1, g.outside))
        def _():
            @pl.when(m == 0)
            def _():
                pltpu.make_async_copy(dy_in, slots.at[1, m], recv_sems.at[1, 1, m]).start()

            @pl.when(m > 0)
            def _():
                remote(dy_in, feed.at[m], feed_send.at[1, 0], feed_recv.at[m], g.me).wait_recv()
                pltpu.make_async_copy(feed.at[m], slots.at[1, m], recv_sems.at[1, 1, m]).start()

        kept = jnp.logical_or(both(inward, g.inside), both(outward, g.outside, m >= g.half))
        return jnp.where(kept, 0, 1), carry[0]

    before, earlier = lax.fori_loop(0, g.steps, body, (jnp.int32(0), jnp.int32(0)))
    settle(g.steps % 2, earlier)
    settle((g.steps + 1) % 2, before)
    for k, head in heads_at:
        @pl.when(g.me != head)
        def _():
            remote(x_in, slots.at[0, 0], feed_send.at[0, k], recv_sems.at[0, 0, 0], jnp.int32(head)).wait_send()
            remote(dy_in, feed.at[0], feed_send.at[1, k], feed_recv.at[0], jnp.int32(head)).wait_send()

    @pl.when(jnp.logical_not(g.outside))
    def _():
        for w, ref in ((0, y_out), (1, dx_out)):
            remote(out.at[0], ref, send_sems.at[0], final_sems.at[w], g.me).wait_recv()

    cp = pltpu.make_async_copy(acc, sums, b_sems.at[0])
    cp.start()
    cp.wait()


def run_walk(mesh, heads, seq, xt, dyt, weights):
    n = mesh.shape['pp']
    d, tok = xt.shape
    f = weights[2].shape[2]
    prow = (tok // seq) * (heads // 2) * seq
    st, vm, dma = jax.ShapeDtypeStruct, pltpu.VMEM, pltpu.SemaphoreType.DMA
    act, tall, hid = ((d, tok), BF16), ((3 * d, tok), BF16), ((f, tok), BF16)
    outs = [st(*act)] * 2 + [st((2, n) + v, k) for v, k in (
        act, tall, act, ((prow, 2 * seq), F32), ((2 * f, tok // 2), F32), ((8, tok), F32), act, act, act, hid,
        act, hid, act, tall)] + [st((n, d, tok), BF16), st((2, d, LANES), F32)]
    scratch = [vm(w.shape, w.dtype) for w in weights] + [
        vm((2, n, d, tok), BF16), vm((2, d, tok), BF16), vm(*act), vm(*tall), vm(*act), vm(*act), vm(*hid),
        vm((2 * f, tok // 2), F32), vm((d, tok), F32), vm((8, tok), F32), vm((2, d, LANES), F32),
        dma((2, len(weights))), dma((2, 2, n)), dma((2,)), dma((2,)), dma((2, 2)), dma((n,)), dma((10,)), dma((6,)), dma((4,))]
    return pl.pallas_call(
        functools.partial(walk_kernel, n, heads, seq), out_shape=outs, in_specs=[HBM] * 7, out_specs=[HBM] * len(outs),
        scratch_shapes=scratch, name='walk',
        compiler_params=pltpu.CompilerParams(vmem_limit_bytes=VMEM_LIMIT, collective_id=0, has_side_effects=True),
    )(xt, dyt, *weights)


PAIR = 2


def grads_kernel(n, *refs):
    ins, refs = refs[:8], refs[8:]
    outs, bias_outs, refs = refs[:4], refs[4:7], refs[7:]
    accs, biases, (buf, in_sems, out_sems) = refs[:4], refs[4:7], refs[7:]
    steps = n // PAIR
    tok = buf.shape[3]

    def fetches(c, k, j):
        slot = lax.rem(j, 2)
        rows, cols = ins[2 * k].shape[2], ins[2 * k + 1].shape[2]
        at = pl.ds(j * PAIR, PAIR)
        return (pltpu.make_async_copy(ins[2 * k].at[c, at], buf.at[slot, :, pl.ds(0, rows), :], in_sems.at[slot, 0]),
                pltpu.make_async_copy(ins[2 * k + 1].at[c, at], buf.at[slot, :, pl.ds(rows, cols), :], in_sems.at[slot, 1]))

    def begin(c, k, j):
        for cp in fetches(c, k, j):
            cp.start()

    def results(c, k):
        cps = [pltpu.make_async_copy(accs[k], outs[k].at[c], out_sems.at[k])]
        if k < 3:
            cps.append(pltpu.make_async_copy(biases[k], bias_outs[k].at[c], out_sems.at[4 + k]))
        return cps

    begin(jnp.int32(0), 0, jnp.int32(0))

    def stage(c, carry):
        for k in range(4):
            rows, cols = ins[2 * k].shape[2], ins[2 * k + 1].shape[2]

            def step(j, carry, k=k, rows=rows, cols=cols):
                @pl.when(j + 1 < steps)
                def _():
                    begin(c, k, j + 1)

                @pl.when(j + 1 == steps)
                def _():
                    if k < 3:
                        begin(c, k + 1, jnp.int32(0))
                    else:
                        @pl.when(c == 0)
                        def _():
                            begin(jnp.int32(1), 0, jnp.int32(0))

                @pl.when(jnp.logical_and(j == 0, c == 1))
                def _():
                    for cp in results(jnp.int32(0), k):
                        cp.wait()

                for cp in fetches(c, k, j):
                    cp.wait()
                slot = lax.rem(j, 2)
                later = j > 0
                for i in range(0, rows, CH):
                    z = jnp.where(later, accs[k][i:i + CH, :], 0.0)
                    if i == 0 and k < 3:
                        e = jnp.where(later, biases[k][...], 0.0)
                    for q in range(PAIR):
                        x = buf[slot, q, i:i + CH, :]
                        if i == 0 and k < 3:
                            x = jnp.concatenate([x, jnp.ones((16, tok), BF16)], 0)
                        v = dot(x, buf[slot, q, rows:rows + cols, :], 1, 1).astype(BF16).astype(F32)
                        z = z + v[:CH]
                        if i == 0 and k < 3:
                            e = e + v[CH:CH + 8]
                    accs[k][i:i + CH, :] = z
                    if i == 0 and k < 3:
                        biases[k][...] = e
                return carry

            lax.fori_loop(0, steps, step, 0)
            for cp in results(c, k):
                cp.start()
        return carry

    lax.fori_loop(0, 2, stage, 0)
    for k in range(4):
        for cp in results(jnp.int32(1), k):
            cp.wait()


def run_grads(pairs):
    n, tok = pairs[0][0].shape[1], pairs[0][0].shape[3]
    sizes = [(a.shape[2], b.shape[2]) for a, b in pairs]
    st = jax.ShapeDtypeStruct
    vm = pltpu.VMEM
    most = max(a + b for a, b in sizes)
    return pl.pallas_call(
        functools.partial(grads_kernel, n),
        out_shape=[st((2,) + v, F32) for v in sizes] + [st((2, 8, v[1]), F32) for v in sizes[:3]],
        in_specs=[HBM] * 8, out_specs=[HBM] * 7,
        scratch_shapes=[vm(v, F32) for v in sizes] + [vm((8, v[1]), F32) for v in sizes[:3]] + [
            vm((2, PAIR, most, tok), BF16), pltpu.SemaphoreType.DMA((2, 2)), pltpu.SemaphoreType.DMA((7,))],
        name='weight_grads', compiler_params=pltpu.CompilerParams(vmem_limit_bytes=VMEM_LIMIT),
    )(*[v for p in pairs for v in p])


def solution(mesh):
    data_spec = P(('dp', 'pp'))
    weight_spec = P('pp')

    def per_device(x, dy, w_qkv, w_attn, w_fc, w_proj, b_qkv, b_fc, vec_d):
        _, batch, seq, d = x.shape
        heads = w_qkv.shape[5]
        tok = batch * seq

        cols = jnp.concatenate([vec_d[0, :, 0], b_qkv.reshape(2, 3, d), b_fc.reshape(2, -1, d)], axis=1)
        cols = jnp.pad(cols.transpose(0, 2, 1), ((0, 0), (0, 0), (0, LANES - cols.shape[1])))
        weights = (w_qkv.reshape(2, d, 3 * d).transpose(0, 2, 1), w_attn.reshape(2, d, d), w_fc[0, :, 0], w_proj[0, :, 0],
                   cols)
        xt = x.reshape(tok, d).T
        dyt = dy.reshape(tok, d).T
        yt, dxt, *stash, sums = run_walk(mesh, heads, seq, xt, dyt, weights)
        as_, os_, bs, us, dys, dgs, drs, dts = stash[6:14]
        g1, g2, go, gq, gb1, gb2, gbo = run_grads(((bs, dgs), (us, dys), (os_, drs), (dts, as_)))
        s = sums[:, :, :7].transpose(0, 2, 1)
        gv = jnp.stack([s[:, 0], s[:, 1], gbo[:, 0], s[:, 2], s[:, 3], gb2[:, 0]], axis=1)
        back = lambda v: v.T.reshape(x.shape)
        return (back(yt), back(dxt),
                gq.transpose(0, 2, 1).reshape(w_qkv.shape), go.reshape(w_attn.shape), g1.reshape(w_fc.shape),
                g2.reshape(w_proj.shape), s[:, 4:7].reshape(b_qkv.shape), gb1[:, 0].reshape(b_fc.shape),
                gv.reshape(vec_d.shape))

    return jax.shard_map(per_device, mesh=mesh, in_specs=(data_spec, data_spec) + (weight_spec,) * 7,
                         out_specs=(data_spec, data_spec) + (data_spec,) * 7, check_vma=False)
```

```python
import functools

import jax
import jax.numpy as jnp
from jax import lax
from jax.experimental import pallas as pl
from jax.experimental.pallas import tpu as pltpu
from jax.sharding import PartitionSpec as P

EPS = 1e-5
F32 = jnp.float32
BF16 = jnp.bfloat16
LANES = 128
ROWS = 96
CH = 256
SKEW = 8
K0 = 0.7978845608028654
K1 = K0 * 0.044715
VMEM_LIMIT = 67043328
HBM = pl.BlockSpec(memory_space=pl.ANY)


def dot(lhs, rhs, lc=1, rc=0):
    return lax.dot_general(lhs, rhs, (((lc,), (rc,)), ((), ())), preferred_element_type=F32)


def rows_sum(v):
    r, t = v.shape
    return jnp.sum(v.reshape(r // 8, 8, t), axis=0)


def column(cols, lane, row, count):
    return cols[row:row + count, lane:lane + 1].astype(F32)


def lane_fold(v):
    return functools.reduce(jnp.add, [v[:, k:k + LANES] for k in range(0, v.shape[1], LANES)])


def rounded(v):
    return v.astype(BF16).astype(F32)


def token_sum(v):
    return rounded(jnp.sum(lane_fold(v), axis=1, keepdims=True))


def block_diag(a, b):
    z = jnp.zeros_like(a)
    return jnp.concatenate([jnp.concatenate([a, z], 1), jnp.concatenate([z, b], 1)], 0)


def f_norm(src, cols, lane, dst, stats, row):
    d, t = src.shape
    acc = jnp.zeros((8, t), F32)
    for i in range(0, d, ROWS):
        acc += rows_sum(src[i:i + ROWS, :].astype(F32))
    mean = jnp.sum(acc, axis=0, keepdims=True) * (1.0 / d)
    acc = jnp.zeros((8, t), F32)
    for i in range(0, d, ROWS):
        c = src[i:i + ROWS, :].astype(F32) - mean
        acc += rows_sum(c * c)
    rstd = lax.rsqrt(jnp.sum(acc, axis=0, keepdims=True) * (1.0 / d) + EPS)
    for i in range(0, d, ROWS):
        c = (src[i:i + ROWS, :].astype(F32) - mean) * rstd
        dst[i:i + ROWS, :] = (c * column(cols, lane, i, ROWS) + column(cols, lane + 1, i, ROWS)).astype(BF16)
    stats[row:row + 1, :] = mean
    stats[row + 1:row + 2, :] = rstd


def b_norm(dn, src, cols, gain, skip, dst, stats, row, acc, lane):
    d, t = src.shape
    mean = stats[row:row + 1, :]
    rstd = stats[row + 1:row + 2, :]

    def terms(i):
        c = (src[i:i + ROWS, :].astype(F32) - mean) * rstd
        v = dn[i:i + ROWS, :].astype(F32)
        return c, v, v * column(cols, gain, i, ROWS)

    at = lax.broadcasted_iota(jnp.int32, (ROWS, LANES), 1)
    s1 = jnp.zeros((8, t), F32)
    s2 = jnp.zeros((8, t), F32)
    for i in range(0, d, ROWS):
        c, v, g = terms(i)
        s1 += rows_sum(g)
        s2 += rows_sum(g * c)
        acc[i:i + ROWS, :] += jnp.where(at == lane, token_sum(v * c), jnp.where(at == lane + 1, token_sum(v), 0.0))
    m1 = jnp.sum(s1, axis=0, keepdims=True) * (1.0 / d)
    m2 = jnp.sum(s2, axis=0, keepdims=True) * (1.0 / d)
    for i in range(0, d, ROWS):
        c, _, g = terms(i)
        z = (g - m1 - c * m2) * rstd + skip[i:i + ROWS, :].astype(F32)
        dst[i:i + ROWS, :] = z.astype(BF16)


def skewed(jobs, first, second):
    pending = []
    for job in jobs:
        pending.append((job, first(*job)))
        if len(pending) > SKEW:
            job, v = pending.pop(0)
            second(*job, v)
    for job, v in pending:
        second(*job, v)


def f_heads(t, o, p, heads, seq, after):
    d, n = o.shape
    head = d // heads
    two = 2 * head
    pairs = heads // 2
    key = lax.broadcasted_iota(jnp.int32, (seq, 2 * seq), 0)
    qry = lax.rem(lax.broadcasted_iota(jnp.int32, (seq, 2 * seq), 1), seq)
    ok = key <= qry
    c = (head ** -0.5) * 1.4426950408889634

    def score(b, j):
        r0, lanes = two * j, slice(b * seq, (b + 1) * seq)
        q = t[r0:r0 + two, lanes]
        return dot(t[d + r0:d + r0 + two, lanes], block_diag(q[:head], q[head:]), 0, 0)

    def mix(b, j, s):
        r0, lanes = two * j, slice(b * seq, (b + 1) * seq)
        s = jnp.where(ok, s, -1e30)
        m = jnp.max(s, axis=0, keepdims=True)
        e = jnp.exp2((s - m) * c)
        e = e * (1.0 / jnp.sum(e, axis=0, keepdims=True))
        k0 = (b * pairs + j) * seq
        p[k0:k0 + seq, :] = e
        x = dot(t[2 * d + r0:2 * d + r0 + two, lanes], e.astype(BF16))
        o[r0:r0 + head, lanes] = x[:head, :seq].astype(BF16)
        o[r0 + head:r0 + two, lanes] = x[head:, seq:].astype(BF16)
        if j == pairs - 1:
            after(b)

    skewed([(b, j) for b in range(n // seq) for j in range(pairs)], score, mix)


def b_heads(t, do, p, heads, seq, after):
    d, n = do.shape
    head = d // heads
    two = 2 * head
    pairs = heads // 2
    scale = head ** -0.5

    def first(b, j):
        r0, lanes = two * j, slice(b * seq, (b + 1) * seq)
        z = do[r0:r0 + two, lanes]
        return dot(t[2 * d + r0:2 * d + r0 + two, lanes], block_diag(z[:head], z[head:]), 0, 0)

    def diag(r0, lanes, x, k):
        t[r0:r0 + head, lanes] = (x[:head, :seq] * k).astype(BF16)
        t[r0 + head:r0 + two, lanes] = (x[head:, seq:] * k).astype(BF16)

    def second(b, j, dp):
        r0, lanes = two * j, slice(b * seq, (b + 1) * seq)
        k0 = (b * pairs + j) * seq
        e = p[k0:k0 + seq, :]
        w = e * dp
        ds = (w - e * jnp.sum(w, axis=0, keepdims=True)).astype(BF16)
        eb = e.astype(BF16)
        q, k = t[r0:r0 + two, lanes], t[d + r0:d + r0 + two, lanes]
        tall = jnp.concatenate([ds[:, :seq], ds[:, seq:]], 0)
        dq, dk = dot(k, ds), dot(q, tall, 1, 1)
        tall = jnp.concatenate([eb[:, :seq], eb[:, seq:]], 0)
        dv = dot(do[r0:r0 + two, lanes], tall, 1, 1)
        diag(r0, lanes, dq, scale)
        diag(d + r0, lanes, dk, scale)
        diag(2 * d + r0, lanes, dv, 1.0)
        if j == pairs - 1:
            after(b)

    skewed([(b, j) for b in range(n // seq) for j in range(pairs)], first, second)


def gelu_and_slope(x):
    x2 = x * x
    hp = 0.5 * jnp.tanh(x * (x2 * K1 + K0)) + 0.5
    u = x * hp
    return u, hp + (u - u * hp) * (x2 * (6.0 * K1) + 2.0 * K0)


ORDERS = (
    (0, 1, 2, 3, 4, 5, 6, 7, 8, 16, 9, 17, 10, 18, 11, 19, 12, 20, 13, 21, 14, 22, 15, 23, 24, 32, 33, 25, 34, 35, 26,
     36, 37, 27, 38, 39, 28, 40, 41, 29, 42, 43, 30, 31),
    (0, 1, 2, 3, 4, 5, 6, 7, 8, 9, 16, 10, 17, 11, 18, 12, 19, 13, 14, 20, 15, 21, 24, 22, 25, 23, 26, 32, 33, 27, 34, 35,
     28, 29, 36, 30, 37, 38, 31, 39, 40, 41, 42, 43),
    (0, 1, 2, 3, 8, 4, 9, 5, 10, 6, 11, 7, 12, 16, 13, 17, 14, 18, 15, 19, 24, 20, 25, 21, 26, 22, 27, 23, 28, 29, 32,
     30, 33, 34, 31, 35, 36, 37, 38, 39, 40, 41, 42, 43),
    (0, 8, 1, 9, 2, 10, 3, 11, 4, 12, 5, 13, 6, 14, 7, 15, 16, 24, 17, 25, 18, 26, 19, 27, 20, 28, 21, 29, 22, 30, 23, 31,
     32, 33, 34, 35, 36, 37, 38, 39, 40, 41, 42, 43),
)
BLOCKS = 12


class Group:
    def __init__(self, n):
        self.n, self.half, self.last, self.steps = n, n // 2, n - 1, len(ORDERS[0])
        self.me = lax.axis_index('pp')
        self.side = self.me // self.half
        self.depth = self.me + self.side * (self.last - 2 * self.me)
        self.inner = self.me + 1 - 2 * self.side
        self.outer = self.me - 1 + 2 * self.side
        self.inside = self.depth == self.half - 1
        self.outside = self.depth == 0
        self.codes = []
        for k in range(self.steps):
            v = jnp.int32(ORDERS[0][k])
            for i in range(1, self.half):
                v = jnp.where(self.depth == i, ORDERS[i][k], v)
            self.codes.append(v)

    def place(self, i):
        far = lax.rem(i - self.half + self.half // 2, self.half) + self.half
        return jnp.where(i < self.half, i, far)

    def step(self, s):
        code = self.codes[0]
        for k in range(1, self.steps):
            code = jnp.where(s == k, self.codes[k], code)
        kind = code // self.n
        m = code - self.n * kind
        back = jnp.logical_and(kind >= 2, kind < 4)
        sec = jnp.where(jnp.logical_or(kind == 1, kind == 2), 1, 0)
        c = jnp.where(sec == 1, 1 - self.side, self.side)
        return kind, back, sec, m, c, code - 4 * self.n


def both(a, *rest):
    return functools.reduce(jnp.logical_and, rest, a)


def walk_kernel(n, heads, seq, x_in, dy_in, wq, wo, w1, w2, cols,
                y_out, dx_out, hs, ts, rs, ps, gs, ss, as_, os_, bs, us, dys, dgs, drs, dts, feed, sums, blocks, edges,
                vwq, vwo, vw1, vw2, vcols, slots, out, a, t, o, r, u, pg, ya, stats, acc, edge,
                load_sems, recv_sems, send_sems, final_sems, feed_send, feed_recv, f_sems, b_in, b_sems, w_in, w_out):
    g = Group(n)
    d, tok = a.shape
    f = u.shape[0]
    half = tok // 2
    prow = ps.shape[2]
    part = prow // (tok // seq)
    weights = ((wq, vwq), (wo, vwo), (w1, vw1), (w2, vw2), (cols, vcols))

    def weight_copies(c):
        return [pltpu.make_async_copy(h.at[c], v.at[c], load_sems.at[c, i]) for i, (h, v) in enumerate(weights)]

    def remote(src, dst, send, recv, dev):
        return pltpu.make_async_remote_copy(src_ref=src, dst_ref=dst, send_sem=send, recv_sem=recv, device_id={'pp': dev})

    def saver(c, m, sems):
        def copy(i, v, dst, at=None):
            hbm = dst.at[c, m]
            if at is not None:
                v, hbm = v.at[pl.ds(*at), :], hbm.at[pl.ds(*at), :]
            return pltpu.make_async_copy(v, hbm, sems.at[i])
        return copy

    def fetch(i, c, m, at=None):
        hbm, v = ((gs, pg), (ps, pg.at[pl.ds(0, prow), :]), (ts, t), (rs, r), (hs, a), (ss, stats))[i]
        hbm = hbm.at[c, m]
        if at is not None:
            hbm, v = hbm.at[pl.ds(*at), :], v.at[pl.ds(*at), :]
        return pltpu.make_async_copy(hbm, v, b_in.at[i])

    def forward(c, m, x, y):
        copy = saver(c, m, f_sems)
        cv = vcols.at[c]
        copy(0, x, hs).start()
        f_norm(x, cv, 0, a, stats, 0)
        copy(1, a, as_).start()
        v = a[...]
        for i in range(0, 3 * d, CH):
            z = dot(vwq[c, i:i + CH, :], v) + column(cv, 6 + i // d, i % d, CH)
            t[i:i + CH, :] = z.astype(BF16)
        copy(2, t, ts).start()
        f_heads(t, o, pg, heads, seq, lambda b: copy(4, pg, ps, (b * part, part)).start())
        copy(3, o, os_).start()
        v = o[...]
        for i in range(0, d, CH):
            z = dot(vwo[c, :, i:i + CH], v, 0, 0) + column(cv, 2, i, CH) + x[i:i + CH, :].astype(F32)
            r[i:i + CH, :] = z.astype(BF16)
        copy(5, r, rs).start()
        copy(1, a, as_).wait()
        f_norm(r, cv, 3, a, stats, 2)
        copy(6, a, bs).start()
        copy(7, stats, ss).start()
        copy(4, pg.at[pl.ds(0, prow), :], ps).wait()
        v = a[...]

        def up(k):
            for i in range(k * d, (k + 1) * d, CH):
                h = dot(vw1[c, :, i:i + CH], v, 0, 0) + column(cv, 9 + k, i % d, CH)
                uu, slope = gelu_and_slope(h)
                u[i:i + CH, :] = uu.astype(BF16)
                pg[2 * i:2 * i + CH, :] = slope[:, :half]
                pg[2 * i + CH:2 * i + 2 * CH, :] = slope[:, half:]
                copy(8, u, us, (i, CH)).start()
                copy(9, pg, gs, (2 * i, 2 * CH)).start()

        def down(k):
            w = u[k * d:(k + 1) * d, :]
            for i in range(0, d, CH):
                z = dot(vw2[c, k * d:(k + 1) * d, i:i + CH], w, 0, 0)
                z += (column(cv, 5, i, CH) + r[i:i + CH, :].astype(F32)) if k == 0 else ya[i:i + CH, :]
                if (k + 1) * d < f:
                    ya[i:i + CH, :] = z
                else:
                    y[i:i + CH, :] = z.astype(BF16)

        up(0)
        for k in range(1, f // d):
            up(k)
            down(k - 1)
        down(f // d - 1)
        for i, v, dst in ((0, x, hs), (2, t, ts), (3, o, os_), (5, r, rs), (6, a, bs), (7, stats, ss), (8, u, us),
                          (9, pg, gs)):
            copy(i, v, dst).wait()

    def backward(c, m, dy, y, then):
        copy = saver(c, m, b_sems)
        cv = vcols.at[c]
        copy(0, dy, dys).start()
        fetch(0, c, m).wait()
        v = dy[...]
        for i in range(0, f, CH):
            du = dot(vw2[c, i:i + CH, :], v).astype(BF16).astype(F32)
            u[i:i + CH, :half] = (du[:, :half] * pg[2 * i:2 * i + CH, :]).astype(BF16)
            u[i:i + CH, half:] = (du[:, half:] * pg[2 * i + CH:2 * i + 2 * CH, :]).astype(BF16)
        fetch(1, c, m).start()
        then(0, (prow, 2 * f - prow))
        copy(1, u, dgs).start()
        v = u[...]
        for i in range(0, d, CH):
            y[i:i + CH, :] = dot(vw1[c, i:i + CH, :], v).astype(BF16)
        fetch(3, c, m).wait()
        fetch(5, c, m).wait()
        b_norm(y, r, cv, 3, dy, o, stats, 2, acc.at[c], 2)
        then(3)
        copy(2, o, drs).start()
        v = o[...]
        for i in range(0, d, CH):
            y[i:i + CH, :] = dot(vwo[c, i:i + CH, :], v).astype(BF16)
        fetch(1, c, m).wait()
        fetch(2, c, m).wait()
        b_heads(t, y, pg, heads, seq, lambda b: then(0, (b * part, part)))
        copy(3, t, dts).start()
        v = t[...]
        at = lax.broadcasted_iota(jnp.int32, (ROWS, LANES), 1)
        for i in range(0, d, CH):
            y[i:i + CH, :] = dot(vwq[c, :, i:i + CH], v, 0, 0).astype(BF16)
        for i in range(0, d, ROWS):
            e = 0.0
            for k in range(3):
                e = jnp.where(at == 4 + k, token_sum(t[k * d + i:k * d + i + ROWS, :].astype(F32)), e)
            acc[c, i:i + ROWS, :] += e
        fetch(4, c, m).wait()
        b_norm(y, a, cv, 0, o, y, stats, 0, acc.at[c], 0)
        then(4)
        then(5)
        for i, v, dst in ((0, dy, dys), (1, u, dgs), (2, o, drs), (3, t, dts)):
            copy(i, v, dst).wait()
        then(2)

    c_last = 1 - g.side

    def operands(k, m, slot, act):
        def pair(lhs, i, rhs, j):
            for q, (h, i0) in enumerate(((lhs, i), (rhs, j))):
                cp = pltpu.make_async_copy(h.at[c_last, m, pl.ds(pl.multiple_of(i0 * d, d), d), :],
                                           u.at[pl.ds((2 * slot + q) * d, d), :], w_in.at[slot, q])
                act(cp)

        for lo, hi, lhs, rhs, left in ((0, 4, bs, dgs, False), (4, 8, us, dys, True), (8, 9, os_, drs, True),
                                       (9, 12, dts, as_, True)):
            @pl.when(both(k >= lo, k < hi))
            def _(lo=lo, lhs=lhs, rhs=rhs, left=left):
                pair(lhs, (k - lo) if left else 0, rhs, 0 if left else (k - lo))

    def block_out(k, par):
        rows = pl.ds(pl.multiple_of(par * 3 * d, 3 * d), 3 * d)
        return (pltpu.make_async_copy(pg.at[rows, :], blocks.at[k], w_out.at[par, 0]),
                pltpu.make_async_copy(edge.at[par], edges.at[k], w_out.at[par, 1]))

    def weight_block(k, par, ran, ran2, again):
        begin = lambda cp: cp.start()
        end = lambda cp: cp.wait()
        base = par * 3 * d

        @pl.when(ran == 0)
        def _():
            operands(k, 0, 0, begin)

        @pl.when(both(ran == 1, ran2 == 1))
        def _():
            for cp in block_out(k - 2, par):
                cp.wait()

        def pairs(j, carry):
            for slot in range(2):
                m = 2 * j + slot
                if slot == 0:
                    operands(k, m + 1, 1, begin)
                else:
                    @pl.when(m + 1 < n)
                    def _():
                        operands(k, m + 1, 0, begin)

                    @pl.when(both(m + 1 == n, again))
                    def _():
                        operands(k + 1, 0, 0, begin)
                operands(k, m, slot, end)
                lhs, rhs = 2 * slot * d, (2 * slot + 1) * d
                w = u[rhs:rhs + d, :]
                for i in range(0, d, CH):
                    x = u[lhs + i:lhs + i + CH, :]
                    if i == 0:
                        x = jnp.concatenate([x, jnp.ones((16, tok), BF16)], 0)
                    z = rounded(dot(x, w, 1, 1))
                    for q in range(3):
                        rows = pl.ds(pl.multiple_of(base + q * d + i, CH), CH)
                        v = z[:CH, q * CH:(q + 1) * CH]
                        pg[rows, :] = v + (jnp.where(m > 0, pg[rows, :], 0.0) if slot == 0 else pg[rows, :])
                    if i == 0:
                        v = z[CH:CH + 8]
                        edge[par] = v + (jnp.where(m > 0, edge[par], 0.0) if slot == 0 else edge[par])
            return carry

        lax.fori_loop(0, n // 2, pairs, 0)
        for cp in block_out(k, par):
            cp.start()

        @pl.when(jnp.logical_not(again))
        def _():
            for cp in block_out(k, par):
                cp.wait()

            @pl.when(ran == 1)
            def _():
                for cp in block_out(k - 1, 1 - par):
                    cp.wait()

    for c in (g.side, 1 - g.side):
        for w in weight_copies(c):
            w.start()
    barrier = pltpu.get_barrier_semaphore()
    for i in range(n):
        pl.semaphore_signal(barrier, inc=1, device_id={'pp': jnp.int32(i)})
    pl.semaphore_wait(barrier, n)

    heads_at = ((0, 0), (1, g.last))
    for k, head in heads_at:
        spot = g.place(g.me + k * (g.last - 2 * g.me))

        @pl.when(g.me == head)
        def _():
            pltpu.make_async_copy(x_in, slots.at[0, spot], recv_sems.at[0, 0, spot]).start()

        @pl.when(g.me != head)
        def _():
            remote(x_in, slots.at[0, spot], feed_send.at[0, k], recv_sems.at[0, 0, spot], jnp.int32(head)).start()
            remote(dy_in, feed.at[spot], feed_send.at[1, k], feed_recv.at[spot], jnp.int32(head)).start()

    acc[...] = jnp.zeros_like(acc)

    def settle(par, flag):
        @pl.when(flag == 1)
        def _():
            remote(out.at[par], slots.at[0, 0], send_sems.at[par], recv_sems.at[0, 0, 0], g.me).wait_send()

    def body(s, carry):
        kind, back, sec, m, c, block = g.step(s)
        nxt = jnp.minimum(s + 1, g.steps - 1)
        _, back2, _, m2, c2, block2 = g.step(nxt)
        more = both(back2, s + 1 < g.steps)
        fill = block >= 0
        again = both(block2 >= 0, s + 1 < g.steps)
        par = lax.rem(s, 2)
        inward = jnp.logical_or(kind == 0, kind == 2)
        outward = jnp.logical_or(kind == 1, kind == 3)
        way = jnp.where(back, 1, 0)

        @pl.when(jnp.logical_or(s == 0, both(kind == 1, m == 0)))
        def _():
            for w in weight_copies(c):
                w.wait()

        settle(par, carry[1])

        @pl.when(jnp.logical_not(jnp.logical_or(fill, both(outward, g.inside))))
        def _():
            remote(out.at[par], slots.at[sec, m], send_sems.at[par], recv_sems.at[way, sec, m], g.me).wait_recv()

        @pl.when(kind < 2)
        def _():
            forward(c, m, slots.at[sec, m], out.at[par])

        @pl.when(fill)
        def _():
            weight_block(block, par, carry[2], carry[3], again)

        @pl.when(both(more, jnp.logical_not(back)))
        def _():
            for i in (0, 2, 3, 4, 5):
                fetch(i, c2, m2).start()

        @pl.when(back)
        def _():
            def then(i, at=None):
                @pl.when(more)
                def _():
                    fetch(i, c2, m2, at).start()

            backward(c, m, slots.at[sec, m], out.at[par], then)

        @pl.when(both(inward, g.inside))
        def _():
            slots[1 - sec, m] = out[par]

        @pl.when(both(inward, jnp.logical_not(g.inside)))
        def _():
            remote(out.at[par], slots.at[sec, m], send_sems.at[par], recv_sems.at[way, sec, m], g.inner).start()

        @pl.when(both(outward, jnp.logical_not(g.outside)))
        def _():
            remote(out.at[par], slots.at[sec, m], send_sems.at[par], recv_sems.at[way, sec, m], g.outer).start()

        owner = m + g.side * (g.last - 2 * m)
        done = both(outward, g.outside, m < g.half)
        for w, ref in ((0, y_out), (1, dx_out)):
            mine = both(done, way == w)

            @pl.when(both(mine, owner == g.me))
            def _():
                pltpu.make_async_copy(out.at[par], ref, send_sems.at[par]).start()

            @pl.when(both(mine, owner != g.me))
            def _():
                remote(out.at[par], ref, send_sems.at[par], final_sems.at[w], owner).start()

        @pl.when(both(kind == 1, g.outside))
        def _():
            @pl.when(m == 0)
            def _():
                pltpu.make_async_copy(dy_in, slots.at[1, m], recv_sems.at[1, 1, m]).start()

            @pl.when(m > 0)
            def _():
                remote(dy_in, feed.at[m], feed_send.at[1, 0], feed_recv.at[m], g.me).wait_recv()
                pltpu.make_async_copy(feed.at[m], slots.at[1, m], recv_sems.at[1, 1, m]).start()

        kept = jnp.logical_or(jnp.logical_or(fill, both(inward, g.inside)), both(outward, g.outside, m >= g.half))
        return jnp.where(kept, 0, 1), carry[0], jnp.where(fill, 1, 0), carry[2]

    before, earlier, _, _ = lax.fori_loop(0, g.steps, body, (jnp.int32(0),) * 4)
    settle(g.steps % 2, earlier)
    settle((g.steps + 1) % 2, before)
    for k, head in heads_at:
        @pl.when(g.me != head)
        def _():
            remote(x_in, slots.at[0, 0], feed_send.at[0, k], recv_sems.at[0, 0, 0], jnp.int32(head)).wait_send()
            remote(dy_in, feed.at[0], feed_send.at[1, k], feed_recv.at[0], jnp.int32(head)).wait_send()

    @pl.when(jnp.logical_not(g.outside))
    def _():
        for w, ref in ((0, y_out), (1, dx_out)):
            remote(out.at[0], ref, send_sems.at[0], final_sems.at[w], g.me).wait_recv()

    cp = pltpu.make_async_copy(acc, sums, b_sems.at[0])
    cp.start()
    cp.wait()


def run_walk(mesh, heads, seq, xt, dyt, weights):
    n = mesh.shape['pp']
    d, tok = xt.shape
    f = weights[2].shape[2]
    prow = (tok // seq) * (heads // 2) * seq
    st, vm, dma = jax.ShapeDtypeStruct, pltpu.VMEM, pltpu.SemaphoreType.DMA
    act, tall, hid = ((d, tok), BF16), ((3 * d, tok), BF16), ((f, tok), BF16)
    outs = [st(*act)] * 2 + [st((2, n) + v, k) for v, k in (
        act, tall, act, ((prow, 2 * seq), F32), ((2 * f, tok // 2), F32), ((8, tok), F32), act, act, act, hid,
        act, hid, act, tall)] + [
        st((n, d, tok), BF16), st((2, d, LANES), F32), st((BLOCKS, 3 * d, tok // 2), F32), st((BLOCKS, 8, d), F32)]
    scratch = [vm(w.shape, w.dtype) for w in weights] + [
        vm((2, n, d, tok), BF16), vm((2, d, tok), BF16), vm(*act), vm(*tall), vm(*act), vm(*act), vm(*hid),
        vm((2 * f, tok // 2), F32), vm((d, tok), F32), vm((8, tok), F32), vm((2, d, LANES), F32), vm((2, 8, d), F32),
        dma((2, len(weights))), dma((2, 2, n)), dma((2,)), dma((2,)), dma((2, 2)), dma((n,)), dma((10,)), dma((6,)), dma((4,)), dma((2, 2)), dma((2, 2))]
    return pl.pallas_call(
        functools.partial(walk_kernel, n, heads, seq), out_shape=outs, in_specs=[HBM] * 7, out_specs=[HBM] * len(outs),
        scratch_shapes=scratch, name='walk',
        compiler_params=pltpu.CompilerParams(vmem_limit_bytes=VMEM_LIMIT, collective_id=0, has_side_effects=True),
    )(xt, dyt, *weights)


PAIR = 2


def grads_kernel(n, *refs):
    ins, blocks, edges, refs = refs[:8], refs[8], refs[9], refs[10:]
    outs, bias_outs, refs = refs[:4], refs[4:7], refs[7:]
    accs, biases, (buf, stage, rim, in_sems, out_sems, move_in, move_out, rim_sems) = refs[:4], refs[4:7], refs[7:]
    steps = n // PAIR
    tok = buf.shape[3]
    d = edges.shape[2]
    wide = blocks.shape[2]
    me = lax.axis_index('pp')
    c = me // (n // 2)
    other = 1 - c

    def fetches(k, j):
        slot = lax.rem(j, 2)
        rows, cols = ins[2 * k].shape[2], ins[2 * k + 1].shape[2]
        at = pl.ds(j * PAIR, PAIR)
        return (pltpu.make_async_copy(ins[2 * k].at[c, at], buf.at[slot, :, pl.ds(0, rows), :], in_sems.at[slot, 0]),
                pltpu.make_async_copy(ins[2 * k + 1].at[c, at], buf.at[slot, :, pl.ds(rows, cols), :], in_sems.at[slot, 1]))

    def begin(k, j):
        for cp in fetches(k, j):
            cp.start()

    def results(k):
        cps = [pltpu.make_async_copy(accs[k], outs[k].at[c], out_sems.at[k])]
        if k < 3:
            cps.append(pltpu.make_async_copy(biases[k], bias_outs[k].at[c], out_sems.at[4 + k]))
        return cps

    def load(i, slot):
        return pltpu.make_async_copy(blocks.at[i], stage.at[slot], move_in.at[slot])

    def place(out, row, col, slot):
        return [pltpu.make_async_copy(stage.at[slot, pl.ds(q * d, d), :],
                                      out.at[other, pl.ds(row, d), pl.ds(col + q * wide, wide)], move_out.at[slot, q])
                for q in range(3)]

    rims = pltpu.make_async_copy(edges, rim, rim_sems.at[0])
    rims.start()
    begin(0, jnp.int32(0))
    for k in range(4):
        rows, cols = ins[2 * k].shape[2], ins[2 * k + 1].shape[2]

        def step(j, carry, k=k, rows=rows, cols=cols):
            slot = lax.rem(j, 2)

            @pl.when(j + 1 < steps)
            def _():
                begin(k, j + 1)

            if k < 3:
                @pl.when(j + 1 == steps)
                def _():
                    begin(k + 1, jnp.int32(0))

                if k > 0:
                    for cp in place(outs[0], 0, 0, slot):
                        cp.wait()
                else:
                    @pl.when(j >= 2)
                    def _():
                        for cp in place(outs[0], 0, 0, slot):
                            cp.wait()
                load(4 * k + j, slot).start()

            for cp in fetches(k, j):
                cp.wait()
            later = j > 0
            for i in range(0, rows, CH):
                z = jnp.where(later, accs[k][i:i + CH, :], 0.0)
                if i == 0 and k < 3:
                    e = jnp.where(later, biases[k][...], 0.0)
                for q in range(PAIR):
                    x = buf[slot, q, i:i + CH, :]
                    if i == 0 and k < 3:
                        x = jnp.concatenate([x, jnp.ones((16, tok), BF16)], 0)
                    v = rounded(dot(x, buf[slot, q, rows:rows + cols, :], 1, 1))
                    z = z + v[:CH]
                    if i == 0 and k < 3:
                        e = e + v[CH:CH + 8]
                accs[k][i:i + CH, :] = z
                if i == 0 and k < 3:
                    biases[k][...] = e

            if k < 3:
                load(4 * k + j, slot).wait()
                at = pl.multiple_of(j * d, d)
                if k == 0:
                    for cp in place(outs[0], 0, at, slot):
                        cp.start()
                elif k == 1:
                    for cp in place(outs[1], at, 0, slot):
                        cp.start()
                else:
                    @pl.when(j == 0)
                    def _():
                        for cp in place(outs[2], 0, 0, slot):
                            cp.start()

                    @pl.when(j > 0)
                    def _():
                        for cp in place(outs[3], pl.multiple_of((j - 1) * d, d), 0, slot):
                            cp.start()
            return carry

        lax.fori_loop(0, steps, step, 0)
        for cp in results(k):
            cp.start()
    rims.wait()
    edge_copies = [pltpu.make_async_copy(rim.at[i], bias_outs[0].at[other, :, pl.ds(i * d, d)], rim_sems.at[1 + i])
                   for i in range(4)]
    edge_copies += [pltpu.make_async_copy(rim.at[4], bias_outs[1].at[other], rim_sems.at[5]),
                    pltpu.make_async_copy(rim.at[8], bias_outs[2].at[other], rim_sems.at[6])]
    for cp in edge_copies:
        cp.start()
    for cp in edge_copies:
        cp.wait()
    for slot in range(2):
        for cp in place(outs[0], 0, 0, slot):
            cp.wait()
    for k in range(4):
        for cp in results(k):
            cp.wait()


def run_grads(pairs, blocks, edges):
    n, tok = pairs[0][0].shape[1], pairs[0][0].shape[3]
    sizes = [(a.shape[2], b.shape[2]) for a, b in pairs]
    st, vm, dma = jax.ShapeDtypeStruct, pltpu.VMEM, pltpu.SemaphoreType.DMA
    most = max(a + b for a, b in sizes)
    return pl.pallas_call(
        functools.partial(grads_kernel, n),
        out_shape=[st((2,) + v, F32) for v in sizes] + [st((2, 8, v[1]), F32) for v in sizes[:3]],
        in_specs=[HBM] * 10, out_specs=[HBM] * 7,
        scratch_shapes=[vm(v, F32) for v in sizes] + [vm((8, v[1]), F32) for v in sizes[:3]] + [
            vm((2, PAIR, most, tok), BF16), vm((2,) + blocks.shape[1:], F32), vm(edges.shape, F32),
            dma((2, 2)), dma((7,)), dma((2,)), dma((2, 3)), dma((7,))],
        name='weight_grads', compiler_params=pltpu.CompilerParams(vmem_limit_bytes=VMEM_LIMIT),
    )(*[v for p in pairs for v in p], blocks, edges)


def solution(mesh):
    data_spec = P(('dp', 'pp'))
    weight_spec = P('pp')

    def per_device(x, dy, w_qkv, w_attn, w_fc, w_proj, b_qkv, b_fc, vec_d):
        _, batch, seq, d = x.shape
        heads = w_qkv.shape[5]
        tok = batch * seq

        cols = jnp.concatenate([vec_d[0, :, 0], b_qkv.reshape(2, 3, d), b_fc.reshape(2, -1, d)], axis=1)
        cols = jnp.pad(cols.transpose(0, 2, 1), ((0, 0), (0, 0), (0, LANES - cols.shape[1])))
        weights = (w_qkv.reshape(2, d, 3 * d).transpose(0, 2, 1), w_attn.reshape(2, d, d), w_fc[0, :, 0], w_proj[0, :, 0],
                   cols)
        xt = x.reshape(tok, d).T
        dyt = dy.reshape(tok, d).T
        yt, dxt, *stash, sums, blocks, edges = run_walk(mesh, heads, seq, xt, dyt, weights)
        as_, os_, bs, us, dys, dgs, drs, dts = stash[6:14]
        g1, g2, go, gq, gb1, gb2, gbo = run_grads(((bs, dgs), (us, dys), (os_, drs), (dts, as_)), blocks, edges)
        s = sums[:, :, :7].transpose(0, 2, 1)
        gv = jnp.stack([s[:, 0], s[:, 1], gbo[:, 0], s[:, 2], s[:, 3], gb2[:, 0]], axis=1)
        back = lambda v: v.T.reshape(x.shape)
        return (back(yt), back(dxt),
                gq.transpose(0, 2, 1).reshape(w_qkv.shape), go.reshape(w_attn.shape), g1.reshape(w_fc.shape),
                g2.reshape(w_proj.shape), s[:, 4:7].reshape(b_qkv.shape), gb1[:, 0].reshape(b_fc.shape),
                gv.reshape(vec_d.shape))

    return jax.shard_map(per_device, mesh=mesh, in_specs=(data_spec, data_spec) + (weight_spec,) * 7,
                         out_specs=(data_spec, data_spec) + (data_spec,) * 7, check_vma=False)
```

```python
import functools

import jax
import jax.numpy as jnp
from jax import lax
from jax.experimental import pallas as pl
from jax.experimental.pallas import tpu as pltpu
from jax.sharding import PartitionSpec as P

EPS = 1e-5
F32 = jnp.float32
BF16 = jnp.bfloat16
LANES = 128
ROWS = 96
CH = 256
SKEW = 8
K0 = 0.7978845608028654
K1 = K0 * 0.044715
VMEM_LIMIT = 67043328
HBM = pl.BlockSpec(memory_space=pl.ANY)


def dot(lhs, rhs, lc=1, rc=0):
    return lax.dot_general(lhs, rhs, (((lc,), (rc,)), ((), ())), preferred_element_type=F32)


def rows_sum(v):
    r, t = v.shape
    return jnp.sum(v.reshape(r // 8, 8, t), axis=0)


def column(cols, lane, row, count):
    return cols[row:row + count, lane:lane + 1].astype(F32)


def lane_fold(v):
    return functools.reduce(jnp.add, [v[:, k:k + LANES] for k in range(0, v.shape[1], LANES)])


def rounded(v):
    return v.astype(BF16).astype(F32)


def token_sum(v):
    return rounded(jnp.sum(lane_fold(v), axis=1, keepdims=True))


def block_diag(a, b):
    z = jnp.zeros_like(a)
    return jnp.concatenate([jnp.concatenate([a, z], 1), jnp.concatenate([z, b], 1)], 0)


def f_norm(src, cols, lane, dst, stats, row):
    d, t = src.shape
    acc = jnp.zeros((8, t), F32)
    for i in range(0, d, ROWS):
        acc += rows_sum(src[i:i + ROWS, :].astype(F32))
    mean = jnp.sum(acc, axis=0, keepdims=True) * (1.0 / d)
    acc = jnp.zeros((8, t), F32)
    for i in range(0, d, ROWS):
        c = src[i:i + ROWS, :].astype(F32) - mean
        acc += rows_sum(c * c)
    rstd = lax.rsqrt(jnp.sum(acc, axis=0, keepdims=True) * (1.0 / d) + EPS)
    for i in range(0, d, ROWS):
        c = (src[i:i + ROWS, :].astype(F32) - mean) * rstd
        dst[i:i + ROWS, :] = (c * column(cols, lane, i, ROWS) + column(cols, lane + 1, i, ROWS)).astype(BF16)
    stats[row:row + 1, :] = mean
    stats[row + 1:row + 2, :] = rstd


def b_norm(dn, src, cols, gain, skip, dst, stats, row, acc, lane):
    d, t = src.shape
    mean = stats[row:row + 1, :]
    rstd = stats[row + 1:row + 2, :]

    def terms(i):
        c = (src[i:i + ROWS, :].astype(F32) - mean) * rstd
        v = dn[i:i + ROWS, :].astype(F32)
        return c, v, v * column(cols, gain, i, ROWS)

    at = lax.broadcasted_iota(jnp.int32, (ROWS, LANES), 1)
    s1 = jnp.zeros((8, t), F32)
    s2 = jnp.zeros((8, t), F32)
    for i in range(0, d, ROWS):
        c, v, g = terms(i)
        s1 += rows_sum(g)
        s2 += rows_sum(g * c)
        acc[i:i + ROWS, :] += jnp.where(at == lane, token_sum(v * c), jnp.where(at == lane + 1, token_sum(v), 0.0))
    m1 = jnp.sum(s1, axis=0, keepdims=True) * (1.0 / d)
    m2 = jnp.sum(s2, axis=0, keepdims=True) * (1.0 / d)
    for i in range(0, d, ROWS):
        c, _, g = terms(i)
        z = (g - m1 - c * m2) * rstd + skip[i:i + ROWS, :].astype(F32)
        dst[i:i + ROWS, :] = z.astype(BF16)


def skewed(jobs, first, second):
    pending = []
    for job in jobs:
        pending.append((job, first(*job)))
        if len(pending) > SKEW:
            job, v = pending.pop(0)
            second(*job, v)
    for job, v in pending:
        second(*job, v)


def f_heads(t, o, p, heads, seq, after):
    d, n = o.shape
    head = d // heads
    two = 2 * head
    pairs = heads // 2
    key = lax.broadcasted_iota(jnp.int32, (seq, 2 * seq), 0)
    qry = lax.rem(lax.broadcasted_iota(jnp.int32, (seq, 2 * seq), 1), seq)
    ok = key <= qry
    c = (head ** -0.5) * 1.4426950408889634

    def score(b, j):
        r0, lanes = two * j, slice(b * seq, (b + 1) * seq)
        q = t[r0:r0 + two, lanes]
        return dot(t[d + r0:d + r0 + two, lanes], block_diag(q[:head], q[head:]), 0, 0)

    def mix(b, j, s):
        r0, lanes = two * j, slice(b * seq, (b + 1) * seq)
        s = jnp.where(ok, s, -1e30)
        m = jnp.max(s, axis=0, keepdims=True)
        e = jnp.exp2((s - m) * c)
        e = e * (1.0 / jnp.sum(e, axis=0, keepdims=True))
        k0 = (b * pairs + j) * seq
        p[k0:k0 + seq, :] = e
        x = dot(t[2 * d + r0:2 * d + r0 + two, lanes], e.astype(BF16))
        o[r0:r0 + head, lanes] = x[:head, :seq].astype(BF16)
        o[r0 + head:r0 + two, lanes] = x[head:, seq:].astype(BF16)
        if j == pairs - 1:
            after(b)

    skewed([(b, j) for b in range(n // seq) for j in range(pairs)], score, mix)


def b_heads(t, do, p, heads, seq, after):
    d, n = do.shape
    head = d // heads
    two = 2 * head
    pairs = heads // 2
    scale = head ** -0.5

    def first(b, j):
        r0, lanes = two * j, slice(b * seq, (b + 1) * seq)
        z = do[r0:r0 + two, lanes]
        return dot(t[2 * d + r0:2 * d + r0 + two, lanes], block_diag(z[:head], z[head:]), 0, 0)

    def diag(r0, lanes, x, k):
        t[r0:r0 + head, lanes] = (x[:head, :seq] * k).astype(BF16)
        t[r0 + head:r0 + two, lanes] = (x[head:, seq:] * k).astype(BF16)

    def second(b, j, dp):
        r0, lanes = two * j, slice(b * seq, (b + 1) * seq)
        k0 = (b * pairs + j) * seq
        e = p[k0:k0 + seq, :]
        w = e * dp
        ds = (w - e * jnp.sum(w, axis=0, keepdims=True)).astype(BF16)
        eb = e.astype(BF16)
        q, k = t[r0:r0 + two, lanes], t[d + r0:d + r0 + two, lanes]
        tall = jnp.concatenate([ds[:, :seq], ds[:, seq:]], 0)
        dq, dk = dot(k, ds), dot(q, tall, 1, 1)
        tall = jnp.concatenate([eb[:, :seq], eb[:, seq:]], 0)
        dv = dot(do[r0:r0 + two, lanes], tall, 1, 1)
        diag(r0, lanes, dq, scale)
        diag(d + r0, lanes, dk, scale)
        diag(2 * d + r0, lanes, dv, 1.0)
        if j == pairs - 1:
            after(b)

    skewed([(b, j) for b in range(n // seq) for j in range(pairs)], first, second)


def gelu_and_slope(x):
    x2 = x * x
    hp = 0.5 * jnp.tanh(x * (x2 * K1 + K0)) + 0.5
    u = x * hp
    return u, hp + (u - u * hp) * (x2 * (6.0 * K1) + 2.0 * K0)


ORDERS = (
    (0, 1, 2, 3, 4, 5, 6, 7, 8, 16, 9, 17, 10, 18, 11, 19, 12, 20, 13, 21, 14, 22, 15, 23, 24, 25, 26, 27, 28, 29, 30, 31),
    (0, 1, 2, 3, 4, 5, 6, 7, 8, 9, 16, 10, 17, 11, 12, 18, 13, 19, 14, 20, 15, 21, 24, 22, 25, 23, 26, 27, 28, 29, 30, 31),
    (0, 1, 2, 3, 8, 4, 9, 5, 10, 6, 11, 7, 12, 16, 13, 17, 14, 18, 15, 19, 24, 20, 25, 21, 26, 22, 27, 23, 28, 29, 30, 31),
    (0, 8, 1, 9, 2, 10, 3, 11, 4, 12, 5, 13, 6, 14, 7, 15, 16, 24, 17, 25, 18, 26, 19, 27, 20, 28, 21, 29, 22, 30, 23, 31),
)


class Group:
    def __init__(self, n):
        self.n, self.half, self.last, self.steps = n, n // 2, n - 1, 4 * n
        self.me = lax.axis_index('pp')
        self.side = self.me // self.half
        self.depth = self.me + self.side * (self.last - 2 * self.me)
        self.inner = self.me + 1 - 2 * self.side
        self.outer = self.me - 1 + 2 * self.side
        self.inside = self.depth == self.half - 1
        self.outside = self.depth == 0
        self.codes = []
        for k in range(self.steps):
            v = jnp.int32(ORDERS[0][k])
            for i in range(1, self.half):
                v = jnp.where(self.depth == i, ORDERS[i][k], v)
            self.codes.append(v)

    def place(self, i):
        far = lax.rem(i - self.half + self.half // 2, self.half) + self.half
        return jnp.where(i < self.half, i, far)

    def step(self, s):
        code = self.codes[0]
        for k in range(1, self.steps):
            code = jnp.where(s == k, self.codes[k], code)
        kind = code // self.n
        m = code - self.n * kind
        back = kind >= 2
        sec = jnp.where(jnp.logical_or(kind == 1, kind == 2), 1, 0)
        c = jnp.where(sec == 1, 1 - self.side, self.side)
        return kind, back, sec, m, c


def both(a, *rest):
    return functools.reduce(jnp.logical_and, rest, a)


def walk_kernel(n, heads, seq, x_in, dy_in, wq, wo, w1, w2, vec, bq, b1,
                y_out, dx_out, hs, ts, rs, ps, gs, ss, as_, os_, bs, us, dys, dgs, drs, dts, feed, sums, x_t, dy_t,
                vwq, vwo, vw1, vw2, vcols, vvec, vbq, vb1, slots, out, a, t, o, r, u, pg, ya, stats, acc,
                load_sems, recv_sems, send_sems, final_sems, feed_send, feed_recv, f_sems, b_in, b_sems, lead_sems):
    g = Group(n)
    d, tok = a.shape
    f = u.shape[0]
    half = tok // 2
    prow = ps.shape[2]
    part = prow // (tok // seq)
    weights = ((wq, vwq), (wo, vwo), (w1, vw1), (w2, vw2))

    def weight(c, i):
        h, v = weights[i]
        return pltpu.make_async_copy(h.at[c], v.at[c], load_sems.at[c, i])

    def remote(src, dst, send, recv, dev):
        return pltpu.make_async_remote_copy(src_ref=src, dst_ref=dst, send_sem=send, recv_sem=recv, device_id={'pp': dev})

    def saver(c, m, sems):
        def copy(i, v, dst, at=None):
            hbm = dst.at[c, m]
            if at is not None:
                v, hbm = v.at[pl.ds(*at), :], hbm.at[pl.ds(*at), :]
            return pltpu.make_async_copy(v, hbm, sems.at[i])
        return copy

    def fetch(i, c, m, at=None):
        hbm, v = ((gs, pg), (ps, pg.at[pl.ds(0, prow), :]), (ts, t), (rs, r), (hs, a), (ss, stats))[i]
        hbm = hbm.at[c, m]
        if at is not None:
            hbm, v = hbm.at[pl.ds(*at), :], v.at[pl.ds(*at), :]
        return pltpu.make_async_copy(hbm, v, b_in.at[i])

    def forward(c, m, x, y, fresh):
        copy = saver(c, m, f_sems)

        def need(*which):
            @pl.when(fresh)
            def _():
                for i in which:
                    weight(c, i).wait()

        cv = vcols.at[c]
        copy(0, x, hs).start()
        f_norm(x, cv, 0, a, stats, 0)
        copy(1, a, as_).start()
        need(0)
        v = a[...]
        for i in range(0, 3 * d, CH):
            z = dot(vwq[c, i:i + CH, :], v) + column(cv, 6 + i // d, i % d, CH)
            t[i:i + CH, :] = z.astype(BF16)
        copy(2, t, ts).start()
        f_heads(t, o, pg, heads, seq, lambda b: copy(4, pg, ps, (b * part, part)).start())
        copy(3, o, os_).start()
        need(1)
        v = o[...]
        for i in range(0, d, CH):
            z = dot(vwo[c, :, i:i + CH], v, 0, 0) + column(cv, 2, i, CH) + x[i:i + CH, :].astype(F32)
            r[i:i + CH, :] = z.astype(BF16)
        copy(5, r, rs).start()
        copy(1, a, as_).wait()
        f_norm(r, cv, 3, a, stats, 2)
        copy(6, a, bs).start()
        copy(7, stats, ss).start()
        copy(4, pg.at[pl.ds(0, prow), :], ps).wait()
        need(2, 3)
        v = a[...]

        def up(k):
            for i in range(k * d, (k + 1) * d, CH):
                h = dot(vw1[c, :, i:i + CH], v, 0, 0) + column(cv, 9 + k, i % d, CH)
                uu, slope = gelu_and_slope(h)
                u[i:i + CH, :] = uu.astype(BF16)
                pg[2 * i:2 * i + CH, :] = slope[:, :half]
                pg[2 * i + CH:2 * i + 2 * CH, :] = slope[:, half:]
                copy(8, u, us, (i, CH)).start()
                copy(9, pg, gs, (2 * i, 2 * CH)).start()

        def down(k):
            w = u[k * d:(k + 1) * d, :]
            for i in range(0, d, CH):
                z = dot(vw2[c, k * d:(k + 1) * d, i:i + CH], w, 0, 0)
                z += (column(cv, 5, i, CH) + r[i:i + CH, :].astype(F32)) if k == 0 else ya[i:i + CH, :]
                if (k + 1) * d < f:
                    ya[i:i + CH, :] = z
                else:
                    y[i:i + CH, :] = z.astype(BF16)

        up(0)
        for k in range(1, f // d):
            up(k)
            down(k - 1)
        down(f // d - 1)
        for i, v, dst in ((0, x, hs), (2, t, ts), (3, o, os_), (5, r, rs), (6, a, bs), (7, stats, ss), (8, u, us),
                          (9, pg, gs)):
            copy(i, v, dst).wait()

    def backward(c, m, dy, y, then):
        copy = saver(c, m, b_sems)
        cv = vcols.at[c]
        copy(0, dy, dys).start()
        fetch(0, c, m).wait()
        v = dy[...]
        for i in range(0, f, CH):
            du = dot(vw2[c, i:i + CH, :], v).astype(BF16).astype(F32)
            u[i:i + CH, :half] = (du[:, :half] * pg[2 * i:2 * i + CH, :]).astype(BF16)
            u[i:i + CH, half:] = (du[:, half:] * pg[2 * i + CH:2 * i + 2 * CH, :]).astype(BF16)
        fetch(1, c, m).start()
        then(0, (prow, 2 * f - prow))
        copy(1, u, dgs).start()
        v = u[...]
        for i in range(0, d, CH):
            y[i:i + CH, :] = dot(vw1[c, i:i + CH, :], v).astype(BF16)
        fetch(3, c, m).wait()
        fetch(5, c, m).wait()
        b_norm(y, r, cv, 3, dy, o, stats, 2, acc.at[c], 2)
        then(3)
        copy(2, o, drs).start()
        v = o[...]
        for i in range(0, d, CH):
            y[i:i + CH, :] = dot(vwo[c, i:i + CH, :], v).astype(BF16)
        fetch(1, c, m).wait()
        fetch(2, c, m).wait()
        b_heads(t, y, pg, heads, seq, lambda b: then(0, (b * part, part)))
        copy(3, t, dts).start()
        v = t[...]
        at = lax.broadcasted_iota(jnp.int32, (ROWS, LANES), 1)
        for i in range(0, d, CH):
            y[i:i + CH, :] = dot(vwq[c, :, i:i + CH], v, 0, 0).astype(BF16)
        for i in range(0, d, ROWS):
            e = 0.0
            for k in range(3):
                e = jnp.where(at == 4 + k, token_sum(t[k * d + i:k * d + i + ROWS, :].astype(F32)), e)
            acc[c, i:i + ROWS, :] += e
        fetch(4, c, m).wait()
        b_norm(y, a, cv, 0, o, y, stats, 0, acc.at[c], 0)
        then(4)
        then(5)
        for i, v, dst in ((0, dy, dys), (1, u, dgs), (2, o, drs), (3, t, dts)):
            copy(i, v, dst).wait()
        then(2)

    late = 1 - g.side
    loads = [pltpu.make_async_copy(x_in, vwq.at[late, pl.ds(0, tok), :], lead_sems.at[0]),
             pltpu.make_async_copy(dy_in, vwq.at[late, pl.ds(tok, tok), :], lead_sems.at[1]),
             pltpu.make_async_copy(vec, vvec, lead_sems.at[2]), pltpu.make_async_copy(bq, vbq, lead_sems.at[3]),
             pltpu.make_async_copy(b1, vb1, lead_sems.at[4])]
    for cp in loads:
        cp.start()
    for i in range(4):
        weight(g.side, i).start()
    for i in range(1, 4):
        weight(late, i).start()
    barrier = pltpu.get_barrier_semaphore()
    for i in range(n):
        pl.semaphore_signal(barrier, inc=1, device_id={'pp': jnp.int32(i)})
    for cp in loads:
        cp.wait()
    out[0] = vwq[late, 0:tok, :].T
    out[1] = vwq[late, tok:2 * tok, :].T

    @pl.when(g.outside)
    def _():
        slots[0, 0] = out[0]
    fed = [pltpu.make_async_copy(out.at[0], x_t, lead_sems.at[0]), pltpu.make_async_copy(out.at[1], dy_t, lead_sems.at[1])]
    for cp in fed:
        cp.start()
    weight(late, 0).start()
    pl.semaphore_wait(barrier, n)
    for cp in fed:
        cp.wait()

    heads_at = ((0, 0), (1, g.last))
    for k, head in heads_at:
        spot = g.place(g.me + k * (g.last - 2 * g.me))

        @pl.when(g.me != head)
        def _():
            remote(x_t, slots.at[0, spot], feed_send.at[0, k], recv_sems.at[0, 0, spot], jnp.int32(head)).start()
            remote(dy_t, feed.at[spot], feed_send.at[1, k], feed_recv.at[spot], jnp.int32(head)).start()

    for c in range(2):
        rows = [vvec[i, c:c + 1, :] for i in range(6)] + [vbq[c, i:i + 1, :] for i in range(3)]
        rows += [vb1[c:c + 1, i:i + d] for i in range(0, f, d)]
        rows = [v.astype(F32) for v in rows] + [jnp.zeros((LANES - len(rows), d), F32)]
        vcols[c] = jnp.concatenate(rows, 0).T.astype(BF16)
    acc[...] = jnp.zeros_like(acc)

    def settle(par, flag):
        @pl.when(flag == 1)
        def _():
            remote(out.at[par], slots.at[0, 0], send_sems.at[par], recv_sems.at[0, 0, 0], g.me).wait_send()

    def body(s, carry):
        kind, back, sec, m, c = g.step(s)
        nxt = jnp.minimum(s + 1, g.steps - 1)
        _, back2, _, m2, c2 = g.step(nxt)
        more = both(back2, s + 1 < g.steps)
        par = lax.rem(s, 2)
        inward = jnp.logical_or(kind == 0, kind == 2)
        outward = jnp.logical_not(inward)
        way = jnp.where(back, 1, 0)

        settle(par, carry[1])

        own = jnp.logical_or(both(outward, g.inside), both(kind == 0, m == 0, g.outside))

        @pl.when(jnp.logical_not(own))
        def _():
            remote(out.at[par], slots.at[sec, m], send_sems.at[par], recv_sems.at[way, sec, m], g.me).wait_recv()

        @pl.when(jnp.logical_not(back))
        def _():
            forward(c, m, slots.at[sec, m], out.at[par], jnp.logical_or(s == 0, both(kind == 1, m == 0)))

            @pl.when(more)
            def _():
                for i in (0, 2, 3, 4, 5):
                    fetch(i, c2, m2).start()

        @pl.when(back)
        def _():
            def then(i, at=None):
                @pl.when(more)
                def _():
                    fetch(i, c2, m2, at).start()

            backward(c, m, slots.at[sec, m], out.at[par], then)

        @pl.when(both(inward, g.inside))
        def _():
            slots[1 - sec, m] = out[par]

        @pl.when(both(inward, jnp.logical_not(g.inside)))
        def _():
            remote(out.at[par], slots.at[sec, m], send_sems.at[par], recv_sems.at[way, sec, m], g.inner).start()

        @pl.when(both(outward, jnp.logical_not(g.outside)))
        def _():
            remote(out.at[par], slots.at[sec, m], send_sems.at[par], recv_sems.at[way, sec, m], g.outer).start()

        owner = m + g.side * (g.last - 2 * m)
        done = both(outward, g.outside, m < g.half)
        for w, ref in ((0, y_out), (1, dx_out)):
            mine = both(done, way == w)

            @pl.when(both(mine, owner == g.me))
            def _():
                pltpu.make_async_copy(out.at[par], ref, send_sems.at[par]).start()

            @pl.when(both(mine, owner != g.me))
            def _():
                remote(out.at[par], ref, send_sems.at[par], final_sems.at[w], owner).start()

        @pl.when(both(kind == 1, g.outside))
        def _():
            @pl.when(m == 0)
            def _():
                pltpu.make_async_copy(dy_t, slots.at[1, m], recv_sems.at[1, 1, m]).start()

            @pl.when(m > 0)
            def _():
                remote(dy_t, feed.at[m], feed_send.at[1, 0], feed_recv.at[m], g.me).wait_recv()
                pltpu.make_async_copy(feed.at[m], slots.at[1, m], recv_sems.at[1, 1, m]).start()

        kept = jnp.logical_or(both(inward, g.inside), both(outward, g.outside, m >= g.half))
        return jnp.where(kept, 0, 1), carry[0]

    before, earlier = lax.fori_loop(0, g.steps, body, (jnp.int32(0), jnp.int32(0)))
    settle(g.steps % 2, earlier)
    settle((g.steps + 1) % 2, before)
    for k, head in heads_at:
        @pl.when(g.me != head)
        def _():
            remote(x_t, slots.at[0, 0], feed_send.at[0, k], recv_sems.at[0, 0, 0], jnp.int32(head)).wait_send()
            remote(dy_t, feed.at[0], feed_send.at[1, k], feed_recv.at[0], jnp.int32(head)).wait_send()

    @pl.when(jnp.logical_not(g.outside))
    def _():
        for w, ref in ((0, y_out), (1, dx_out)):
            remote(out.at[0], ref, send_sems.at[0], final_sems.at[w], g.me).wait_recv()

    cp = pltpu.make_async_copy(acc, sums, b_sems.at[0])
    cp.start()
    cp.wait()


def run_walk(n, heads, seq, x, dy, weights, vec, bq, b1):
    tok, d = x.shape
    f = weights[2].shape[2]
    prow = (tok // seq) * (heads // 2) * seq
    st, vm, dma = jax.ShapeDtypeStruct, pltpu.VMEM, pltpu.SemaphoreType.DMA
    act, tall, hid = ((d, tok), BF16), ((3 * d, tok), BF16), ((f, tok), BF16)
    outs = [st(*act)] * 2 + [st((2, n) + v, k) for v, k in (
        act, tall, act, ((prow, 2 * seq), F32), ((2 * f, tok // 2), F32), ((8, tok), F32), act, act, act, hid,
        act, hid, act, tall)] + [st((n, d, tok), BF16), st((2, d, LANES), F32)] + [st(*act)] * 2
    scratch = [vm(w.shape, w.dtype) for w in weights] + [vm((2, d, LANES), BF16)] + [vm(v.shape, v.dtype) for v in (vec, bq, b1)] + [
        vm((2, n, d, tok), BF16), vm((2, d, tok), BF16), vm(*act), vm(*tall), vm(*act), vm(*act), vm(*hid),
        vm((2 * f, tok // 2), F32), vm((d, tok), F32), vm((8, tok), F32), vm((2, d, LANES), F32),
        dma((2, len(weights))), dma((2, 2, n)), dma((2,)), dma((2,)), dma((2, 2)), dma((n,)), dma((10,)), dma((6,)), dma((4,)),
        dma((5,))]
    args = (x, dy, *weights, vec, bq, b1)
    return pl.pallas_call(
        functools.partial(walk_kernel, n, heads, seq), out_shape=outs, in_specs=[HBM] * len(args), out_specs=[HBM] * len(outs),
        scratch_shapes=scratch, name='walk',
        compiler_params=pltpu.CompilerParams(vmem_limit_bytes=VMEM_LIMIT, collective_id=0, has_side_effects=True),
    )(*args)


PAIR = 2


def grads_kernel(n, *refs):
    ins, (y_t, dx_t, sums), refs = refs[:8], refs[8:11], refs[11:]
    outs, (b1_out, y_out, dx_out, vec_out, bq_out), refs = refs[:4], refs[4:9], refs[9:]
    accs, biases, refs = refs[:4], refs[4:7], refs[7:]
    buf, va, vb, vsum, b1_row, vec_rows, bq_rows, in_sems, out_sems, end_sems = refs
    steps = n // PAIR
    tok = buf.shape[3]

    def fetches(c, k, j):
        slot = lax.rem(j, 2)
        rows, cols = ins[2 * k].shape[2], ins[2 * k + 1].shape[2]
        at = pl.ds(j * PAIR, PAIR)
        return (pltpu.make_async_copy(ins[2 * k].at[c, at], buf.at[slot, :, pl.ds(0, rows), :], in_sems.at[slot, 0]),
                pltpu.make_async_copy(ins[2 * k + 1].at[c, at], buf.at[slot, :, pl.ds(rows, cols), :], in_sems.at[slot, 1]))

    def begin(c, k, j):
        for cp in fetches(c, k, j):
            cp.start()

    def results(c, k):
        cps = [pltpu.make_async_copy(accs[k], outs[k].at[c], out_sems.at[k])]
        return cps

    begin(jnp.int32(0), 0, jnp.int32(0))
    acts = ((y_t, y_out), (dx_t, dx_out))
    loads = [pltpu.make_async_copy(h, va.at[i], end_sems.at[i]) for i, (h, _) in enumerate(acts)]
    loads.append(pltpu.make_async_copy(sums, vsum, end_sems.at[2]))
    for cp in loads:
        cp.start()
    for cp in loads:
        cp.wait()
    for i in range(2):
        vb[i] = va[i].T
    turned = [pltpu.make_async_copy(vb.at[i], h, end_sems.at[i]) for i, (_, h) in enumerate(acts)]
    for cp in turned:
        cp.start()
    for i in range(2):
        part = vsum[i].T
        for row, src in ((0, 0), (1, 1), (3, 2), (4, 3)):
            vec_rows[i, row] = part[src:src + 1, :]
        for row in range(3):
            bq_rows[i, row] = part[4 + row:5 + row, :]

    def stage(c, carry):
        for k in range(4):
            rows, cols = ins[2 * k].shape[2], ins[2 * k + 1].shape[2]

            def step(j, carry, k=k, rows=rows, cols=cols):
                @pl.when(j + 1 < steps)
                def _():
                    begin(c, k, j + 1)

                @pl.when(j + 1 == steps)
                def _():
                    if k < 3:
                        begin(c, k + 1, jnp.int32(0))
                    else:
                        @pl.when(c == 0)
                        def _():
                            begin(jnp.int32(1), 0, jnp.int32(0))

                @pl.when(jnp.logical_and(j == 0, c == 1))
                def _():
                    for cp in results(jnp.int32(0), k):
                        cp.wait()

                for cp in fetches(c, k, j):
                    cp.wait()
                slot = lax.rem(j, 2)
                later = j > 0
                for i in range(0, rows, CH):
                    z = jnp.where(later, accs[k][i:i + CH, :], 0.0)
                    if i == 0 and k < 3:
                        e = jnp.where(later, biases[k][...], 0.0)
                    for q in range(PAIR):
                        x = buf[slot, q, i:i + CH, :]
                        if i == 0 and k < 3:
                            x = jnp.concatenate([x, jnp.ones((16, tok), BF16)], 0)
                        v = dot(x, buf[slot, q, rows:rows + cols, :], 1, 1).astype(BF16).astype(F32)
                        z = z + v[:CH]
                        if i == 0 and k < 3:
                            e = e + v[CH:CH + 8]
                    accs[k][i:i + CH, :] = z
                    if i == 0 and k < 3:
                        biases[k][...] = e
                return carry

            lax.fori_loop(0, steps, step, 0)
            for cp in results(c, k):
                cp.start()
        b1_row[c] = biases[0][0:1, :]
        vec_rows[c, 5] = biases[1][0:1, :]
        vec_rows[c, 2] = biases[2][0:1, :]
        return carry

    lax.fori_loop(0, 2, stage, 0)
    rows = [pltpu.make_async_copy(v, h, end_sems.at[2 + i])
            for i, (v, h) in enumerate(((b1_row, b1_out), (vec_rows, vec_out), (bq_rows, bq_out)))]
    for cp in rows:
        cp.start()
    for cp in rows + turned:
        cp.wait()
    for k in range(4):
        for cp in results(jnp.int32(1), k):
            cp.wait()


def run_grads(pairs, y_t, dx_t, sums):
    n, tok = pairs[0][0].shape[1], pairs[0][0].shape[3]
    sizes = [(a.shape[2], b.shape[2]) for a, b in pairs]
    d, f = sizes[0]
    st, vm, dma = jax.ShapeDtypeStruct, pltpu.VMEM, pltpu.SemaphoreType.DMA
    most = max(a + b for a, b in sizes)
    rows = [((2, 1, f), F32), ((2, 6, 1, d), F32), ((2, 3, 1, d), F32)]
    return pl.pallas_call(
        functools.partial(grads_kernel, n),
        out_shape=[st((2,) + v, F32) for v in sizes] + [st(*rows[0]), st((tok, d), BF16), st((tok, d), BF16), st(*rows[1]),
                                                        st(*rows[2])],
        in_specs=[HBM] * 11, out_specs=[HBM] * 9,
        scratch_shapes=[vm(v, F32) for v in sizes] + [vm((8, v[1]), F32) for v in sizes[:3]] + [
            vm((2, PAIR, most, tok), BF16), vm((2, d, tok), BF16), vm((2, tok, d), BF16), vm(sums.shape, F32)] + [
            vm(*v) for v in rows] + [dma((2, 2)), dma((4,)), dma((5,))],
        name='weight_grads', compiler_params=pltpu.CompilerParams(vmem_limit_bytes=VMEM_LIMIT),
    )(*[v for p in pairs for v in p], y_t, dx_t, sums)


def solution(mesh):
    data_spec = P(('dp', 'pp'))
    weight_spec = P('pp')

    def per_device(x, dy, w_qkv, w_attn, w_fc, w_proj, b_qkv, b_fc, vec_d):
        _, batch, seq, d = x.shape
        heads = w_qkv.shape[5]
        tok = batch * seq

        weights = (w_qkv.reshape(2, d, 3 * d).transpose(0, 2, 1), w_attn.reshape(2, d, d), w_fc[0, :, 0], w_proj[0, :, 0])
        y_t, dx_t, *stash = run_walk(
            mesh.shape['pp'], heads, seq, x.reshape(tok, d), dy.reshape(tok, d), weights,
            vec_d[0, :, 0].transpose(1, 0, 2), b_qkv.reshape(2, 3, d), b_fc[0, :, 0])
        as_, os_, bs, us, dys, dgs, drs, dts, _, sums = stash[6:16]
        g1, g2, go, gq, gb1, y, dx, gv, gbq = run_grads(((bs, dgs), (us, dys), (os_, drs), (dts, as_)), y_t, dx_t, sums)
        return (y.reshape(x.shape), dx.reshape(x.shape),
                gq.transpose(0, 2, 1).reshape(w_qkv.shape), go.reshape(w_attn.shape), g1.reshape(w_fc.shape),
                g2.reshape(w_proj.shape), gbq.reshape(b_qkv.shape), gb1.reshape(b_fc.shape), gv.reshape(vec_d.shape))

    return jax.shard_map(per_device, mesh=mesh, in_specs=(data_spec, data_spec) + (weight_spec,) * 7,
                         out_specs=(data_spec, data_spec) + (data_spec,) * 7, check_vma=False)
```

```python
import functools

import jax
import jax.numpy as jnp
from jax import lax
from jax.experimental import pallas as pl
from jax.experimental.pallas import tpu as pltpu
from jax.sharding import PartitionSpec as P

EPS = 1e-5
F32 = jnp.float32
BF16 = jnp.bfloat16
LANES = 128
ROWS = 96
CH = 256
SKEW = 8
K0 = 0.7978845608028654
K1 = K0 * 0.044715
VMEM_LIMIT = 67043328
HBM = pl.BlockSpec(memory_space=pl.ANY)


def dot(lhs, rhs, lc=1, rc=0):
    return lax.dot_general(lhs, rhs, (((lc,), (rc,)), ((), ())), preferred_element_type=F32)


def rows_sum(v):
    r, t = v.shape
    return jnp.sum(v.reshape(r // 8, 8, t), axis=0)


def column(cols, lane, row, count):
    return cols[row:row + count, lane:lane + 1].astype(F32)


def lane_fold(v):
    return functools.reduce(jnp.add, [v[:, k:k + LANES] for k in range(0, v.shape[1], LANES)])


def rounded(v):
    return v.astype(BF16).astype(F32)


def token_sum(v):
    return rounded(jnp.sum(lane_fold(v), axis=1, keepdims=True))


def block_diag(a, b):
    z = jnp.zeros_like(a)
    return jnp.concatenate([jnp.concatenate([a, z], 1), jnp.concatenate([z, b], 1)], 0)


def f_norm(src, cols, lane, dst, stats, row, hold):
    d, t = src.shape
    acc = jnp.zeros((8, t), F32)
    for i in range(0, d, ROWS):
        acc += rows_sum(src[i:i + ROWS, :].astype(F32))
    mean = jnp.sum(acc, axis=0, keepdims=True) * (1.0 / d)
    acc = jnp.zeros((8, t), F32)
    for i in range(0, d, ROWS):
        c = src[i:i + ROWS, :].astype(F32) - mean
        hold[i:i + ROWS, :] = c
        acc += rows_sum(c * c)
    rstd = lax.rsqrt(jnp.sum(acc, axis=0, keepdims=True) * (1.0 / d) + EPS)
    for i in range(0, d, ROWS):
        c = hold[i:i + ROWS, :] * rstd
        dst[i:i + ROWS, :] = (c * column(cols, lane, i, ROWS) + column(cols, lane + 1, i, ROWS)).astype(BF16)
    stats[row:row + 1, :] = mean
    stats[row + 1:row + 2, :] = rstd


def token_totals(v):
    return dot(v, jnp.ones((v.shape[1], LANES), BF16))


def b_norm(dn, src, cols, gain, skip, dst, stats, row, acc, lane, hold):
    d, t = src.shape
    mean = stats[row:row + 1, :]
    rstd = stats[row + 1:row + 2, :]
    at = lax.broadcasted_iota(jnp.int32, (ROWS, LANES), 1)
    m1 = dot(cols[...], dn[...], 0, 0)[gain:gain + 1, :] * (1.0 / d)
    shift = token_totals(dn[...])
    s2 = jnp.zeros((8, t), F32)
    for i in range(0, d, ROWS):
        c = (src[i:i + ROWS, :].astype(F32) - mean) * rstd
        hold[i:i + ROWS, :] = c
        w = dn[i:i + ROWS, :].astype(F32) * c
        s2 += rows_sum(w * column(cols, gain, i, ROWS))
        acc[i:i + ROWS, :] += jnp.where(at == lane, token_sum(w), jnp.where(at == lane + 1, rounded(shift[i:i + ROWS]), 0.0))
    m2 = jnp.sum(s2, axis=0, keepdims=True) * (1.0 / d)
    for i in range(0, d, ROWS):
        g = dn[i:i + ROWS, :].astype(F32) * column(cols, gain, i, ROWS)
        z = (g - m1 - hold[i:i + ROWS, :] * m2) * rstd + skip[i:i + ROWS, :].astype(F32)
        dst[i:i + ROWS, :] = z.astype(BF16)


def skewed(jobs, first, second):
    pending = []
    for job in jobs:
        pending.append((job, first(*job)))
        if len(pending) > SKEW:
            job, v = pending.pop(0)
            second(*job, v)
    for job, v in pending:
        second(*job, v)


def f_heads(t, o, p, heads, seq, after):
    d, n = o.shape
    head = d // heads
    two = 2 * head
    pairs = heads // 2
    key = lax.broadcasted_iota(jnp.int32, (seq, 2 * seq), 0)
    qry = lax.rem(lax.broadcasted_iota(jnp.int32, (seq, 2 * seq), 1), seq)
    ok = key <= qry
    c = (head ** -0.5) * 1.4426950408889634

    def score(b, j):
        r0, lanes = two * j, slice(b * seq, (b + 1) * seq)
        q = t[r0:r0 + two, lanes]
        return dot(t[d + r0:d + r0 + two, lanes], block_diag(q[:head], q[head:]), 0, 0)

    def mix(b, j, s):
        r0, lanes = two * j, slice(b * seq, (b + 1) * seq)
        s = jnp.where(ok, s, -1e30)
        m = jnp.max(s, axis=0, keepdims=True)
        e = jnp.exp2((s - m) * c)
        e = e * (1.0 / jnp.sum(e, axis=0, keepdims=True))
        k0 = (b * pairs + j) * seq
        p[k0:k0 + seq, :] = e
        x = dot(t[2 * d + r0:2 * d + r0 + two, lanes], e.astype(BF16))
        o[r0:r0 + head, lanes] = x[:head, :seq].astype(BF16)
        o[r0 + head:r0 + two, lanes] = x[head:, seq:].astype(BF16)
        if j == pairs - 1:
            after(b)

    skewed([(b, j) for b in range(n // seq) for j in range(pairs)], score, mix)


def b_heads(t, do, p, heads, seq, after):
    d, n = do.shape
    head = d // heads
    two = 2 * head
    pairs = heads // 2
    scale = head ** -0.5

    def first(b, j):
        r0, lanes = two * j, slice(b * seq, (b + 1) * seq)
        z = do[r0:r0 + two, lanes]
        return dot(t[2 * d + r0:2 * d + r0 + two, lanes], block_diag(z[:head], z[head:]), 0, 0)

    def diag(r0, lanes, x, k):
        t[r0:r0 + head, lanes] = (x[:head, :seq] * k).astype(BF16)
        t[r0 + head:r0 + two, lanes] = (x[head:, seq:] * k).astype(BF16)

    def second(b, j, dp):
        r0, lanes = two * j, slice(b * seq, (b + 1) * seq)
        k0 = (b * pairs + j) * seq
        e = p[k0:k0 + seq, :]
        w = e * dp
        ds = (w - e * jnp.sum(w, axis=0, keepdims=True)).astype(BF16)
        eb = e.astype(BF16)
        q, k = t[r0:r0 + two, lanes], t[d + r0:d + r0 + two, lanes]
        tall = jnp.concatenate([ds[:, :seq], ds[:, seq:]], 0)
        dq, dk = dot(k, ds), dot(q, tall, 1, 1)
        tall = jnp.concatenate([eb[:, :seq], eb[:, seq:]], 0)
        dv = dot(do[r0:r0 + two, lanes], tall, 1, 1)
        diag(r0, lanes, dq, scale)
        diag(d + r0, lanes, dk, scale)
        diag(2 * d + r0, lanes, dv, 1.0)
        if j == pairs - 1:
            after(b)

    skewed([(b, j) for b in range(n // seq) for j in range(pairs)], first, second)


def gelu_and_slope(x):
    x2 = x * x
    hp = 0.5 * jnp.tanh(x * (x2 * K1 + K0)) + 0.5
    u = x * hp
    return u, hp + (u - u * hp) * (x2 * (6.0 * K1) + 2.0 * K0)


ORDERS = (
    (0, 1, 2, 3, 4, 5, 6, 7, 8, 16, 9, 17, 10, 18, 11, 19, 12, 20, 13, 21, 14, 22, 15, 23, 24, 25, 26, 27, 28, 29, 30, 31),
    (0, 1, 2, 3, 4, 5, 6, 7, 8, 9, 16, 10, 17, 11, 12, 18, 13, 19, 14, 20, 15, 21, 24, 22, 25, 23, 26, 27, 28, 29, 30, 31),
    (0, 1, 2, 3, 8, 4, 9, 5, 10, 6, 11, 7, 12, 16, 13, 17, 14, 18, 15, 19, 24, 20, 25, 21, 26, 22, 27, 23, 28, 29, 30, 31),
    (0, 8, 1, 9, 2, 10, 3, 11, 4, 12, 5, 13, 6, 14, 7, 15, 16, 24, 17, 25, 18, 26, 19, 27, 20, 28, 21, 29, 22, 30, 23, 31),
)


class Group:
    def __init__(self, n):
        self.n, self.half, self.last, self.steps = n, n // 2, n - 1, 4 * n
        self.me = lax.axis_index('pp')
        self.side = self.me // self.half
        self.depth = self.me + self.side * (self.last - 2 * self.me)
        self.inner = self.me + 1 - 2 * self.side
        self.outer = self.me - 1 + 2 * self.side
        self.inside = self.depth == self.half - 1
        self.outside = self.depth == 0
        self.codes = []
        for k in range(self.steps):
            v = jnp.int32(ORDERS[0][k])
            for i in range(1, self.half):
                v = jnp.where(self.depth == i, ORDERS[i][k], v)
            self.codes.append(v)

    def place(self, i):
        far = lax.rem(i - self.half + self.half // 2, self.half) + self.half
        return jnp.where(i < self.half, i, far)

    def step(self, s):
        code = self.codes[0]
        for k in range(1, self.steps):
            code = jnp.where(s == k, self.codes[k], code)
        kind = code // self.n
        m = code - self.n * kind
        back = kind >= 2
        sec = jnp.where(jnp.logical_or(kind == 1, kind == 2), 1, 0)
        c = jnp.where(sec == 1, 1 - self.side, self.side)
        return kind, back, sec, m, c


def both(a, *rest):
    return functools.reduce(jnp.logical_and, rest, a)


def walk_kernel(n, heads, seq, x_in, dy_in, wq, wo, w1, w2, vec, bq, b1,
                y_out, dx_out, hs, ts, rs, ps, gs, ss, as_, os_, bs, us, dys, dgs, drs, dts, feed, sums, x_t, dy_t,
                vwq, vwo, vw1, vw2, vcols, vvec, vbq, vb1, slots, out, a, t, o, r, u, pg, ya, stats, acc,
                load_sems, recv_sems, send_sems, final_sems, feed_send, feed_recv, f_sems, b_in, b_sems, lead_sems):
    g = Group(n)
    d, tok = a.shape
    f = u.shape[0]
    half = tok // 2
    prow = ps.shape[2]
    part = prow // (tok // seq)
    weights = ((wq, vwq), (wo, vwo), (w1, vw1), (w2, vw2))

    def weight(c, i):
        h, v = weights[i]
        return pltpu.make_async_copy(h.at[c], v.at[c], load_sems.at[c, i])

    def remote(src, dst, send, recv, dev):
        return pltpu.make_async_remote_copy(src_ref=src, dst_ref=dst, send_sem=send, recv_sem=recv, device_id={'pp': dev})

    def saver(c, m, sems):
        def copy(i, v, dst, at=None):
            hbm = dst.at[c, m]
            if at is not None:
                v, hbm = v.at[pl.ds(*at), :], hbm.at[pl.ds(*at), :]
            return pltpu.make_async_copy(v, hbm, sems.at[i])
        return copy

    def fetch(i, c, m, at=None):
        hbm, v = ((gs, pg), (ps, pg.at[pl.ds(0, prow), :]), (ts, t), (rs, r), (hs, a), (ss, stats))[i]
        hbm = hbm.at[c, m]
        if at is not None:
            hbm, v = hbm.at[pl.ds(*at), :], v.at[pl.ds(*at), :]
        return pltpu.make_async_copy(hbm, v, b_in.at[i])

    def forward(c, m, x, y):
        copy = saver(c, m, f_sems)
        cv = vcols.at[c]
        copy(0, x, hs).start()
        f_norm(x, cv, 0, a, stats, 0, ya)
        copy(1, a, as_).start()
        v = a[...]
        for i in range(0, 3 * d, CH):
            z = dot(vwq[c, i:i + CH, :], v) + column(cv, 6 + i // d, i % d, CH)
            t[i:i + CH, :] = z.astype(BF16)
        copy(2, t, ts).start()
        f_heads(t, o, pg, heads, seq, lambda b: copy(4, pg, ps, (b * part, part)).start())
        copy(3, o, os_).start()
        v = o[...]
        for i in range(0, d, CH):
            z = dot(vwo[c, :, i:i + CH], v, 0, 0) + column(cv, 2, i, CH) + x[i:i + CH, :].astype(F32)
            r[i:i + CH, :] = z.astype(BF16)
        copy(5, r, rs).start()
        copy(1, a, as_).wait()
        f_norm(r, cv, 3, a, stats, 2, ya)
        copy(6, a, bs).start()
        copy(7, stats, ss).start()
        copy(4, pg.at[pl.ds(0, prow), :], ps).wait()
        v = a[...]

        def up(k):
            for i in range(k * d, (k + 1) * d, CH):
                h = dot(vw1[c, :, i:i + CH], v, 0, 0) + column(cv, 9 + k, i % d, CH)
                uu, slope = gelu_and_slope(h)
                u[i:i + CH, :] = uu.astype(BF16)
                pg[2 * i:2 * i + CH, :] = slope[:, :half]
                pg[2 * i + CH:2 * i + 2 * CH, :] = slope[:, half:]
                copy(8, u, us, (i, CH)).start()
                copy(9, pg, gs, (2 * i, 2 * CH)).start()

        def down(k):
            w = u[k * d:(k + 1) * d, :]
            for i in range(0, d, CH):
                z = dot(vw2[c, k * d:(k + 1) * d, i:i + CH], w, 0, 0)
                z += (column(cv, 5, i, CH) + r[i:i + CH, :].astype(F32)) if k == 0 else ya[i:i + CH, :]
                if (k + 1) * d < f:
                    ya[i:i + CH, :] = z
                else:
                    y[i:i + CH, :] = z.astype(BF16)

        up(0)
        for k in range(1, f // d):
            up(k)
            down(k - 1)
        down(f // d - 1)
        for i, v, dst in ((0, x, hs), (2, t, ts), (3, o, os_), (5, r, rs), (6, a, bs), (7, stats, ss), (8, u, us),
                          (9, pg, gs)):
            copy(i, v, dst).wait()

    def backward(c, m, dy, y, then):
        copy = saver(c, m, b_sems)
        cv = vcols.at[c]
        copy(0, dy, dys).start()
        fetch(0, c, m).wait()
        v = dy[...]
        for i in range(0, f, CH):
            du = dot(vw2[c, i:i + CH, :], v).astype(BF16).astype(F32)
            u[i:i + CH, :half] = (du[:, :half] * pg[2 * i:2 * i + CH, :]).astype(BF16)
            u[i:i + CH, half:] = (du[:, half:] * pg[2 * i + CH:2 * i + 2 * CH, :]).astype(BF16)
        fetch(1, c, m).start()
        then(0, (prow, 2 * f - prow))
        copy(1, u, dgs).start()
        v = u[...]
        for i in range(0, d, CH):
            y[i:i + CH, :] = dot(vw1[c, i:i + CH, :], v).astype(BF16)
        for i in (3, 4, 5):
            fetch(i, c, m).wait()
        b_norm(y, r, cv, 3, dy, o, stats, 2, acc.at[c], 2, ya)
        then(3)
        copy(2, o, drs).start()
        v = o[...]
        for i in range(0, d, CH):
            y[i:i + CH, :] = dot(vwo[c, i:i + CH, :], v).astype(BF16)
        for i in (1, 2):
            fetch(i, c, m).wait()
        b_heads(t, y, pg, heads, seq, lambda b: then(0, (b * part, part)))
        copy(3, t, dts).start()
        v = t[...]
        at = lax.broadcasted_iota(jnp.int32, (ROWS, LANES), 1)
        for i in range(0, d, CH):
            y[i:i + CH, :] = dot(vwq[c, :, i:i + CH], v, 0, 0).astype(BF16)
        b_norm(y, a, cv, 0, o, y, stats, 0, acc.at[c], 0, ya)
        for i in range(0, d, ROWS):
            e = 0.0
            for k in range(3):
                e = jnp.where(at == 4 + k, token_sum(t[k * d + i:k * d + i + ROWS, :].astype(F32)), e)
            acc[c, i:i + ROWS, :] += e
        then(4)
        then(5)
        for i, v, dst in ((0, dy, dys), (1, u, dgs), (2, o, drs), (3, t, dts)):
            copy(i, v, dst).wait()
        then(2)

    late = 1 - g.side
    loads = [pltpu.make_async_copy(x_in, vwq.at[late, pl.ds(0, tok), :], lead_sems.at[0]),
             pltpu.make_async_copy(dy_in, vwq.at[late, pl.ds(tok, tok), :], lead_sems.at[1]),
             pltpu.make_async_copy(vec, vvec, lead_sems.at[2]), pltpu.make_async_copy(bq, vbq, lead_sems.at[3]),
             pltpu.make_async_copy(b1, vb1, lead_sems.at[4])]
    for cp in loads:
        cp.start()
    for i in range(4):
        weight(g.side, i).start()
    for i in range(1, 4):
        weight(late, i).start()
    barrier = pltpu.get_barrier_semaphore()
    for i in range(n):
        pl.semaphore_signal(barrier, inc=1, device_id={'pp': jnp.int32(i)})
    for cp in loads:
        cp.wait()
    out[0] = vwq[late, 0:tok, :].T
    out[1] = vwq[late, tok:2 * tok, :].T

    @pl.when(g.outside)
    def _():
        slots[0, 0] = out[0]
    fed = [pltpu.make_async_copy(out.at[0], x_t, lead_sems.at[0]), pltpu.make_async_copy(out.at[1], dy_t, lead_sems.at[1])]
    for cp in fed:
        cp.start()
    weight(late, 0).start()
    pl.semaphore_wait(barrier, n)
    for cp in fed:
        cp.wait()

    heads_at = ((0, 0), (1, g.last))
    for k, head in heads_at:
        spot = g.place(g.me + k * (g.last - 2 * g.me))

        @pl.when(g.me != head)
        def _():
            remote(x_t, slots.at[0, spot], feed_send.at[0, k], recv_sems.at[0, 0, spot], jnp.int32(head)).start()
            remote(dy_t, feed.at[spot], feed_send.at[1, k], feed_recv.at[spot], jnp.int32(head)).start()

    for c in range(2):
        rows = [vvec[i, c:c + 1, :] for i in range(6)] + [vbq[c, i:i + 1, :] for i in range(3)]
        rows += [vb1[c:c + 1, i:i + d] for i in range(0, f, d)]
        rows = [v.astype(F32) for v in rows] + [jnp.zeros((LANES - len(rows), d), F32)]
        vcols[c] = jnp.concatenate(rows, 0).T.astype(BF16)
    acc[...] = jnp.zeros_like(acc)

    def settle(par, flag):
        @pl.when(flag == 1)
        def _():
            remote(out.at[par], slots.at[0, 0], send_sems.at[par], recv_sems.at[0, 0, 0], g.me).wait_send()

    def body(s, carry):
        kind, back, sec, m, c = g.step(s)
        nxt = jnp.minimum(s + 1, g.steps - 1)
        _, back2, _, m2, c2 = g.step(nxt)
        more = both(back2, s + 1 < g.steps)
        par = lax.rem(s, 2)
        inward = jnp.logical_or(kind == 0, kind == 2)
        outward = jnp.logical_not(inward)
        way = jnp.where(back, 1, 0)

        @pl.when(jnp.logical_or(s == 0, both(kind == 1, m == 0)))
        def _():
            for i in range(4):
                weight(c, i).wait()

        settle(par, carry[1])

        own = jnp.logical_or(both(outward, g.inside), both(kind == 0, m == 0, g.outside))

        @pl.when(jnp.logical_not(own))
        def _():
            remote(out.at[par], slots.at[sec, m], send_sems.at[par], recv_sems.at[way, sec, m], g.me).wait_recv()

        @pl.when(jnp.logical_not(back))
        def _():
            forward(c, m, slots.at[sec, m], out.at[par])

            @pl.when(more)
            def _():
                for i in (0, 2, 3, 4, 5):
                    fetch(i, c2, m2).start()

        @pl.when(back)
        def _():
            def then(i, at=None):
                @pl.when(more)
                def _():
                    fetch(i, c2, m2, at).start()

            backward(c, m, slots.at[sec, m], out.at[par], then)

        @pl.when(both(inward, g.inside))
        def _():
            slots[1 - sec, m] = out[par]

        @pl.when(both(inward, jnp.logical_not(g.inside)))
        def _():
            remote(out.at[par], slots.at[sec, m], send_sems.at[par], recv_sems.at[way, sec, m], g.inner).start()

        @pl.when(both(outward, jnp.logical_not(g.outside)))
        def _():
            remote(out.at[par], slots.at[sec, m], send_sems.at[par], recv_sems.at[way, sec, m], g.outer).start()

        owner = m + g.side * (g.last - 2 * m)
        done = both(outward, g.outside, m < g.half)
        for w, ref in ((0, y_out), (1, dx_out)):
            mine = both(done, way == w)

            @pl.when(both(mine, owner == g.me))
            def _():
                pltpu.make_async_copy(out.at[par], ref, send_sems.at[par]).start()

            @pl.when(both(mine, owner != g.me))
            def _():
                remote(out.at[par], ref, send_sems.at[par], final_sems.at[w], owner).start()

        @pl.when(both(kind == 1, g.outside))
        def _():
            @pl.when(m == 0)
            def _():
                pltpu.make_async_copy(dy_t, slots.at[1, m], recv_sems.at[1, 1, m]).start()

            @pl.when(m > 0)
            def _():
                remote(dy_t, feed.at[m], feed_send.at[1, 0], feed_recv.at[m], g.me).wait_recv()
                pltpu.make_async_copy(feed.at[m], slots.at[1, m], recv_sems.at[1, 1, m]).start()

        kept = jnp.logical_or(both(inward, g.inside), both(outward, g.outside, m >= g.half))
        return jnp.where(kept, 0, 1), carry[0]

    before, earlier = lax.fori_loop(0, g.steps, body, (jnp.int32(0), jnp.int32(0)))
    settle(g.steps % 2, earlier)
    settle((g.steps + 1) % 2, before)
    for k, head in heads_at:
        @pl.when(g.me != head)
        def _():
            remote(x_t, slots.at[0, 0], feed_send.at[0, k], recv_sems.at[0, 0, 0], jnp.int32(head)).wait_send()
            remote(dy_t, feed.at[0], feed_send.at[1, k], feed_recv.at[0], jnp.int32(head)).wait_send()

    @pl.when(jnp.logical_not(g.outside))
    def _():
        for w, ref in ((0, y_out), (1, dx_out)):
            remote(out.at[0], ref, send_sems.at[0], final_sems.at[w], g.me).wait_recv()

    cp = pltpu.make_async_copy(acc, sums, b_sems.at[0])
    cp.start()
    cp.wait()


def run_walk(n, heads, seq, x, dy, weights, vec, bq, b1):
    tok, d = x.shape
    f = weights[2].shape[2]
    prow = (tok // seq) * (heads // 2) * seq
    st, vm, dma = jax.ShapeDtypeStruct, pltpu.VMEM, pltpu.SemaphoreType.DMA
    act, tall, hid = ((d, tok), BF16), ((3 * d, tok), BF16), ((f, tok), BF16)
    outs = [st(*act)] * 2 + [st((2, n) + v, k) for v, k in (
        act, tall, act, ((prow, 2 * seq), F32), ((2 * f, tok // 2), F32), ((8, tok), F32), act, act, act, hid,
        act, hid, act, tall)] + [st((n, d, tok), BF16), st((2, d, LANES), F32)] + [st(*act)] * 2
    scratch = [vm(w.shape, w.dtype) for w in weights] + [vm((2, d, LANES), BF16)] + [vm(v.shape, v.dtype) for v in (vec, bq, b1)] + [
        vm((2, n, d, tok), BF16), vm((2, d, tok), BF16), vm(*act), vm(*tall), vm(*act), vm(*act), vm(*hid),
        vm((2 * f, tok // 2), F32), vm((d, tok), F32), vm((8, tok), F32), vm((2, d, LANES), F32),
        dma((2, len(weights))), dma((2, 2, n)), dma((2,)), dma((2,)), dma((2, 2)), dma((n,)), dma((10,)), dma((6,)), dma((4,)),
        dma((5,))]
    args = (x, dy, *weights, vec, bq, b1)
    return pl.pallas_call(
        functools.partial(walk_kernel, n, heads, seq), out_shape=outs, in_specs=[HBM] * len(args), out_specs=[HBM] * len(outs),
        scratch_shapes=scratch, name='walk',
        compiler_params=pltpu.CompilerParams(vmem_limit_bytes=VMEM_LIMIT, collective_id=0, has_side_effects=True),
    )(*args)


PAIR = 2


def grads_kernel(n, *refs):
    ins, (y_t, dx_t, sums), refs = refs[:8], refs[8:11], refs[11:]
    outs, (b1_out, y_out, dx_out, vec_out, bq_out), refs = refs[:4], refs[4:9], refs[9:]
    accs, biases, refs = refs[:4], refs[4:7], refs[7:]
    buf, va, vb, vsum, b1_row, vec_rows, bq_rows, in_sems, out_sems, end_sems = refs
    steps = n // PAIR
    tok = buf.shape[3]
    d = y_t.shape[0]

    def fetches(c, k, j):
        slot = lax.rem(j, 2)
        rows, cols = ins[2 * k].shape[2], ins[2 * k + 1].shape[2]
        at = pl.ds(j * PAIR, PAIR)
        return (pltpu.make_async_copy(ins[2 * k].at[c, at], buf.at[slot, :, pl.ds(0, rows), :], in_sems.at[slot, 0]),
                pltpu.make_async_copy(ins[2 * k + 1].at[c, at], buf.at[slot, :, pl.ds(rows, cols), :], in_sems.at[slot, 1]))

    def begin(c, k, j):
        for cp in fetches(c, k, j):
            cp.start()

    def results(c, k):
        cps = [pltpu.make_async_copy(accs[k], outs[k].at[c], out_sems.at[k])]
        return cps

    begin(jnp.int32(0), 0, jnp.int32(0))
    acts = ((y_t, y_out), (dx_t, dx_out))
    loads = [pltpu.make_async_copy(h, va.at[i], end_sems.at[i]) for i, (h, _) in enumerate(acts)]
    loads.append(pltpu.make_async_copy(sums, vsum, end_sems.at[2]))
    for cp in loads:
        cp.start()
    for cp in loads:
        cp.wait()
    for i in range(2):
        vb[i] = va[i].T
    turned = [pltpu.make_async_copy(vb.at[i], h, end_sems.at[i]) for i, (_, h) in enumerate(acts)]
    for cp in turned:
        cp.start()
    for i in range(2):
        part = vsum[i].T
        for row, src in ((0, 0), (1, 1), (3, 2), (4, 3)):
            vec_rows[i, row] = part[src:src + 1, :]
        for row in range(3):
            bq_rows[i, row] = part[4 + row:5 + row, :]

    def stage(c, carry):
        for k in range(4):
            rows, cols = ins[2 * k].shape[2], ins[2 * k + 1].shape[2]

            def step(j, carry, k=k, rows=rows, cols=cols):
                @pl.when(j + 1 < steps)
                def _():
                    begin(c, k, j + 1)

                @pl.when(j + 1 == steps)
                def _():
                    if k < 3:
                        begin(c, k + 1, jnp.int32(0))
                    else:
                        @pl.when(c == 0)
                        def _():
                            begin(jnp.int32(1), 0, jnp.int32(0))

                @pl.when(jnp.logical_and(j == 0, c == 1))
                def _():
                    for cp in results(jnp.int32(0), k):
                        cp.wait()

                for cp in fetches(c, k, j):
                    cp.wait()
                slot = lax.rem(j, 2)
                later = j > 0
                parts = 2 if max(rows, cols) > 3 * d else 1
                tall = rows > cols
                height, width = (rows // parts, cols) if tall else (rows, cols // parts)

                def block(h, carry):
                    top = pl.multiple_of(h * height, CH) if tall and parts > 1 else 0
                    left = pl.multiple_of(h * width, CH) if not tall and parts > 1 else 0
                    w = [buf[slot, q, pl.ds(rows + left, width), :] for q in range(PAIR)]
                    for i in range(0, height, CH):
                        at = (pl.ds(top + i, CH), pl.ds(left, width))
                        z = jnp.where(later, accs[k][at], 0.0)
                        edge = i == 0 and k < 3
                        if edge:
                            e = jnp.where(later, biases[k][:, at[1]], 0.0)
                        for q in range(PAIR):
                            x = buf[slot, q, pl.ds(top + i, CH), :]
                            if edge:
                                x = jnp.concatenate([x, jnp.ones((16, tok), BF16)], 0)
                            v = rounded(dot(x, w[q], 1, 1))
                            z = z + v[:CH]
                            if edge:
                                e = e + v[CH:CH + 8]
                        accs[k][at] = z
                        if edge and tall and parts > 1:
                            biases[k][:, at[1]] = jnp.where(h == 0, e, biases[k][:, at[1]])
                        elif edge:
                            biases[k][:, at[1]] = e
                    return carry

                if parts > 1:
                    lax.fori_loop(0, parts, block, 0)
                else:
                    block(0, 0)
                return carry

            lax.fori_loop(0, steps, step, 0)
            for cp in results(c, k):
                cp.start()
        b1_row[c] = biases[0][0:1, :]
        vec_rows[c, 5] = biases[1][0:1, :]
        vec_rows[c, 2] = biases[2][0:1, :]
        return carry

    lax.fori_loop(0, 2, stage, 0)
    rows = [pltpu.make_async_copy(v, h, end_sems.at[2 + i])
            for i, (v, h) in enumerate(((b1_row, b1_out), (vec_rows, vec_out), (bq_rows, bq_out)))]
    for cp in rows:
        cp.start()
    for cp in rows + turned:
        cp.wait()
    for k in range(4):
        for cp in results(jnp.int32(1), k):
            cp.wait()


def run_grads(pairs, y_t, dx_t, sums):
    n, tok = pairs[0][0].shape[1], pairs[0][0].shape[3]
    sizes = [(a.shape[2], b.shape[2]) for a, b in pairs]
    d, f = sizes[0]
    st, vm, dma = jax.ShapeDtypeStruct, pltpu.VMEM, pltpu.SemaphoreType.DMA
    most = max(a + b for a, b in sizes)
    rows = [((2, 1, f), F32), ((2, 6, 1, d), F32), ((2, 3, 1, d), F32)]
    return pl.pallas_call(
        functools.partial(grads_kernel, n),
        out_shape=[st((2,) + v, F32) for v in sizes] + [st(*rows[0]), st((tok, d), BF16), st((tok, d), BF16), st(*rows[1]),
                                                        st(*rows[2])],
        in_specs=[HBM] * 11, out_specs=[HBM] * 9,
        scratch_shapes=[vm(v, F32) for v in sizes] + [vm((8, v[1]), F32) for v in sizes[:3]] + [
            vm((2, PAIR, most, tok), BF16), vm((2, d, tok), BF16), vm((2, tok, d), BF16), vm(sums.shape, F32)] + [
            vm(*v) for v in rows] + [dma((2, 2)), dma((4,)), dma((5,))],
        name='weight_grads', compiler_params=pltpu.CompilerParams(vmem_limit_bytes=VMEM_LIMIT),
    )(*[v for p in pairs for v in p], y_t, dx_t, sums)


def solution(mesh):
    data_spec = P(('dp', 'pp'))
    weight_spec = P('pp')

    def per_device(x, dy, w_qkv, w_attn, w_fc, w_proj, b_qkv, b_fc, vec_d):
        _, batch, seq, d = x.shape
        heads = w_qkv.shape[5]
        tok = batch * seq

        weights = (w_qkv.reshape(2, d, 3 * d).transpose(0, 2, 1), w_attn.reshape(2, d, d), w_fc[0, :, 0], w_proj[0, :, 0])
        y_t, dx_t, *stash = run_walk(
            mesh.shape['pp'], heads, seq, x.reshape(tok, d), dy.reshape(tok, d), weights,
            vec_d[0, :, 0].transpose(1, 0, 2), b_qkv.reshape(2, 3, d), b_fc[0, :, 0])
        as_, os_, bs, us, dys, dgs, drs, dts, _, sums = stash[6:16]
        g1, g2, go, gq, gb1, y, dx, gv, gbq = run_grads(((bs, dgs), (us, dys), (os_, drs), (dts, as_)), y_t, dx_t, sums)
        return (y.reshape(x.shape), dx.reshape(x.shape),
                gq.transpose(0, 2, 1).reshape(w_qkv.shape), go.reshape(w_attn.shape), g1.reshape(w_fc.shape),
                g2.reshape(w_proj.shape), gbq.reshape(b_qkv.shape), gb1.reshape(b_fc.shape), gv.reshape(vec_d.shape))

    return jax.shard_map(per_device, mesh=mesh, in_specs=(data_spec, data_spec) + (weight_spec,) * 7,
                         out_specs=(data_spec, data_spec) + (data_spec,) * 7, check_vma=False)
```

```python
import functools

import jax
import jax.numpy as jnp
from jax import lax
from jax.experimental import pallas as pl
from jax.experimental.pallas import tpu as pltpu
from jax.sharding import PartitionSpec as P

EPS = 1e-5
F32 = jnp.float32
BF16 = jnp.bfloat16
LANES = 128
ROWS = 96
CH = 256
GROUP = 256
SKEW = 8
K0 = 0.7978845608028654
K1 = K0 * 0.044715
VMEM_LIMIT = 67043328
HBM = pl.BlockSpec(memory_space=pl.ANY)


def dot(lhs, rhs, lc=1, rc=0):
    return lax.dot_general(lhs, rhs, (((lc,), (rc,)), ((), ())), preferred_element_type=F32)


def rows_sum(v):
    r, t = v.shape
    return jnp.sum(v.reshape(r // 8, 8, t), axis=0)


def column(cols, lane, row, count):
    return cols[row:row + count, lane:lane + 1].astype(F32)


def lane_fold(v):
    return functools.reduce(jnp.add, [v[:, k:k + LANES] for k in range(0, v.shape[1], LANES)])


def rounded(v):
    return v.astype(BF16).astype(F32)


def token_sum(v):
    return rounded(jnp.sum(lane_fold(v), axis=1, keepdims=True))


def block_diag(a, b):
    z = jnp.zeros_like(a)
    return jnp.concatenate([jnp.concatenate([a, z], 1), jnp.concatenate([z, b], 1)], 0)


def f_norm(src, cols, lane, dst, stats, row, hold, acc=None):
    d, t = src.shape
    if acc is None:
        acc = jnp.zeros((8, t), F32)
        for i in range(0, d, ROWS):
            acc += rows_sum(src[i:i + ROWS, :].astype(F32))
    mean = jnp.sum(acc, axis=0, keepdims=True) * (1.0 / d)
    acc = jnp.zeros((8, t), F32)
    for i in range(0, d, ROWS):
        c = src[i:i + ROWS, :].astype(F32) - mean
        hold[i:i + ROWS, :] = c
        acc += rows_sum(c * c)
    rstd = lax.rsqrt(jnp.sum(acc, axis=0, keepdims=True) * (1.0 / d) + EPS)
    for i in range(0, d, ROWS):
        c = hold[i:i + ROWS, :] * rstd
        dst[i:i + ROWS, :] = (c * column(cols, lane, i, ROWS) + column(cols, lane + 1, i, ROWS)).astype(BF16)
    stats[row:row + 1, :] = mean
    stats[row + 1:row + 2, :] = rstd


def token_totals(v):
    return dot(v, jnp.ones((v.shape[1], LANES), BF16))


def b_norm(dn, src, cols, gain, skip, dst, stats, row, acc, lane, hold):
    d, t = src.shape
    mean = stats[row:row + 1, :]
    rstd = stats[row + 1:row + 2, :]
    at = lax.broadcasted_iota(jnp.int32, (ROWS, LANES), 1)
    m1 = dot(cols[...], dn[...], 0, 0)[gain:gain + 1, :] * (1.0 / d)
    shift = token_totals(dn[...])
    s2 = jnp.zeros((8, t), F32)
    for i in range(0, d, ROWS):
        c = (src[i:i + ROWS, :].astype(F32) - mean) * rstd
        hold[i:i + ROWS, :] = c
        w = dn[i:i + ROWS, :].astype(F32) * c
        s2 += rows_sum(w * column(cols, gain, i, ROWS))
        acc[i:i + ROWS, :] += jnp.where(at == lane, token_sum(w), jnp.where(at == lane + 1, rounded(shift[i:i + ROWS]), 0.0))
    m2 = jnp.sum(s2, axis=0, keepdims=True) * (1.0 / d)
    for i in range(0, d, ROWS):
        g = dn[i:i + ROWS, :].astype(F32) * column(cols, gain, i, ROWS)
        z = (g - m1 - hold[i:i + ROWS, :] * m2) * rstd + skip[i:i + ROWS, :].astype(F32)
        dst[i:i + ROWS, :] = z.astype(BF16)


def skewed(jobs, first, second):
    pending = []
    for job in jobs:
        pending.append((job, first(*job)))
        if len(pending) > SKEW:
            job, v = pending.pop(0)
            second(*job, v)
    for job, v in pending:
        second(*job, v)


def f_heads(t, o, p, heads, seq, after):
    d, n = o.shape
    head = d // heads
    two = 2 * head
    pairs = heads // 2
    key = lax.broadcasted_iota(jnp.int32, (seq, 2 * seq), 0)
    qry = lax.rem(lax.broadcasted_iota(jnp.int32, (seq, 2 * seq), 1), seq)
    ok = key <= qry
    c = (head ** -0.5) * 1.4426950408889634

    def score(b, j):
        r0, lanes = two * j, slice(b * seq, (b + 1) * seq)
        q = t[r0:r0 + two, lanes]
        return dot(t[d + r0:d + r0 + two, lanes], block_diag(q[:head], q[head:]), 0, 0)

    def mix(b, j, s):
        r0, lanes = two * j, slice(b * seq, (b + 1) * seq)
        s = jnp.where(ok, s, -1e30)
        m = jnp.max(s, axis=0, keepdims=True)
        e = jnp.exp2((s - m) * c)
        e = e * (1.0 / jnp.sum(e, axis=0, keepdims=True))
        k0 = (b * pairs + j) * seq
        p[k0:k0 + seq, :] = e
        x = dot(t[2 * d + r0:2 * d + r0 + two, lanes], e.astype(BF16))
        o[r0:r0 + head, lanes] = x[:head, :seq].astype(BF16)
        o[r0 + head:r0 + two, lanes] = x[head:, seq:].astype(BF16)
        if j == pairs - 1:
            after(b)

    skewed([(b, j) for b in range(n // seq) for j in range(pairs)], score, mix)


def b_heads(t, do, p, heads, seq, after):
    d, n = do.shape
    head = d // heads
    two = 2 * head
    pairs = heads // 2
    scale = head ** -0.5

    def first(b, j):
        r0, lanes = two * j, slice(b * seq, (b + 1) * seq)
        z = do[r0:r0 + two, lanes]
        return dot(t[2 * d + r0:2 * d + r0 + two, lanes], block_diag(z[:head], z[head:]), 0, 0)

    def diag(r0, lanes, x, k):
        t[r0:r0 + head, lanes] = (x[:head, :seq] * k).astype(BF16)
        t[r0 + head:r0 + two, lanes] = (x[head:, seq:] * k).astype(BF16)

    def second(b, j, dp):
        r0, lanes = two * j, slice(b * seq, (b + 1) * seq)
        k0 = (b * pairs + j) * seq
        e = p[k0:k0 + seq, :]
        w = e * dp
        ds = (w - e * jnp.sum(w, axis=0, keepdims=True)).astype(BF16)
        eb = e.astype(BF16)
        q, k = t[r0:r0 + two, lanes], t[d + r0:d + r0 + two, lanes]
        tall = jnp.concatenate([ds[:, :seq], ds[:, seq:]], 0)
        dq, dk = dot(k, ds), dot(q, tall, 1, 1)
        tall = jnp.concatenate([eb[:, :seq], eb[:, seq:]], 0)
        dv = dot(do[r0:r0 + two, lanes], tall, 1, 1)
        diag(r0, lanes, dq, scale)
        diag(d + r0, lanes, dk, scale)
        diag(2 * d + r0, lanes, dv, 1.0)
        if j == pairs - 1:
            after(b)

    skewed([(b, j) for b in range(n // seq) for j in range(pairs)], first, second)


def gelu_and_slope(x):
    x2 = x * x
    hp = 0.5 * jnp.tanh(x * (x2 * K1 + K0)) + 0.5
    u = x * hp
    return u, hp + (u - u * hp) * (x2 * (6.0 * K1) + 2.0 * K0)


ORDERS = (
    (0, 1, 2, 3, 4, 5, 6, 7, 8, 16, 9, 17, 10, 18, 11, 19, 12, 20, 13, 21, 14, 22, 15, 23, 24, 25, 26, 27, 28, 29, 30, 31),
    (0, 1, 2, 3, 4, 5, 6, 7, 8, 9, 16, 10, 17, 11, 12, 18, 13, 19, 14, 20, 15, 21, 24, 22, 25, 23, 26, 27, 28, 29, 30, 31),
    (0, 1, 2, 3, 8, 4, 9, 5, 10, 6, 11, 7, 12, 16, 13, 17, 14, 18, 15, 19, 24, 20, 25, 21, 26, 22, 27, 23, 28, 29, 30, 31),
    (0, 8, 1, 9, 2, 10, 3, 11, 4, 12, 5, 13, 6, 14, 7, 15, 16, 24, 17, 25, 18, 26, 19, 27, 20, 28, 21, 29, 22, 30, 23, 31),
)


class Group:
    def __init__(self, n):
        self.n, self.half, self.last, self.steps = n, n // 2, n - 1, 4 * n
        self.me = lax.axis_index('pp')
        self.side = self.me // self.half
        self.depth = self.me + self.side * (self.last - 2 * self.me)
        self.inner = self.me + 1 - 2 * self.side
        self.outer = self.me - 1 + 2 * self.side
        self.inside = self.depth == self.half - 1
        self.outside = self.depth == 0
        self.codes = []
        for k in range(self.steps):
            v = jnp.int32(ORDERS[0][k])
            for i in range(1, self.half):
                v = jnp.where(self.depth == i, ORDERS[i][k], v)
            self.codes.append(v)

    def place(self, i):
        far = lax.rem(i - self.half + self.half // 2, self.half) + self.half
        return jnp.where(i < self.half, i, far)

    def step(self, s):
        code = self.codes[0]
        for k in range(1, self.steps):
            code = jnp.where(s == k, self.codes[k], code)
        kind = code // self.n
        m = code - self.n * kind
        back = kind >= 2
        sec = jnp.where(jnp.logical_or(kind == 1, kind == 2), 1, 0)
        c = jnp.where(sec == 1, 1 - self.side, self.side)
        return kind, back, sec, m, c


def both(a, *rest):
    return functools.reduce(jnp.logical_and, rest, a)


def walk_kernel(n, heads, seq, x_in, dy_in, wq, wo, w1, w2, vec, bq, b1,
                y_out, dx_out, hs, ts, rs, ps, gs, ss, as_, os_, bs, us, dys, dgs, drs, dts, feed, sums, x_t, dy_t,
                vwq, vwo, vw1, vw2, vcols, vvec, vbq, vb1, slots, out, a, t, o, r, u, pg, ya, stats, acc,
                load_sems, recv_sems, send_sems, final_sems, feed_send, feed_recv, f_sems, b_in, b_sems, lead_sems):
    g = Group(n)
    d, tok = a.shape
    f = u.shape[0]
    half = tok // 2
    prow = ps.shape[2]
    part = prow // (tok // seq)
    weights = ((wq, vwq), (wo, vwo), (w1, vw1), (w2, vw2))

    def weight(c, i):
        h, v = weights[i]
        return pltpu.make_async_copy(h.at[c], v.at[c], load_sems.at[c, i])

    def remote(src, dst, send, recv, dev):
        return pltpu.make_async_remote_copy(src_ref=src, dst_ref=dst, send_sem=send, recv_sem=recv, device_id={'pp': dev})

    def saver(c, m, sems):
        def copy(i, v, dst, at=None):
            hbm = dst.at[c, m]
            if at is not None:
                v, hbm = v.at[pl.ds(*at), :], hbm.at[pl.ds(*at), :]
            return pltpu.make_async_copy(v, hbm, sems.at[i])
        return copy

    def fetch(i, c, m, at=None):
        hbm, v = ((gs, pg), (ps, pg.at[pl.ds(0, prow), :]), (ts, t), (rs, r), (hs, a), (ss, stats))[i]
        hbm = hbm.at[c, m]
        if at is not None:
            hbm, v = hbm.at[pl.ds(*at), :], v.at[pl.ds(*at), :]
        return pltpu.make_async_copy(hbm, v, b_in.at[i])

    def forward(c, m, x, y):
        copy = saver(c, m, f_sems)
        cv = vcols.at[c]
        copy(0, x, hs).start()
        f_norm(x, cv, 0, a, stats, 0, ya)
        copy(1, a, as_).start()
        v = a[...]
        for i in range(0, 3 * d, CH):
            z = dot(vwq[c, i:i + CH, :], v) + column(cv, 6 + i // d, i % d, CH)
            t[i:i + CH, :] = z.astype(BF16)
        copy(2, t, ts).start()
        f_heads(t, o, pg, heads, seq, lambda b: copy(4, pg, ps, (b * part, part)).start())
        copy(3, o, os_).start()
        v = o[...]
        total = jnp.zeros((8, tok), F32)
        for i in range(0, d, CH):
            z = dot(vwo[c, :, i:i + CH], v, 0, 0) + column(cv, 2, i, CH) + x[i:i + CH, :].astype(F32)
            z = z.astype(BF16)
            r[i:i + CH, :] = z
            total += rows_sum(z.astype(F32))
        copy(5, r, rs).start()
        copy(1, a, as_).wait()
        f_norm(r, cv, 3, a, stats, 2, ya, total)
        copy(6, a, bs).start()
        copy(7, stats, ss).start()
        copy(4, pg.at[pl.ds(0, prow), :], ps).wait()
        v = a[...]

        def up(k):
            for i in range(k * GROUP, (k + 1) * GROUP, CH):
                h = dot(vw1[c, :, i:i + CH], v, 0, 0) + column(cv, 9 + i // d, i % d, CH)
                uu, slope = gelu_and_slope(h)
                u[i:i + CH, :] = uu.astype(BF16)
                pg[2 * i:2 * i + CH, :] = slope[:, :half]
                pg[2 * i + CH:2 * i + 2 * CH, :] = slope[:, half:]
                copy(8, u, us, (i, CH)).start()
                copy(9, pg, gs, (2 * i, 2 * CH)).start()

        def down(k):
            ks = slice(k * GROUP, (k + 1) * GROUP)
            w = u[ks, :]
            for i in range(0, d, CH):
                z = dot(vw2[c, ks, i:i + CH], w, 0, 0)
                z += (column(cv, 5, i, CH) + r[i:i + CH, :].astype(F32)) if k == 0 else ya[i:i + CH, :]
                if ks.stop < f:
                    ya[i:i + CH, :] = z
                else:
                    y[i:i + CH, :] = z.astype(BF16)

        many = f // GROUP
        for k in range(many + 2):
            if k < many:
                up(k)
            if k >= 2:
                down(k - 2)
        for i, v, dst in ((0, x, hs), (2, t, ts), (3, o, os_), (5, r, rs), (6, a, bs), (7, stats, ss), (8, u, us),
                          (9, pg, gs)):
            copy(i, v, dst).wait()

    def backward(c, m, dy, y, then):
        copy = saver(c, m, b_sems)
        cv = vcols.at[c]
        copy(0, dy, dys).start()
        fetch(0, c, m).wait()
        v = dy[...]
        for i in range(0, f, CH):
            du = dot(vw2[c, i:i + CH, :], v).astype(BF16).astype(F32)
            u[i:i + CH, :half] = (du[:, :half] * pg[2 * i:2 * i + CH, :]).astype(BF16)
            u[i:i + CH, half:] = (du[:, half:] * pg[2 * i + CH:2 * i + 2 * CH, :]).astype(BF16)
        fetch(1, c, m).start()
        then(0, (prow, 2 * f - prow))
        copy(1, u, dgs).start()
        v = u[...]
        for i in range(0, d, CH):
            y[i:i + CH, :] = dot(vw1[c, i:i + CH, :], v).astype(BF16)
        for i in (3, 4, 5):
            fetch(i, c, m).wait()
        b_norm(y, r, cv, 3, dy, o, stats, 2, acc.at[c], 2, ya)
        then(3)
        copy(2, o, drs).start()
        v = o[...]
        for i in range(0, d, CH):
            y[i:i + CH, :] = dot(vwo[c, i:i + CH, :], v).astype(BF16)
        for i in (1, 2):
            fetch(i, c, m).wait()
        b_heads(t, y, pg, heads, seq, lambda b: then(0, (b * part, part)))
        copy(3, t, dts).start()
        v = t[...]
        at = lax.broadcasted_iota(jnp.int32, (ROWS, LANES), 1)
        for i in range(0, d, CH):
            y[i:i + CH, :] = dot(vwq[c, :, i:i + CH], v, 0, 0).astype(BF16)
        b_norm(y, a, cv, 0, o, y, stats, 0, acc.at[c], 0, ya)
        for i in range(0, d, ROWS):
            e = 0.0
            for k in range(3):
                e = jnp.where(at == 4 + k, token_sum(t[k * d + i:k * d + i + ROWS, :].astype(F32)), e)
            acc[c, i:i + ROWS, :] += e
        then(4)
        then(5)
        for i, v, dst in ((0, dy, dys), (1, u, dgs), (2, o, drs), (3, t, dts)):
            copy(i, v, dst).wait()
        then(2)

    late = 1 - g.side
    loads = [pltpu.make_async_copy(x_in, vwq.at[late, pl.ds(0, tok), :], lead_sems.at[0]),
             pltpu.make_async_copy(dy_in, vwq.at[late, pl.ds(tok, tok), :], lead_sems.at[1]),
             pltpu.make_async_copy(vec, vvec, lead_sems.at[2]), pltpu.make_async_copy(bq, vbq, lead_sems.at[3]),
             pltpu.make_async_copy(b1, vb1, lead_sems.at[4])]
    for cp in loads:
        cp.start()
    for i in range(4):
        weight(g.side, i).start()
    barrier = pltpu.get_barrier_semaphore()
    for i in range(n):
        pl.semaphore_signal(barrier, inc=1, device_id={'pp': jnp.int32(i)})
    for cp in loads:
        cp.wait()
    out[0] = vwq[late, 0:tok, :].T
    out[1] = vwq[late, tok:2 * tok, :].T

    @pl.when(g.outside)
    def _():
        slots[0, 0] = out[0]
    fed = [pltpu.make_async_copy(out.at[0], x_t, lead_sems.at[0]), pltpu.make_async_copy(out.at[1], dy_t, lead_sems.at[1])]
    for cp in fed:
        cp.start()
    pl.semaphore_wait(barrier, n)
    for cp in fed:
        cp.wait()

    heads_at = ((0, 0), (1, g.last))
    for k, head in heads_at:
        spot = g.place(g.me + k * (g.last - 2 * g.me))

        @pl.when(g.me != head)
        def _():
            remote(x_t, slots.at[0, spot], feed_send.at[0, k], recv_sems.at[0, 0, spot], jnp.int32(head)).start()
            remote(dy_t, feed.at[spot], feed_send.at[1, k], feed_recv.at[spot], jnp.int32(head)).start()

    for c in range(2):
        rows = [vvec[i, c:c + 1, :] for i in range(6)] + [vbq[c, i:i + 1, :] for i in range(3)]
        rows += [vb1[c:c + 1, i:i + d] for i in range(0, f, d)]
        rows = [v.astype(F32) for v in rows] + [jnp.zeros((LANES - len(rows), d), F32)]
        vcols[c] = jnp.concatenate(rows, 0).T.astype(BF16)
    acc[...] = jnp.zeros_like(acc)

    def settle(par, flag):
        @pl.when(flag == 1)
        def _():
            remote(out.at[par], slots.at[0, 0], send_sems.at[par], recv_sems.at[0, 0, 0], g.me).wait_send()

    def body(s, carry):
        kind, back, sec, m, c = g.step(s)
        nxt = jnp.minimum(s + 1, g.steps - 1)
        _, back2, _, m2, c2 = g.step(nxt)
        more = both(back2, s + 1 < g.steps)
        par = lax.rem(s, 2)
        inward = jnp.logical_or(kind == 0, kind == 2)
        outward = jnp.logical_not(inward)
        way = jnp.where(back, 1, 0)

        @pl.when(jnp.logical_or(s == 0, both(kind == 1, m == 0)))
        def _():
            for i in range(4):
                weight(c, i).wait()

        @pl.when(s == 0)
        def _():
            for i in range(4):
                weight(late, i).start()

        settle(par, carry[1])

        own = jnp.logical_or(both(outward, g.inside), both(kind == 0, m == 0, g.outside))

        @pl.when(jnp.logical_not(own))
        def _():
            remote(out.at[par], slots.at[sec, m], send_sems.at[par], recv_sems.at[way, sec, m], g.me).wait_recv()

        @pl.when(jnp.logical_not(back))
        def _():
            forward(c, m, slots.at[sec, m], out.at[par])

            @pl.when(more)
            def _():
                for i in (0, 2, 3, 4, 5):
                    fetch(i, c2, m2).start()

        @pl.when(back)
        def _():
            def then(i, at=None):
                @pl.when(more)
                def _():
                    fetch(i, c2, m2, at).start()

            backward(c, m, slots.at[sec, m], out.at[par], then)

        @pl.when(both(inward, g.inside))
        def _():
            slots[1 - sec, m] = out[par]

        @pl.when(both(inward, jnp.logical_not(g.inside)))
        def _():
            remote(out.at[par], slots.at[sec, m], send_sems.at[par], recv_sems.at[way, sec, m], g.inner).start()

        @pl.when(both(outward, jnp.logical_not(g.outside)))
        def _():
            remote(out.at[par], slots.at[sec, m], send_sems.at[par], recv_sems.at[way, sec, m], g.outer).start()

        owner = m + g.side * (g.last - 2 * m)
        done = both(outward, g.outside, m < g.half)
        for w, ref in ((0, y_out), (1, dx_out)):
            mine = both(done, way == w)

            @pl.when(both(mine, owner == g.me))
            def _():
                pltpu.make_async_copy(out.at[par], ref, send_sems.at[par]).start()

            @pl.when(both(mine, owner != g.me))
            def _():
                remote(out.at[par], ref, send_sems.at[par], final_sems.at[w], owner).start()

        @pl.when(both(kind == 1, g.outside))
        def _():
            @pl.when(m == 0)
            def _():
                pltpu.make_async_copy(dy_t, slots.at[1, m], recv_sems.at[1, 1, m]).start()

            @pl.when(m > 0)
            def _():
                remote(dy_t, feed.at[m], feed_send.at[1, 0], feed_recv.at[m], g.me).wait_recv()
                pltpu.make_async_copy(feed.at[m], slots.at[1, m], recv_sems.at[1, 1, m]).start()

        kept = jnp.logical_or(both(inward, g.inside), both(outward, g.outside, m >= g.half))
        return jnp.where(kept, 0, 1), carry[0]

    before, earlier = lax.fori_loop(0, g.steps, body, (jnp.int32(0), jnp.int32(0)))
    settle(g.steps % 2, earlier)
    settle((g.steps + 1) % 2, before)
    for k, head in heads_at:
        @pl.when(g.me != head)
        def _():
            remote(x_t, slots.at[0, 0], feed_send.at[0, k], recv_sems.at[0, 0, 0], jnp.int32(head)).wait_send()
            remote(dy_t, feed.at[0], feed_send.at[1, k], feed_recv.at[0], jnp.int32(head)).wait_send()

    @pl.when(jnp.logical_not(g.outside))
    def _():
        for w, ref in ((0, y_out), (1, dx_out)):
            remote(out.at[0], ref, send_sems.at[0], final_sems.at[w], g.me).wait_recv()

    cp = pltpu.make_async_copy(acc, sums, b_sems.at[0])
    cp.start()
    cp.wait()


def run_walk(n, heads, seq, x, dy, weights, vec, bq, b1):
    tok, d = x.shape
    f = weights[2].shape[2]
    prow = (tok // seq) * (heads // 2) * seq
    st, vm, dma = jax.ShapeDtypeStruct, pltpu.VMEM, pltpu.SemaphoreType.DMA
    act, tall, hid = ((d, tok), BF16), ((3 * d, tok), BF16), ((f, tok), BF16)
    outs = [st(*act)] * 2 + [st((2, n) + v, k) for v, k in (
        act, tall, act, ((prow, 2 * seq), F32), ((2 * f, tok // 2), F32), ((8, tok), F32), act, act, act, hid,
        act, hid, act, tall)] + [st((n, d, tok), BF16), st((2, d, LANES), F32)] + [st(*act)] * 2
    scratch = [vm(w.shape, w.dtype) for w in weights] + [vm((2, d, LANES), BF16)] + [vm(v.shape, v.dtype) for v in (vec, bq, b1)] + [
        vm((2, n, d, tok), BF16), vm((2, d, tok), BF16), vm(*act), vm(*tall), vm(*act), vm(*act), vm(*hid),
        vm((2 * f, tok // 2), F32), vm((d, tok), F32), vm((8, tok), F32), vm((2, d, LANES), F32),
        dma((2, len(weights))), dma((2, 2, n)), dma((2,)), dma((2,)), dma((2, 2)), dma((n,)), dma((10,)), dma((6,)), dma((4,)),
        dma((5,))]
    args = (x, dy, *weights, vec, bq, b1)
    return pl.pallas_call(
        functools.partial(walk_kernel, n, heads, seq), out_shape=outs, in_specs=[HBM] * len(args), out_specs=[HBM] * len(outs),
        scratch_shapes=scratch, name='walk',
        compiler_params=pltpu.CompilerParams(vmem_limit_bytes=VMEM_LIMIT, collective_id=0, has_side_effects=True),
    )(*args)


PAIR = 2


def grads_kernel(n, *refs):
    ins, (y_t, dx_t, sums), refs = refs[:8], refs[8:11], refs[11:]
    outs, (b1_out, y_out, dx_out, vec_out, bq_out), refs = refs[:4], refs[4:9], refs[9:]
    accs, biases, refs = refs[:4], refs[4:7], refs[7:]
    buf, va, vb, vsum, b1_row, vec_rows, bq_rows, in_sems, out_sems, end_sems = refs
    steps = n // PAIR
    tok = buf.shape[3]
    d = y_t.shape[0]

    def fetches(c, k, j):
        slot = lax.rem(j, 2)
        rows, cols = ins[2 * k].shape[2], ins[2 * k + 1].shape[2]
        at = pl.ds(j * PAIR, PAIR)
        return (pltpu.make_async_copy(ins[2 * k].at[c, at], buf.at[slot, :, pl.ds(0, rows), :], in_sems.at[slot, 0]),
                pltpu.make_async_copy(ins[2 * k + 1].at[c, at], buf.at[slot, :, pl.ds(rows, cols), :], in_sems.at[slot, 1]))

    def begin(c, k, j):
        for cp in fetches(c, k, j):
            cp.start()

    def results(c, k):
        cps = [pltpu.make_async_copy(accs[k], outs[k].at[c], out_sems.at[k])]
        return cps

    acts = ((y_t, y_out), (dx_t, dx_out))
    loads = [pltpu.make_async_copy(h, va.at[i], end_sems.at[i]) for i, (h, _) in enumerate(acts)]
    loads.append(pltpu.make_async_copy(sums, vsum, end_sems.at[2]))
    for cp in loads:
        cp.start()
    begin(jnp.int32(0), 0, jnp.int32(0))
    for cp in loads:
        cp.wait()
    for i in range(2):
        vb[i] = va[i].T
    turned = [pltpu.make_async_copy(vb.at[i], h, end_sems.at[i]) for i, (_, h) in enumerate(acts)]
    for cp in turned:
        cp.start()
    for i in range(2):
        part = vsum[i].T
        for row, src in ((0, 0), (1, 1), (3, 2), (4, 3)):
            vec_rows[i, row] = part[src:src + 1, :]
        for row in range(3):
            bq_rows[i, row] = part[4 + row:5 + row, :]

    def stage(c, carry):
        for k in range(4):
            rows, cols = ins[2 * k].shape[2], ins[2 * k + 1].shape[2]

            def step(j, carry, k=k, rows=rows, cols=cols):
                @pl.when(j + 1 < steps)
                def _():
                    begin(c, k, j + 1)

                @pl.when(j + 1 == steps)
                def _():
                    if k < 3:
                        begin(c, k + 1, jnp.int32(0))
                    else:
                        @pl.when(c == 0)
                        def _():
                            begin(jnp.int32(1), 0, jnp.int32(0))

                @pl.when(jnp.logical_and(j == 0, c == 1))
                def _():
                    for cp in results(jnp.int32(0), k):
                        cp.wait()

                for cp in fetches(c, k, j):
                    cp.wait()
                slot = lax.rem(j, 2)
                later = j > 0
                parts = 2 if max(rows, cols) > 3 * d else 1
                tall = rows > cols
                height, width = (rows // parts, cols) if tall else (rows, cols // parts)

                def block(h, carry):
                    top = pl.multiple_of(h * height, CH) if tall and parts > 1 else 0
                    left = pl.multiple_of(h * width, CH) if not tall and parts > 1 else 0
                    w = [buf[slot, q, pl.ds(rows + left, width), :] for q in range(PAIR)]
                    for i in range(0, height, CH):
                        at = (pl.ds(top + i, CH), pl.ds(left, width))
                        z = jnp.where(later, accs[k][at], 0.0)
                        edge = i == 0 and k > 0
                        if edge:
                            e = jnp.where(later, biases[k - 1][:, at[1]], 0.0)
                        for q in range(PAIR):
                            x = buf[slot, q, pl.ds(top + i, CH), :]
                            if edge:
                                x = jnp.concatenate([x, jnp.ones((16, tok), BF16)], 0)
                            v = rounded(dot(x, w[q], 1, 1))
                            z = z + v[:CH]
                            if edge:
                                e = e + v[CH:CH + 8]
                        accs[k][at] = z
                        if edge and tall and parts > 1:
                            biases[k - 1][:, at[1]] = jnp.where(h == 0, e, biases[k - 1][:, at[1]])
                        elif edge:
                            biases[k - 1][:, at[1]] = e
                    return carry

                if parts > 1:
                    lax.fori_loop(0, parts, block, 0)
                else:
                    block(0, 0)
                return carry

            lax.fori_loop(0, steps, step, 0)
            for cp in results(c, k):
                cp.start()
        b1_row[c] = biases[0][0:1, :]
        vec_rows[c, 5] = biases[1][0:1, :]
        vec_rows[c, 2] = biases[2][0:1, :]
        return carry

    lax.fori_loop(0, 2, stage, 0)
    rows = [pltpu.make_async_copy(v, h, end_sems.at[2 + i])
            for i, (v, h) in enumerate(((b1_row, b1_out), (vec_rows, vec_out), (bq_rows, bq_out)))]
    for cp in rows:
        cp.start()
    for cp in rows + turned:
        cp.wait()
    for k in range(4):
        for cp in results(jnp.int32(1), k):
            cp.wait()


def run_grads(pairs, y_t, dx_t, sums):
    n, tok = pairs[0][0].shape[1], pairs[0][0].shape[3]
    sizes = [(a.shape[2], b.shape[2]) for a, b in pairs]
    d, f = sizes[1]
    st, vm, dma = jax.ShapeDtypeStruct, pltpu.VMEM, pltpu.SemaphoreType.DMA
    most = max(a + b for a, b in sizes)
    rows = [((2, 1, f), F32), ((2, 6, 1, d), F32), ((2, 3, 1, d), F32)]
    return pl.pallas_call(
        functools.partial(grads_kernel, n),
        out_shape=[st((2,) + v, F32) for v in sizes] + [st(*rows[0]), st((tok, d), BF16), st((tok, d), BF16), st(*rows[1]),
                                                        st(*rows[2])],
        in_specs=[HBM] * 11, out_specs=[HBM] * 9,
        scratch_shapes=[vm(v, F32) for v in sizes] + [vm((8, v[1]), F32) for v in sizes[1:]] + [
            vm((2, PAIR, most, tok), BF16), vm((2, d, tok), BF16), vm((2, tok, d), BF16), vm(sums.shape, F32)] + [
            vm(*v) for v in rows] + [dma((2, 2)), dma((4,)), dma((5,))],
        name='weight_grads', compiler_params=pltpu.CompilerParams(vmem_limit_bytes=VMEM_LIMIT),
    )(*[v for p in pairs for v in p], y_t, dx_t, sums)


def solution(mesh):
    data_spec = P(('dp', 'pp'))
    weight_spec = P('pp')

    def per_device(x, dy, w_qkv, w_attn, w_fc, w_proj, b_qkv, b_fc, vec_d):
        _, batch, seq, d = x.shape
        heads = w_qkv.shape[5]
        tok = batch * seq

        weights = (w_qkv.reshape(2, d, 3 * d).transpose(0, 2, 1), w_attn.reshape(2, d, d), w_fc[0, :, 0], w_proj[0, :, 0])
        y_t, dx_t, *stash = run_walk(
            mesh.shape['pp'], heads, seq, x.reshape(tok, d), dy.reshape(tok, d), weights,
            vec_d[0, :, 0].transpose(1, 0, 2), b_qkv.reshape(2, 3, d), b_fc[0, :, 0])
        as_, os_, bs, us, dys, dgs, drs, dts, _, sums = stash[6:16]
        gq, g1, g2, go, gb1, y, dx, gv, gbq = run_grads(((dts, as_), (bs, dgs), (us, dys), (os_, drs)), y_t, dx_t, sums)
        return (y.reshape(x.shape), dx.reshape(x.shape),
                gq.transpose(0, 2, 1).reshape(w_qkv.shape), go.reshape(w_attn.shape), g1.reshape(w_fc.shape),
                g2.reshape(w_proj.shape), gbq.reshape(b_qkv.shape), gb1.reshape(b_fc.shape), gv.reshape(vec_d.shape))

    return jax.shard_map(per_device, mesh=mesh, in_specs=(data_spec, data_spec) + (weight_spec,) * 7,
                         out_specs=(data_spec, data_spec) + (data_spec,) * 7, check_vma=False)
```

```python
import functools

import jax
import jax.numpy as jnp
from jax import lax
from jax.experimental import pallas as pl
from jax.experimental.pallas import tpu as pltpu
from jax.sharding import PartitionSpec as P

EPS = 1e-5
F32 = jnp.float32
BF16 = jnp.bfloat16
LANES = 128
ROWS = 96
CH = 256
GROUP = 256
SKEW = 8
K0 = 0.7978845608028654
K1 = K0 * 0.044715
VMEM_LIMIT = 67043328
HBM = pl.BlockSpec(memory_space=pl.ANY)


def dot(lhs, rhs, lc=1, rc=0):
    return lax.dot_general(lhs, rhs, (((lc,), (rc,)), ((), ())), preferred_element_type=F32)


def rows_sum(v):
    r, t = v.shape
    return jnp.sum(v.reshape(r // 8, 8, t), axis=0)


def column(cols, lane, row, count):
    return cols[row:row + count, lane:lane + 1].astype(F32)


def lane_fold(v):
    return functools.reduce(jnp.add, [v[:, k:k + LANES] for k in range(0, v.shape[1], LANES)])


def rounded(v):
    return v.astype(BF16).astype(F32)


def token_sum(v):
    return rounded(jnp.sum(lane_fold(v), axis=1, keepdims=True))


def block_diag(a, b):
    z = jnp.zeros_like(a)
    return jnp.concatenate([jnp.concatenate([a, z], 1), jnp.concatenate([z, b], 1)], 0)


def f_norm(src, cols, lane, dst, stats, row, hold, acc=None):
    d, t = src.shape
    if acc is None:
        acc = jnp.zeros((8, t), F32)
        for i in range(0, d, ROWS):
            acc += rows_sum(src[i:i + ROWS, :].astype(F32))
    mean = jnp.sum(acc, axis=0, keepdims=True) * (1.0 / d)
    acc = jnp.zeros((8, t), F32)
    for i in range(0, d, ROWS):
        c = src[i:i + ROWS, :].astype(F32) - mean
        hold[i:i + ROWS, :] = c
        acc += rows_sum(c * c)
    rstd = lax.rsqrt(jnp.sum(acc, axis=0, keepdims=True) * (1.0 / d) + EPS)
    for i in range(0, d, ROWS):
        c = hold[i:i + ROWS, :] * rstd
        dst[i:i + ROWS, :] = (c * column(cols, lane, i, ROWS) + column(cols, lane + 1, i, ROWS)).astype(BF16)
    stats[row:row + 1, :] = mean
    stats[row + 1:row + 2, :] = rstd


def token_totals(v):
    return dot(v, jnp.ones((v.shape[1], LANES), BF16))


def b_norm(dn, src, cols, gain, skip, dst, stats, row, acc, lane, hold):
    d, t = src.shape
    mean = stats[row:row + 1, :]
    rstd = stats[row + 1:row + 2, :]
    at = lax.broadcasted_iota(jnp.int32, (ROWS, LANES), 1)
    m1 = dot(cols[...], dn[...], 0, 0)[gain:gain + 1, :] * (1.0 / d)
    shift = token_totals(dn[...])
    s2 = jnp.zeros((8, t), F32)
    for i in range(0, d, ROWS):
        c = (src[i:i + ROWS, :].astype(F32) - mean) * rstd
        hold[i:i + ROWS, :] = c
        w = dn[i:i + ROWS, :].astype(F32) * c
        s2 += rows_sum(w * column(cols, gain, i, ROWS))
        acc[i:i + ROWS, :] += jnp.where(at == lane, token_sum(w), jnp.where(at == lane + 1, rounded(shift[i:i + ROWS]), 0.0))
    m2 = jnp.sum(s2, axis=0, keepdims=True) * (1.0 / d)
    for i in range(0, d, ROWS):
        g = dn[i:i + ROWS, :].astype(F32) * column(cols, gain, i, ROWS)
        z = (g - m1 - hold[i:i + ROWS, :] * m2) * rstd + skip[i:i + ROWS, :].astype(F32)
        dst[i:i + ROWS, :] = z.astype(BF16)


def skewed(jobs, first, second):
    pending = []
    for job in jobs:
        pending.append((job, first(*job)))
        if len(pending) > SKEW:
            job, v = pending.pop(0)
            second(*job, v)
    for job, v in pending:
        second(*job, v)


def f_heads(t, o, p, heads, seq, after):
    d, n = o.shape
    head = d // heads
    two = 2 * head
    pairs = heads // 2
    key = lax.broadcasted_iota(jnp.int32, (seq, 2 * seq), 0)
    qry = lax.rem(lax.broadcasted_iota(jnp.int32, (seq, 2 * seq), 1), seq)
    ok = key <= qry
    c = (head ** -0.5) * 1.4426950408889634

    def score(b, j):
        r0, lanes = two * j, slice(b * seq, (b + 1) * seq)
        q = t[r0:r0 + two, lanes]
        return dot(t[d + r0:d + r0 + two, lanes], block_diag(q[:head], q[head:]), 0, 0)

    def mix(b, j, s):
        r0, lanes = two * j, slice(b * seq, (b + 1) * seq)
        s = jnp.where(ok, s, -1e30)
        m = jnp.max(s, axis=0, keepdims=True)
        e = jnp.exp2((s - m) * c)
        e = e * (1.0 / jnp.sum(e, axis=0, keepdims=True))
        k0 = (b * pairs + j) * seq
        p[k0:k0 + seq, :] = e
        x = dot(t[2 * d + r0:2 * d + r0 + two, lanes], e.astype(BF16))
        o[r0:r0 + head, lanes] = x[:head, :seq].astype(BF16)
        o[r0 + head:r0 + two, lanes] = x[head:, seq:].astype(BF16)
        if j == pairs - 1:
            after(b)

    skewed([(b, j) for b in range(n // seq) for j in range(pairs)], score, mix)


def b_heads(t, do, p, heads, seq, after):
    d, n = do.shape
    head = d // heads
    two = 2 * head
    pairs = heads // 2
    scale = head ** -0.5

    def first(b, j):
        r0, lanes = two * j, slice(b * seq, (b + 1) * seq)
        z = do[r0:r0 + two, lanes]
        return dot(t[2 * d + r0:2 * d + r0 + two, lanes], block_diag(z[:head], z[head:]), 0, 0)

    def diag(r0, lanes, x, k):
        t[r0:r0 + head, lanes] = (x[:head, :seq] * k).astype(BF16)
        t[r0 + head:r0 + two, lanes] = (x[head:, seq:] * k).astype(BF16)

    def second(b, j, dp):
        r0, lanes = two * j, slice(b * seq, (b + 1) * seq)
        k0 = (b * pairs + j) * seq
        e = p[k0:k0 + seq, :]
        w = e * dp
        ds = (w - e * jnp.sum(w, axis=0, keepdims=True)).astype(BF16)
        eb = e.astype(BF16)
        q, k = t[r0:r0 + two, lanes], t[d + r0:d + r0 + two, lanes]
        tall = jnp.concatenate([ds[:, :seq], ds[:, seq:]], 0)
        dq, dk = dot(k, ds), dot(q, tall, 1, 1)
        tall = jnp.concatenate([eb[:, :seq], eb[:, seq:]], 0)
        dv = dot(do[r0:r0 + two, lanes], tall, 1, 1)
        diag(r0, lanes, dq, scale)
        diag(d + r0, lanes, dk, scale)
        diag(2 * d + r0, lanes, dv, 1.0)
        if j == pairs - 1:
            after(b)

    skewed([(b, j) for b in range(n // seq) for j in range(pairs)], first, second)


def gelu_and_slope(x):
    x2 = x * x
    hp = 0.5 * jnp.tanh(x * (x2 * K1 + K0)) + 0.5
    u = x * hp
    return u, hp + (u - u * hp) * (x2 * (6.0 * K1) + 2.0 * K0)


ORDERS = (
    (0, 1, 2, 3, 4, 5, 6, 7, 8, 16, 9, 17, 10, 18, 11, 19, 12, 20, 13, 21, 14, 22, 15, 23, 24, 25, 26, 27, 28, 29, 30, 31),
    (0, 1, 2, 3, 4, 5, 6, 7, 8, 9, 16, 10, 17, 11, 12, 18, 13, 19, 14, 20, 15, 21, 24, 22, 25, 23, 26, 27, 28, 29, 30, 31),
    (0, 1, 2, 3, 8, 4, 9, 5, 10, 6, 11, 7, 12, 16, 13, 17, 14, 18, 15, 19, 24, 20, 25, 21, 26, 22, 27, 23, 28, 29, 30, 31),
    (0, 8, 1, 9, 2, 10, 3, 11, 4, 12, 5, 13, 6, 14, 7, 15, 16, 24, 17, 25, 18, 26, 19, 27, 20, 28, 21, 29, 22, 30, 23, 31),
)


class Group:
    def __init__(self, n):
        self.n, self.half, self.last, self.steps = n, n // 2, n - 1, 4 * n
        self.me = lax.axis_index('pp')
        self.side = self.me // self.half
        self.depth = self.me + self.side * (self.last - 2 * self.me)
        self.inner = self.me + 1 - 2 * self.side
        self.outer = self.me - 1 + 2 * self.side
        self.inside = self.depth == self.half - 1
        self.outside = self.depth == 0
        self.codes = []
        for k in range(self.steps):
            v = jnp.int32(ORDERS[0][k])
            for i in range(1, self.half):
                v = jnp.where(self.depth == i, ORDERS[i][k], v)
            self.codes.append(v)

    def place(self, i):
        far = lax.rem(i - self.half + self.half // 2, self.half) + self.half
        return jnp.where(i < self.half, i, far)

    def step(self, s):
        code = self.codes[0]
        for k in range(1, self.steps):
            code = jnp.where(s == k, self.codes[k], code)
        kind = code // self.n
        m = code - self.n * kind
        back = kind >= 2
        sec = jnp.where(jnp.logical_or(kind == 1, kind == 2), 1, 0)
        c = jnp.where(sec == 1, 1 - self.side, self.side)
        return kind, back, sec, m, c


def both(a, *rest):
    return functools.reduce(jnp.logical_and, rest, a)


def walk_kernel(n, heads, seq, x_in, dy_in, wq, wo, w1, w2, vec, bq, b1,
                y_out, dx_out, hs, ts, rs, ps, gs, ss, as_, os_, bs, us, dys, dgs, drs, dts, feed, sums, x_t, dy_t,
                vwq, vwo, vw1, vw2, vcols, vvec, vbq, vb1, slots, out, a, t, o, r, u, pg, ya, stats, acc,
                load_sems, recv_sems, send_sems, final_sems, feed_send, feed_recv, f_sems, b_in, b_sems, lead_sems):
    g = Group(n)
    d, tok = a.shape
    f = u.shape[0]
    half = tok // 2
    prow = ps.shape[2]
    part = prow // (tok // seq)
    weights = ((wq, vwq), (wo, vwo), (w1, vw1), (w2, vw2))

    def weight(c, i):
        h, v = weights[i]
        return pltpu.make_async_copy(h.at[c], v.at[c], load_sems.at[c, i])

    def remote(src, dst, send, recv, dev):
        return pltpu.make_async_remote_copy(src_ref=src, dst_ref=dst, send_sem=send, recv_sem=recv, device_id={'pp': dev})

    def saver(c, m, sems):
        def copy(i, v, dst, at=None):
            hbm = dst.at[c, m]
            if at is not None:
                v, hbm = v.at[pl.ds(*at), :], hbm.at[pl.ds(*at), :]
            return pltpu.make_async_copy(v, hbm, sems.at[i])
        return copy

    def fetch(i, c, m, at=None):
        hbm, v = ((gs, pg), (ps, pg.at[pl.ds(0, prow), :]), (ts, t), (rs, r), (hs, a), (ss, stats))[i]
        hbm = hbm.at[c, m]
        if at is not None:
            hbm, v = hbm.at[pl.ds(*at), :], v.at[pl.ds(*at), :]
        return pltpu.make_async_copy(hbm, v, b_in.at[i])

    def forward(c, m, x, y, pending, more_forward):
        copy = saver(c, m, f_sems)
        cv = vcols.at[c]

        def tail():
            copy(8, u, us).wait()
            copy(10, pg, gs, (prow, 2 * f - prow)).wait()

        copy(0, x, hs).start()
        f_norm(x, cv, 0, a, stats, 0, ya)
        copy(1, a, as_).start()
        v = a[...]
        for i in range(0, 3 * d, CH):
            z = dot(vwq[c, i:i + CH, :], v) + column(cv, 6 + i // d, i % d, CH)
            t[i:i + CH, :] = z.astype(BF16)
        copy(2, t, ts).start()
        f_heads(t, o, pg, heads, seq, lambda b: copy(4, pg, ps, (b * part, part)).start())
        copy(3, o, os_).start()
        v = o[...]
        total = jnp.zeros((8, tok), F32)
        for i in range(0, d, CH):
            z = dot(vwo[c, :, i:i + CH], v, 0, 0) + column(cv, 2, i, CH) + x[i:i + CH, :].astype(F32)
            z = z.astype(BF16)
            r[i:i + CH, :] = z
            total += rows_sum(z.astype(F32))
        copy(5, r, rs).start()
        copy(1, a, as_).wait()
        f_norm(r, cv, 3, a, stats, 2, ya, total)
        copy(6, a, bs).start()
        copy(7, stats, ss).start()
        copy(4, pg.at[pl.ds(0, prow), :], ps).wait()

        @pl.when(pending)
        def _():
            tail()

        v = a[...]

        def up(k):
            for i in range(k * GROUP, (k + 1) * GROUP, CH):
                h = dot(vw1[c, :, i:i + CH], v, 0, 0) + column(cv, 9 + i // d, i % d, CH)
                uu, slope = gelu_and_slope(h)
                u[i:i + CH, :] = uu.astype(BF16)
                pg[2 * i:2 * i + CH, :] = slope[:, :half]
                pg[2 * i + CH:2 * i + 2 * CH, :] = slope[:, half:]
                copy(8, u, us, (i, CH)).start()
                copy(9 if 2 * i < prow else 10, pg, gs, (2 * i, 2 * CH)).start()

        def down(k):
            ks = slice(k * GROUP, (k + 1) * GROUP)
            w = u[ks, :]
            for i in range(0, d, CH):
                z = dot(vw2[c, ks, i:i + CH], w, 0, 0)
                z += (column(cv, 5, i, CH) + r[i:i + CH, :].astype(F32)) if k == 0 else ya[i:i + CH, :]
                if ks.stop < f:
                    ya[i:i + CH, :] = z
                else:
                    y[i:i + CH, :] = z.astype(BF16)

        many = f // GROUP
        for k in range(many + 2):
            if k < many:
                up(k)
            if k >= 2:
                down(k - 2)
        for i, v, dst in ((0, x, hs), (2, t, ts), (3, o, os_), (5, r, rs), (6, a, bs), (7, stats, ss)):
            copy(i, v, dst).wait()
        copy(9, pg, gs, (0, prow)).wait()

        @pl.when(jnp.logical_not(more_forward))
        def _():
            tail()

    def backward(c, m, dy, y, then):
        copy = saver(c, m, b_sems)
        cv = vcols.at[c]
        copy(0, dy, dys).start()
        fetch(0, c, m).wait()
        v = dy[...]
        for i in range(0, f, CH):
            du = dot(vw2[c, i:i + CH, :], v).astype(BF16).astype(F32)
            u[i:i + CH, :half] = (du[:, :half] * pg[2 * i:2 * i + CH, :]).astype(BF16)
            u[i:i + CH, half:] = (du[:, half:] * pg[2 * i + CH:2 * i + 2 * CH, :]).astype(BF16)
        fetch(1, c, m).start()
        then(0, (prow, 2 * f - prow))
        copy(1, u, dgs).start()
        v = u[...]
        for i in range(0, d, CH):
            y[i:i + CH, :] = dot(vw1[c, i:i + CH, :], v).astype(BF16)
        for i in (3, 4, 5):
            fetch(i, c, m).wait()
        b_norm(y, r, cv, 3, dy, o, stats, 2, acc.at[c], 2, ya)
        then(3)
        copy(2, o, drs).start()
        v = o[...]
        for i in range(0, d, CH):
            y[i:i + CH, :] = dot(vwo[c, i:i + CH, :], v).astype(BF16)
        for i in (1, 2):
            fetch(i, c, m).wait()
        b_heads(t, y, pg, heads, seq, lambda b: then(0, (b * part, part)))
        copy(3, t, dts).start()
        v = t[...]
        at = lax.broadcasted_iota(jnp.int32, (ROWS, LANES), 1)
        for i in range(0, d, CH):
            y[i:i + CH, :] = dot(vwq[c, :, i:i + CH], v, 0, 0).astype(BF16)
        b_norm(y, a, cv, 0, o, y, stats, 0, acc.at[c], 0, ya)
        for i in range(0, d, ROWS):
            e = 0.0
            for k in range(3):
                e = jnp.where(at == 4 + k, token_sum(t[k * d + i:k * d + i + ROWS, :].astype(F32)), e)
            acc[c, i:i + ROWS, :] += e
        then(4)
        then(5)
        for i, v, dst in ((0, dy, dys), (1, u, dgs), (2, o, drs), (3, t, dts)):
            copy(i, v, dst).wait()
        then(2)

    late = 1 - g.side
    loads = [pltpu.make_async_copy(x_in, vwq.at[late, pl.ds(0, tok), :], lead_sems.at[0]),
             pltpu.make_async_copy(dy_in, vwq.at[late, pl.ds(tok, tok), :], lead_sems.at[1]),
             pltpu.make_async_copy(vec, vvec, lead_sems.at[2]), pltpu.make_async_copy(bq, vbq, lead_sems.at[3]),
             pltpu.make_async_copy(b1, vb1, lead_sems.at[4])]
    for cp in loads:
        cp.start()
    for i in range(4):
        weight(g.side, i).start()
    barrier = pltpu.get_barrier_semaphore()
    for i in range(n):
        pl.semaphore_signal(barrier, inc=1, device_id={'pp': jnp.int32(i)})
    for cp in loads:
        cp.wait()
    out[0] = vwq[late, 0:tok, :].T
    out[1] = vwq[late, tok:2 * tok, :].T

    @pl.when(g.outside)
    def _():
        slots[0, 0] = out[0]
    fed = [pltpu.make_async_copy(out.at[0], x_t, lead_sems.at[0]), pltpu.make_async_copy(out.at[1], dy_t, lead_sems.at[1])]
    for cp in fed:
        cp.start()
    pl.semaphore_wait(barrier, n)
    for cp in fed:
        cp.wait()

    heads_at = ((0, 0), (1, g.last))
    for k, head in heads_at:
        spot = g.place(g.me + k * (g.last - 2 * g.me))

        @pl.when(g.me != head)
        def _():
            remote(x_t, slots.at[0, spot], feed_send.at[0, k], recv_sems.at[0, 0, spot], jnp.int32(head)).start()
            remote(dy_t, feed.at[spot], feed_send.at[1, k], feed_recv.at[spot], jnp.int32(head)).start()

    for c in range(2):
        rows = [vvec[i, c:c + 1, :] for i in range(6)] + [vbq[c, i:i + 1, :] for i in range(3)]
        rows += [vb1[c:c + 1, i:i + d] for i in range(0, f, d)]
        rows = [v.astype(F32) for v in rows] + [jnp.zeros((LANES - len(rows), d), F32)]
        vcols[c] = jnp.concatenate(rows, 0).T.astype(BF16)
    acc[...] = jnp.zeros_like(acc)

    def settle(par, flag):
        @pl.when(flag == 1)
        def _():
            remote(out.at[par], slots.at[0, 0], send_sems.at[par], recv_sems.at[0, 0, 0], g.me).wait_send()

    def body(s, carry):
        kind, back, sec, m, c = g.step(s)
        nxt = jnp.minimum(s + 1, g.steps - 1)
        kind2, back2, _, m2, c2 = g.step(nxt)
        more = both(back2, s + 1 < g.steps)
        onward = both(kind < 2, kind2 < 2)
        par = lax.rem(s, 2)
        inward = jnp.logical_or(kind == 0, kind == 2)
        outward = jnp.logical_not(inward)
        way = jnp.where(back, 1, 0)

        @pl.when(jnp.logical_or(s == 0, both(kind == 1, m == 0)))
        def _():
            for i in range(4):
                weight(c, i).wait()

        @pl.when(s == 0)
        def _():
            for i in range(4):
                weight(late, i).start()

        settle(par, carry[1])

        own = jnp.logical_or(both(outward, g.inside), both(kind == 0, m == 0, g.outside))

        @pl.when(jnp.logical_not(own))
        def _():
            remote(out.at[par], slots.at[sec, m], send_sems.at[par], recv_sems.at[way, sec, m], g.me).wait_recv()

        @pl.when(jnp.logical_not(back))
        def _():
            forward(c, m, slots.at[sec, m], out.at[par], carry[2] == 1, onward)

            @pl.when(more)
            def _():
                for i in (0, 2, 3, 4, 5):
                    fetch(i, c2, m2).start()

        @pl.when(back)
        def _():
            def then(i, at=None):
                @pl.when(more)
                def _():
                    fetch(i, c2, m2, at).start()

            backward(c, m, slots.at[sec, m], out.at[par], then)

        @pl.when(both(inward, g.inside))
        def _():
            slots[1 - sec, m] = out[par]

        @pl.when(both(inward, jnp.logical_not(g.inside)))
        def _():
            remote(out.at[par], slots.at[sec, m], send_sems.at[par], recv_sems.at[way, sec, m], g.inner).start()

        @pl.when(both(outward, jnp.logical_not(g.outside)))
        def _():
            remote(out.at[par], slots.at[sec, m], send_sems.at[par], recv_sems.at[way, sec, m], g.outer).start()

        owner = m + g.side * (g.last - 2 * m)
        done = both(outward, g.outside, m < g.half)
        for w, ref in ((0, y_out), (1, dx_out)):
            mine = both(done, way == w)

            @pl.when(both(mine, owner == g.me))
            def _():
                pltpu.make_async_copy(out.at[par], ref, send_sems.at[par]).start()

            @pl.when(both(mine, owner != g.me))
            def _():
                remote(out.at[par], ref, send_sems.at[par], final_sems.at[w], owner).start()

        @pl.when(both(kind == 1, g.outside))
        def _():
            @pl.when(m == 0)
            def _():
                pltpu.make_async_copy(dy_t, slots.at[1, m], recv_sems.at[1, 1, m]).start()

            @pl.when(m > 0)
            def _():
                remote(dy_t, feed.at[m], feed_send.at[1, 0], feed_recv.at[m], g.me).wait_recv()
                pltpu.make_async_copy(feed.at[m], slots.at[1, m], recv_sems.at[1, 1, m]).start()

        kept = jnp.logical_or(both(inward, g.inside), both(outward, g.outside, m >= g.half))
        return jnp.where(kept, 0, 1), carry[0], jnp.where(onward, 1, 0)

    before, earlier, _ = lax.fori_loop(0, g.steps, body, (jnp.int32(0),) * 3)
    settle(g.steps % 2, earlier)
    settle((g.steps + 1) % 2, before)
    for k, head in heads_at:
        @pl.when(g.me != head)
        def _():
            remote(x_t, slots.at[0, 0], feed_send.at[0, k], recv_sems.at[0, 0, 0], jnp.int32(head)).wait_send()
            remote(dy_t, feed.at[0], feed_send.at[1, k], feed_recv.at[0], jnp.int32(head)).wait_send()

    @pl.when(jnp.logical_not(g.outside))
    def _():
        for w, ref in ((0, y_out), (1, dx_out)):
            remote(out.at[0], ref, send_sems.at[0], final_sems.at[w], g.me).wait_recv()

    cp = pltpu.make_async_copy(acc, sums, b_sems.at[0])
    cp.start()
    cp.wait()


def run_walk(n, heads, seq, x, dy, weights, vec, bq, b1):
    tok, d = x.shape
    f = weights[2].shape[2]
    prow = (tok // seq) * (heads // 2) * seq
    st, vm, dma = jax.ShapeDtypeStruct, pltpu.VMEM, pltpu.SemaphoreType.DMA
    act, tall, hid = ((d, tok), BF16), ((3 * d, tok), BF16), ((f, tok), BF16)
    outs = [st(*act)] * 2 + [st((2, n) + v, k) for v, k in (
        act, tall, act, ((prow, 2 * seq), F32), ((2 * f, tok // 2), F32), ((8, tok), F32), act, act, act, hid,
        act, hid, act, tall)] + [st((n, d, tok), BF16), st((2, d, LANES), F32)] + [st(*act)] * 2
    scratch = [vm(w.shape, w.dtype) for w in weights] + [vm((2, d, LANES), BF16)] + [vm(v.shape, v.dtype) for v in (vec, bq, b1)] + [
        vm((2, n, d, tok), BF16), vm((2, d, tok), BF16), vm(*act), vm(*tall), vm(*act), vm(*act), vm(*hid),
        vm((2 * f, tok // 2), F32), vm((d, tok), F32), vm((8, tok), F32), vm((2, d, LANES), F32),
        dma((2, len(weights))), dma((2, 2, n)), dma((2,)), dma((2,)), dma((2, 2)), dma((n,)), dma((11,)), dma((6,)), dma((4,)),
        dma((5,))]
    args = (x, dy, *weights, vec, bq, b1)
    return pl.pallas_call(
        functools.partial(walk_kernel, n, heads, seq), out_shape=outs, in_specs=[HBM] * len(args), out_specs=[HBM] * len(outs),
        scratch_shapes=scratch, name='walk',
        compiler_params=pltpu.CompilerParams(vmem_limit_bytes=VMEM_LIMIT, collective_id=0, has_side_effects=True),
    )(*args)


PAIR = 2


def grads_kernel(n, *refs):
    ins, (y_t, dx_t, sums), refs = refs[:8], refs[8:11], refs[11:]
    outs, (b1_out, y_out, dx_out, vec_out, bq_out), refs = refs[:4], refs[4:9], refs[9:]
    accs, biases, refs = refs[:4], refs[4:7], refs[7:]
    buf, va, vb, vsum, b1_row, vec_rows, bq_rows, in_sems, out_sems, end_sems = refs
    steps = n // PAIR
    tok = buf.shape[3]
    d = y_t.shape[0]

    def fetches(c, k, j):
        slot = lax.rem(j, 2)
        rows, cols = ins[2 * k].shape[2], ins[2 * k + 1].shape[2]
        at = pl.ds(j * PAIR, PAIR)
        return (pltpu.make_async_copy(ins[2 * k].at[c, at], buf.at[slot, :, pl.ds(0, rows), :], in_sems.at[slot, 0]),
                pltpu.make_async_copy(ins[2 * k + 1].at[c, at], buf.at[slot, :, pl.ds(rows, cols), :], in_sems.at[slot, 1]))

    def begin(c, k, j):
        for cp in fetches(c, k, j):
            cp.start()

    def results(c, k):
        cps = [pltpu.make_async_copy(accs[k], outs[k].at[c], out_sems.at[k])]
        return cps

    acts = ((y_t, y_out), (dx_t, dx_out))
    loads = [pltpu.make_async_copy(h, va.at[i], end_sems.at[i]) for i, (h, _) in enumerate(acts)]
    loads.append(pltpu.make_async_copy(sums, vsum, end_sems.at[2]))
    for cp in loads:
        cp.start()
    begin(jnp.int32(0), 0, jnp.int32(0))
    for cp in loads:
        cp.wait()
    for i in range(2):
        vb[i] = va[i].T
    turned = [pltpu.make_async_copy(vb.at[i], h, end_sems.at[i]) for i, (_, h) in enumerate(acts)]
    for cp in turned:
        cp.start()
    for i in range(2):
        part = vsum[i].T
        for row, src in ((0, 0), (1, 1), (3, 2), (4, 3)):
            vec_rows[i, row] = part[src:src + 1, :]
        for row in range(3):
            bq_rows[i, row] = part[4 + row:5 + row, :]

    def stage(c, carry):
        for k in range(4):
            rows, cols = ins[2 * k].shape[2], ins[2 * k + 1].shape[2]

            def step(j, carry, k=k, rows=rows, cols=cols):
                @pl.when(j + 1 < steps)
                def _():
                    begin(c, k, j + 1)

                @pl.when(j + 1 == steps)
                def _():
                    if k < 3:
                        begin(c, k + 1, jnp.int32(0))
                    else:
                        @pl.when(c == 0)
                        def _():
                            begin(jnp.int32(1), 0, jnp.int32(0))

                @pl.when(jnp.logical_and(j == 0, c == 1))
                def _():
                    for cp in results(jnp.int32(0), k):
                        cp.wait()

                for cp in fetches(c, k, j):
                    cp.wait()
                slot = lax.rem(j, 2)
                later = j > 0
                parts = 2 if max(rows, cols) > 3 * d else 1
                tall = rows > cols
                height, width = (rows // parts, cols) if tall else (rows, cols // parts)

                def block(h, carry):
                    top = pl.multiple_of(h * height, CH) if tall and parts > 1 else 0
                    left = pl.multiple_of(h * width, CH) if not tall and parts > 1 else 0
                    w = [buf[slot, q, pl.ds(rows + left, width), :] for q in range(PAIR)]
                    for i in range(0, height, CH):
                        at = (pl.ds(top + i, CH), pl.ds(left, width))
                        z = jnp.where(later, accs[k][at], 0.0)
                        edge = i == 0 and k > 0
                        if edge:
                            e = jnp.where(later, biases[k - 1][:, at[1]], 0.0)
                        for q in range(PAIR):
                            x = buf[slot, q, pl.ds(top + i, CH), :]
                            if edge:
                                x = jnp.concatenate([x, jnp.ones((16, tok), BF16)], 0)
                            v = rounded(dot(x, w[q], 1, 1))
                            z = z + v[:CH]
                            if edge:
                                e = e + v[CH:CH + 8]
                        accs[k][at] = z
                        if edge and tall and parts > 1:
                            biases[k - 1][:, at[1]] = jnp.where(h == 0, e, biases[k - 1][:, at[1]])
                        elif edge:
                            biases[k - 1][:, at[1]] = e
                    return carry

                if parts > 1:
                    lax.fori_loop(0, parts, block, 0)
                else:
                    block(0, 0)
                return carry

            lax.fori_loop(0, steps, step, 0)
            for cp in results(c, k):
                cp.start()
        b1_row[c] = biases[0][0:1, :]
        vec_rows[c, 5] = biases[1][0:1, :]
        vec_rows[c, 2] = biases[2][0:1, :]
        return carry

    lax.fori_loop(0, 2, stage, 0)
    rows = [pltpu.make_async_copy(v, h, end_sems.at[2 + i])
            for i, (v, h) in enumerate(((b1_row, b1_out), (vec_rows, vec_out), (bq_rows, bq_out)))]
    for cp in rows:
        cp.start()
    for cp in rows + turned:
        cp.wait()
    for k in range(4):
        for cp in results(jnp.int32(1), k):
            cp.wait()


def run_grads(pairs, y_t, dx_t, sums):
    n, tok = pairs[0][0].shape[1], pairs[0][0].shape[3]
    sizes = [(a.shape[2], b.shape[2]) for a, b in pairs]
    d, f = sizes[1]
    st, vm, dma = jax.ShapeDtypeStruct, pltpu.VMEM, pltpu.SemaphoreType.DMA
    most = max(a + b for a, b in sizes)
    rows = [((2, 1, f), F32), ((2, 6, 1, d), F32), ((2, 3, 1, d), F32)]
    return pl.pallas_call(
        functools.partial(grads_kernel, n),
        out_shape=[st((2,) + v, F32) for v in sizes] + [st(*rows[0]), st((tok, d), BF16), st((tok, d), BF16), st(*rows[1]),
                                                        st(*rows[2])],
        in_specs=[HBM] * 11, out_specs=[HBM] * 9,
        scratch_shapes=[vm(v, F32) for v in sizes] + [vm((8, v[1]), F32) for v in sizes[1:]] + [
            vm((2, PAIR, most, tok), BF16), vm((2, d, tok), BF16), vm((2, tok, d), BF16), vm(sums.shape, F32)] + [
            vm(*v) for v in rows] + [dma((2, 2)), dma((4,)), dma((5,))],
        name='weight_grads', compiler_params=pltpu.CompilerParams(vmem_limit_bytes=VMEM_LIMIT),
    )(*[v for p in pairs for v in p], y_t, dx_t, sums)


def solution(mesh):
    data_spec = P(('dp', 'pp'))
    weight_spec = P('pp')

    def per_device(x, dy, w_qkv, w_attn, w_fc, w_proj, b_qkv, b_fc, vec_d):
        _, batch, seq, d = x.shape
        heads = w_qkv.shape[5]
        tok = batch * seq

        weights = (w_qkv.reshape(2, d, 3 * d).transpose(0, 2, 1), w_attn.reshape(2, d, d), w_fc[0, :, 0], w_proj[0, :, 0])
        y_t, dx_t, *stash = run_walk(
            mesh.shape['pp'], heads, seq, x.reshape(tok, d), dy.reshape(tok, d), weights,
            vec_d[0, :, 0].transpose(1, 0, 2), b_qkv.reshape(2, 3, d), b_fc[0, :, 0])
        as_, os_, bs, us, dys, dgs, drs, dts, _, sums = stash[6:16]
        gq, g1, g2, go, gb1, y, dx, gv, gbq = run_grads(((dts, as_), (bs, dgs), (us, dys), (os_, drs)), y_t, dx_t, sums)
        return (y.reshape(x.shape), dx.reshape(x.shape),
                gq.transpose(0, 2, 1).reshape(w_qkv.shape), go.reshape(w_attn.shape), g1.reshape(w_fc.shape),
                g2.reshape(w_proj.shape), gbq.reshape(b_qkv.shape), gb1.reshape(b_fc.shape), gv.reshape(vec_d.shape))

    return jax.shard_map(per_device, mesh=mesh, in_specs=(data_spec, data_spec) + (weight_spec,) * 7,
                         out_specs=(data_spec, data_spec) + (data_spec,) * 7, check_vma=False)
```
